32 devices in a mesh: lat: 4 (over y, x), lon: 8 (over z, core).
Axes of the slice: x: 2, y: 2, z: 4, core: 2. Of those that a mesh axis runs over, the one named last changes fastest.
Arguments:
- grid_latent: float32 [64, 360, 512], P('lat', 'lon'), may hold values from -6 to 6
- mesh_latent: float32 [20480, 512], P(('lat', 'lon')), may hold values from -6 to 6
- grid_senders: int32 [32, 32, 8], P(('lat', 'lon')), may hold values from 0 to 719
- grid_targets: int32 [32, 256], P(('lat', 'lon')), may hold values from -1 to 639, as said below
- grid_geometry: float32 [4, 32, 256], P(None, ('lat', 'lon')), may hold values from -6 to 6
- mesh_senders: int32 [32, 32, 8], P(('lat', 'lon')), may hold values from 0 to 639
- mesh_targets: int32 [32, 256], P(('lat', 'lon')), may hold values from -1 to 639, as said below
- mesh_geometry: float32 [4, 32, 256], P(None, ('lat', 'lon')), may hold values from -6 to 6
- encoder_sender: float32 [512, 512], replicated, may hold values from -0.25 to 0.25
- encoder_receiver: float32 [512, 512], replicated, may hold values from -0.25 to 0.25
- encoder_geometry: float32 [4, 512], replicated, may hold values from -3 to 3
- encoder_bias: float32 [512], replicated, may hold values from -3 to 3
- encoder_output: float32 [512, 512], replicated, may hold values from -0.25 to 0.25
- encoder_outbias: float32 [512], replicated, may hold values from -3 to 3
- update_self: float32 [512, 512], replicated, may hold values from -0.25 to 0.25
- update_summed: float32 [512, 512], replicated, may hold values from -0.25 to 0.25
- update_bias: float32 [512], replicated, may hold values from -3 to 3
- update_output: float32 [512, 512], replicated, may hold values from -0.25 to 0.25
- update_outbias: float32 [512], replicated, may hold values from -3 to 3
- process_sender: float32 [512, 512], replicated, may hold values from -0.25 to 0.25
- process_receiver: float32 [512, 512], replicated, may hold values from -0.25 to 0.25
- process_geometry: float32 [4, 512], replicated, may hold values from -3 to 3
- process_bias: float32 [512], replicated, may hold values from -3 to 3
- process_output: float32 [512, 512], replicated, may hold values from -0.25 to 0.25
- process_outbias: float32 [512], replicated, may hold values from -3 to 3
- refine_self: float32 [512, 512], replicated, may hold values from -0.25 to 0.25
- refine_summed: float32 [512, 512], replicated, may hold values from -0.25 to 0.25
- refine_bias: float32 [512], replicated, may hold values from -3 to 3
- refine_output: float32 [512, 512], replicated, may hold values from -0.25 to 0.25
- refine_outbias: float32 [512], replicated, may hold values from -3 to 3
Outputs:
- mesh_output: float32 [20480, 512], P(('lat', 'lon'))
The draws below stay inside these ranges and needn't reach their ends.
Inputs may be any that keep to these rules, and one draw needn't show every extreme that they name: `grid_targets`: entry [q, p * 8 + c] is the index among patch q's 640 nodes of the mesh node that receives grid edge slot c from patch p, or -1 for an empty slot; the live slots of a pair come first, and every patch's slots from itself are all live. `grid_senders`: entry [p, q, c] is the index of the sending cell among patch p's tile cells; entries of empty slots are ignored. `mesh_targets`: entry [q, p * 8 + c] is the index among patch q's 640 nodes of the mesh node that receives mesh edge slot c from patch p, or -1 for an empty slot; the live slots of a pair come first, and every patch's slots from itself are all live. `mesh_senders`: entry [p, q, c] is the index of the sending node among patch p's 640 nodes; entries of empty slots are ignored.
All inputs are finite; a program needn't handle non-finite values.
Results may differ from the reference program's by a relative error of at most 0.0003.
Values sent between devices are 32-bit elements; how exact they have to be, the bound alone decides.
No kernel may reach another device: no remote copies, remote signals or barrier semaphores. Data moves between devices by JAX's collectives and lax.ppermute only.
A program may use at most 128 MiB of HBM per device.

```python
import jax
import jax.numpy as jnp
from jax import lax

D = 512
GEO = 4
LAT_DEV = 16
LON_DEV = 45
M_DEV = 640
CAP_G = 8
CAP_M = 8
LAT_TILES = 4
LON_TILES = 8
PATCHES = 32
NLAT = 64
NLON = 360
MESH = 20480
GRID_SLOTS = 256
MESH_SLOTS = 256


def slot_targets(key, capacity):
    key_base, key_load, key_node, key_near = jax.random.split(key, 4)
    patch = jnp.arange(PATCHES, dtype=jnp.int32)
    lat_pos = patch // LON_TILES
    lon_pos = patch % LON_TILES
    lat_gap = jnp.abs(lat_pos[:, None] - lat_pos[None, :])
    lon_raw = jnp.abs(lon_pos[:, None] - lon_pos[None, :])
    lon_gap = jnp.minimum(lon_raw, LON_TILES - lon_raw)
    distance = lat_gap + lon_gap
    loading = jax.random.randint(key_load, (PATCHES,), 1, 4)
    base = jax.random.randint(key_base, (PATCHES, PATCHES), 0, capacity // 2 + 1)
    far_counts = jnp.minimum(capacity, base * loading[:, None] // 2)
    near_counts = jax.random.randint(key_near, (PATCHES, PATCHES), capacity // 2, capacity + 1)
    counts = jnp.where(distance <= 1, capacity, jnp.where(distance == 2, near_counts, far_counts))
    chosen = jax.random.randint(key_node, (PATCHES, PATCHES, capacity), 0, M_DEV)
    position = jnp.arange(capacity, dtype=jnp.int32)[None, None, :]
    chosen = jnp.where((position == 0) & jnp.eye(PATCHES, dtype=bool)[:, :, None], M_DEV - 1, chosen)
    live = position < counts[:, :, None]
    return jnp.where(live, chosen, -1).reshape(PATCHES, PATCHES * capacity).astype(jnp.int32)


def draw_grid_targets(key, part):
    return slot_targets(jax.random.fold_in(key, 11), CAP_G)


def draw_mesh_targets(key, part):
    return slot_targets(jax.random.fold_in(key, 23), CAP_M)


def plant(drawn, rng, low, top_value):
    extent = drawn.shape
    place = [jax.random.randint(jax.random.fold_in(rng, axis), (), 0, extent[axis]) for axis in range(len(extent))]
    drawn = drawn.at[tuple(place)].set(low)
    longest = extent.index(max(extent))
    place[longest] = (place[longest] + 1) % extent[longest]
    return drawn.at[tuple(place)].set(top_value)


def block_levels(key, shape, cuts, smallest, high):
    def one(dim, shards_of):
        draws = jax.random.uniform(jax.random.fold_in(jax.random.fold_in(key, 6), dim), (shards_of,), jnp.float32, smallest / len(cuts), high / len(cuts))
        return jnp.repeat(jnp.exp(draws), shape[dim] // shards_of).reshape((-1,) + (1,) * (len(shape) - dim - 1))

    gain = one(*cuts[0])
    for cut in cuts[1:]:
        gain = gain * one(*cut)
    return gain


def scatter_about(key, shape, deviation, bound, shards=(), kind=jnp.bfloat16):
    array = jax.random.normal(key, shape, jnp.float32) * deviation
    if len(shards) > 0:
        array = block_levels(key, shape, shards, -0.22, 0.18) * array
    return jnp.clip(array, min=-bound, max=bound).astype(kind)


def setup_inputs(seed: int = 0) -> dict:
    key_list = jax.random.split(jax.random.key(seed), 31)
    grid_latent = scatter_about(key_list[0], (NLAT, NLON, D), 1.0, 6.0, ((0, 4), (1, 8)), jnp.float32)
    mesh_latent = scatter_about(key_list[1], (MESH, D), 1.0, 6.0, ((0, 32),), jnp.float32)
    grid_senders = plant(jax.random.randint(key_list[2], (PATCHES, PATCHES, CAP_G), 0, LAT_DEV * LON_DEV), jax.random.fold_in(key_list[2], 1), 0, (LAT_DEV * LON_DEV) - 1).astype(jnp.int32)
    grid_targets = draw_grid_targets(jax.random.fold_in(key_list[30], 71), 0)
    grid_geometry = scatter_about(key_list[4], (GEO, PATCHES, GRID_SLOTS), 1.0, 6.0, ((1, 32),), jnp.float32)
    mesh_senders = plant(jax.random.randint(key_list[5], (PATCHES, PATCHES, CAP_M), 0, M_DEV), jax.random.fold_in(key_list[5], 1), 0, M_DEV - 1).astype(jnp.int32)
    mesh_targets = draw_mesh_targets(jax.random.fold_in(key_list[30], 71), 0)
    mesh_geometry = scatter_about(key_list[7], (GEO, PATCHES, MESH_SLOTS), 1.0, 6.0, ((1, 32),), jnp.float32)
    encoder_sender = scatter_about(key_list[8], (D, D), D ** -0.5, 0.25, (), jnp.float32)
    encoder_receiver = scatter_about(key_list[9], (D, D), D ** -0.5, 0.25, (), jnp.float32)
    encoder_geometry = scatter_about(key_list[10], (GEO, D), GEO ** -0.5, 3.0, (), jnp.float32)
    encoder_bias = scatter_about(key_list[11], (D,), 0.5, 3.0, (), jnp.float32)
    encoder_output = scatter_about(key_list[12], (D, D), D ** -0.5, 0.25, (), jnp.float32)
    encoder_outbias = scatter_about(key_list[13], (D,), 0.5, 3.0, (), jnp.float32)
    update_self = scatter_about(key_list[14], (D, D), D ** -0.5, 0.25, (), jnp.float32)
    update_summed = scatter_about(key_list[15], (D, D), D ** -0.5, 0.25, (), jnp.float32)
    update_bias = scatter_about(key_list[16], (D,), 0.5, 3.0, (), jnp.float32)
    update_output = scatter_about(key_list[17], (D, D), D ** -0.5, 0.25, (), jnp.float32)
    update_outbias = scatter_about(key_list[18], (D,), 0.5, 3.0, (), jnp.float32)
    process_sender = scatter_about(key_list[19], (D, D), D ** -0.5, 0.25, (), jnp.float32)
    process_receiver = scatter_about(key_list[20], (D, D), D ** -0.5, 0.25, (), jnp.float32)
    process_geometry = scatter_about(key_list[21], (GEO, D), GEO ** -0.5, 3.0, (), jnp.float32)
    process_bias = scatter_about(key_list[22], (D,), 0.5, 3.0, (), jnp.float32)
    process_output = scatter_about(key_list[23], (D, D), D ** -0.5, 0.25, (), jnp.float32)
    process_outbias = scatter_about(key_list[24], (D,), 0.5, 3.0, (), jnp.float32)
    refine_self = scatter_about(key_list[25], (D, D), D ** -0.5, 0.25, (), jnp.float32)
    refine_summed = scatter_about(key_list[26], (D, D), D ** -0.5, 0.25, (), jnp.float32)
    refine_bias = scatter_about(key_list[27], (D,), 0.5, 3.0, (), jnp.float32)
    refine_output = scatter_about(key_list[28], (D, D), D ** -0.5, 0.25, (), jnp.float32)
    refine_outbias = scatter_about(key_list[29], (D,), 0.5, 3.0, (), jnp.float32)
    return {"grid_latent": grid_latent, "mesh_latent": mesh_latent, "grid_senders": grid_senders, "grid_targets": grid_targets, "grid_geometry": grid_geometry, "mesh_senders": mesh_senders, "mesh_targets": mesh_targets, "mesh_geometry": mesh_geometry, "encoder_sender": encoder_sender, "encoder_receiver": encoder_receiver, "encoder_geometry": encoder_geometry, "encoder_bias": encoder_bias, "encoder_output": encoder_output, "encoder_outbias": encoder_outbias, "update_self": update_self, "update_summed": update_summed, "update_bias": update_bias, "update_output": update_output, "update_outbias": update_outbias, "process_sender": process_sender, "process_receiver": process_receiver, "process_geometry": process_geometry, "process_bias": process_bias, "process_output": process_output, "process_outbias": process_outbias, "refine_self": refine_self, "refine_summed": refine_summed, "refine_bias": refine_bias, "refine_output": refine_output, "refine_outbias": refine_outbias}


PRECISE = lax.Precision.HIGHEST

def matmul(left, right):
    return jnp.dot(left, right, precision=PRECISE, preferred_element_type=jnp.float32)

def norm_rows(values):
    average = lax.optimization_barrier(jnp.mean(values, axis=-1, keepdims=True))
    centred = values - average
    spread = lax.optimization_barrier(jnp.mean(centred * centred, axis=-1, keepdims=True))
    return centred * lax.rsqrt(spread + 1e-05)

def edge_block(sender_rows, receiver_rows, geometry, weight_geometry, bias_hidden, weight_output, bias_output):
    geometric = lax.dot_general(geometry, weight_geometry, (((0,), (0,)), ((), ())), precision=PRECISE, preferred_element_type=jnp.float32)
    hidden = jax.nn.silu(sender_rows + receiver_rows + geometric + bias_hidden)
    return norm_rows(matmul(hidden, weight_output) + bias_output)

def aggregate(messages, targets, number):
    one_hot = (jnp.arange(number, dtype=jnp.int32)[:, None] == targets[None, :]).astype(jnp.float32)
    return matmul(one_hot, messages)

def node_block(latent, summed, weight_self, weight_summed, bias_hidden, weight_output, bias_output):
    hidden = jax.nn.silu(matmul(latent, weight_self) + matmul(summed, weight_summed) + bias_hidden)
    return latent + norm_rows(matmul(hidden, weight_output) + bias_output)

def reference(grid_latent, mesh_latent, grid_senders, grid_targets, grid_geometry, mesh_senders, mesh_targets, mesh_geometry, encoder_sender, encoder_receiver, encoder_geometry, encoder_bias, encoder_output, encoder_outbias, update_self, update_summed, update_bias, update_output, update_outbias, process_sender, process_receiver, process_geometry, process_bias, process_output, process_outbias, refine_self, refine_summed, refine_bias, refine_output, refine_outbias):
    tiles = grid_latent.reshape(LAT_TILES, LAT_DEV, LON_TILES, LON_DEV, D).transpose(0, 2, 1, 3, 4).reshape(PATCHES, LAT_DEV * LON_DEV, D)
    patch_nodes = mesh_latent.reshape(PATCHES, M_DEV, D)
    sources = jnp.arange(PATCHES, dtype=jnp.int32)[:, None]

    def encode(target):
        rows = tiles[sources, grid_senders[:, target, :]].reshape(GRID_SLOTS, D)
        sender_rows = matmul(rows, encoder_sender)
        targets = grid_targets[target]
        local = patch_nodes[target]
        receiver_rows = matmul(local, encoder_receiver)[jnp.maximum(targets, 0)]
        messages = edge_block(sender_rows, receiver_rows, grid_geometry[:, target, :], encoder_geometry, encoder_bias, encoder_output, encoder_outbias)
        summed = aggregate(messages, targets, M_DEV)
        return node_block(local, summed, update_self, update_summed, update_bias, update_output, update_outbias)
    encoded = lax.map(encode, jnp.arange(PATCHES, dtype=jnp.int32))

    def process(target):
        rows = encoded[sources, mesh_senders[:, target, :]].reshape(MESH_SLOTS, D)
        sender_rows = matmul(rows, process_sender)
        targets = mesh_targets[target]
        local = encoded[target]
        receiver_rows = matmul(local, process_receiver)[jnp.maximum(targets, 0)]
        messages = edge_block(sender_rows, receiver_rows, mesh_geometry[:, target, :], process_geometry, process_bias, process_output, process_outbias)
        summed = aggregate(messages, targets, M_DEV)
        return node_block(local, summed, refine_self, refine_summed, refine_bias, refine_output, refine_outbias)
    refined = lax.map(process, jnp.arange(PATCHES, dtype=jnp.int32))
    return refined.reshape(MESH, D)
```

```python
import functools

import jax
import jax.numpy as jnp
from jax import lax
from jax.experimental import pallas as pl
from jax.experimental.pallas import tpu as pltpu
from jax.sharding import PartitionSpec as P

F32 = jnp.float32
BF16 = jnp.bfloat16
VMEM = pl.BlockSpec(memory_space=pltpu.VMEM)
SMEM = pl.BlockSpec(memory_space=pltpu.SMEM)


def split(values):
    high = values.astype(BF16)
    low = (values - high.astype(F32)).astype(BF16)
    return high, low


def dot(left, right):
    return jnp.dot(left, right, preferred_element_type=F32)


def dot3(left, high, low):
    left_high, left_low = split(left)
    return dot(left_high, high) + (dot(left_low, high) + dot(left_high, low))


def pick(one_hot, values):
    high, low = split(values)
    return dot(one_hot, high) + dot(one_hot, low)


def silu(values):
    return values * (1.0 / (1.0 + jnp.exp(-values)))


def norm_rows(values):
    average = jnp.mean(values, axis=-1, keepdims=True)
    centred = values - average
    spread = jnp.mean(centred * centred, axis=-1, keepdims=True)
    return centred * lax.rsqrt(spread + 1e-05)


def gather_rows(count, row_of, pairs, unroll=8):
    def step(i, carry):
        row = row_of(i)
        for source, target in pairs:
            target[pl.ds(i, 1), :] = source[pl.ds(row, 1), :]
        return carry

    lax.fori_loop(0, count, step, 0, unroll=unroll)


def geometry_rows(geometry_ref, weight_ref):
    features, _, slots = geometry_ref.shape
    rows = jnp.concatenate([geometry_ref[k] for k in range(features)], axis=0)
    padded = jnp.concatenate([rows, jnp.zeros((8 - features % 8, slots), F32)], axis=0)
    columns = padded.T
    total = columns[:, 0:1] * weight_ref[0:1, :]
    for k in range(1, features):
        total += columns[:, k : k + 1] * weight_ref[k : k + 1, :]
    return total


def target_matrix(number, targets_ref):
    slots = targets_ref.shape[1]
    nodes = lax.broadcasted_iota(jnp.int32, (number, slots), 0)
    return jnp.where(nodes == targets_ref[...], 1.0, 0.0).astype(F32)


def slot_order(index_ref):
    capacity = index_ref.shape[0]
    bits = capacity.bit_length() - 1
    assert capacity == 1 << bits
    return lambda i: index_ref[i & (capacity - 1), i >> bits]


def pack_kernel(rows_in, columns_in, index_ref, grid_ref, out_ref):
    shift = 20
    factor = -(-(1 << shift) // columns_in)
    assert all((i * factor) >> shift == i // columns_in for i in range(rows_in * columns_in))
    order = slot_order(index_ref)

    def row_of(i):
        cell = order(i)
        row = (cell * factor) >> shift
        return (cell - row * columns_in) * rows_in + row

    gather_rows(out_ref.shape[0], row_of, [(grid_ref, out_ref)])


def before_kernel(
    grid_targets_s,
    mesh_senders_s,
    grid_targets,
    geometry,
    nodes,
    weight_receiver,
    weight_geometry,
    edge_bias,
    weight_self,
    node_bias,
    *refs,
):
    count = (len(refs) - 8) // 3
    weights = refs[:count]
    received, self_all, self_sent, nodes_sent, match = refs[count : count + 5]
    splits = refs[count + 5 : 3 * count + 5]
    near, table, chosen = refs[3 * count + 5 :]
    for k, weight in enumerate(weights):
        splits[2 * k][...], splits[2 * k + 1][...] = split(weight[...])
    self_all[...] = dot3(nodes[...], *split(weight_self[...])) + node_bias[...]
    gather_rows(
        received.shape[0], lambda i: jnp.maximum(grid_targets_s[0, i], 0), [(nodes, near)]
    )
    received[...] = (
        dot3(near[...], *split(weight_receiver[...]))
        + geometry_rows(geometry, weight_geometry)
        + edge_bias[...]
    )
    table[...] = target_matrix(nodes.shape[0], grid_targets)
    gather_rows(
        nodes_sent.shape[0],
        slot_order(mesh_senders_s),
        [(nodes, nodes_sent), (self_all, self_sent), (table, chosen)],
    )
    match[...] = chosen[...].astype(BF16)


def edges(arrived, received, sender, output, bias, summed):
    hidden = silu(dot3(arrived[...], *sender) + received[...])
    messages = norm_rows(dot3(hidden, *output) + bias[...])
    return dot3(messages, *summed)


def encode_kernel(
    arrived,
    received,
    self_sent,
    nodes_sent,
    match,
    sender_high,
    sender_low,
    output_high,
    output_low,
    output_bias,
    summed_high,
    summed_low,
    update_high,
    update_low,
    update_bias,
    sent,
    parts,
):
    part = edges(
        arrived,
        received,
        (sender_high[...], sender_low[...]),
        (output_high[...], output_low[...]),
        output_bias,
        (summed_high[...], summed_low[...]),
    )
    parts[...] = part
    hidden = silu(self_sent[...] + pick(match[...], part))
    sent[...] = nodes_sent[...] + norm_rows(
        dot3(hidden, update_high[...], update_low[...]) + update_bias[...]
    )


def between_kernel(
    mesh_targets_s,
    grid_targets,
    mesh_targets,
    geometry,
    nodes,
    self_all,
    parts,
    update_high,
    update_low,
    update_bias,
    weight_receiver,
    weight_geometry,
    edge_bias,
    weight_self,
    node_bias,
    refine_high,
    refine_low,
    refine_bias,
    received,
    self_near,
    near,
    match,
    base,
    encoded,
    self_next,
    table,
    chosen,
):
    one_hot = target_matrix(nodes.shape[0], grid_targets).astype(BF16)
    hidden = silu(self_all[...] + pick(one_hot, parts[...]))
    encoded[...] = nodes[...] + norm_rows(
        dot3(hidden, update_high[...], update_low[...]) + update_bias[...]
    )
    self_next[...] = dot3(encoded[...], *split(weight_self[...])) + node_bias[...]
    table[...] = target_matrix(nodes.shape[0], mesh_targets)
    gather_rows(
        near.shape[0],
        lambda i: jnp.maximum(mesh_targets_s[0, i], 0),
        [(encoded, near), (self_next, self_near), (table, chosen)],
    )
    match[...] = chosen[...].astype(BF16)
    received[...] = (
        dot3(near[...], *split(weight_receiver[...]))
        + geometry_rows(geometry, weight_geometry)
        + edge_bias[...]
    )
    base[...] = encoded[...] + norm_rows(
        dot3(silu(self_next[...]), refine_high[...], refine_low[...]) + refine_bias[...]
    )


def refine_kernel(
    mesh_targets_s,
    arrived,
    received,
    self_near,
    near,
    match,
    base,
    sender_high,
    sender_low,
    output_high,
    output_low,
    output_bias,
    summed_high,
    summed_low,
    refine_high,
    refine_low,
    refine_bias,
    out,
    rows,
):
    part = edges(
        arrived,
        received,
        (sender_high[...], sender_low[...]),
        (output_high[...], output_low[...]),
        output_bias,
        (summed_high[...], summed_low[...]),
    )
    hidden = silu(self_near[...] + pick(match[...], part))
    rows[...] = near[...] + norm_rows(
        dot3(hidden, refine_high[...], refine_low[...]) + refine_bias[...]
    )
    out[...] = base[...]

    def place(i, carry):
        target = mesh_targets_s[0, i]

        @pl.when(target >= 0)
        def _():
            out[pl.ds(target, 1), :] = rows[pl.ds(i, 1), :]

        return carry

    lax.fori_loop(0, rows.shape[0], place, 0, unroll=8)


def shape(dims, kind=F32):
    return jax.ShapeDtypeStruct(dims, kind)


def call(kernel, out_shape, scalars, arrays, scratch=(), flops=0, name=None):
    return pl.pallas_call(
        kernel,
        out_shape=out_shape,
        in_specs=[SMEM] * len(scalars) + [VMEM] * len(arrays),
        out_specs=jax.tree.map(lambda _: VMEM, out_shape),
        scratch_shapes=list(scratch),
        cost_estimate=pl.CostEstimate(flops=flops, bytes_accessed=4 * 2**20, transcendentals=0),
        compiler_params=pltpu.CompilerParams(vmem_limit_bytes=56 * 2**20),
        name=name,
    )(*scalars, *arrays)


def exchange(rows, patches):
    blocks = rows.reshape(patches, -1, rows.shape[1])
    blocks = lax.all_to_all(blocks, ("lat", "lon"), split_axis=0, concat_axis=0, tiled=True)
    return blocks.reshape(rows.shape)


def per_device(
    grid_latent,
    mesh_latent,
    grid_senders,
    grid_targets,
    grid_geometry,
    mesh_senders,
    mesh_targets,
    mesh_geometry,
    encoder_sender,
    encoder_receiver,
    encoder_geometry,
    encoder_bias,
    encoder_output,
    encoder_outbias,
    update_self,
    update_summed,
    update_bias,
    update_output,
    update_outbias,
    process_sender,
    process_receiver,
    process_geometry,
    process_bias,
    process_output,
    process_outbias,
    refine_self,
    refine_summed,
    refine_bias,
    refine_output,
    refine_outbias,
):
    number, width = mesh_latent.shape
    patches = grid_senders.shape[1]
    grid_slots = grid_targets.shape[1]
    mesh_slots = mesh_targets.shape[1]
    rows_in, columns_in = grid_latent.shape[:2]
    square = 2 * width * width
    row = lambda bias: bias.reshape(1, width)

    cells = grid_latent.transpose(1, 0, 2).reshape(rows_in * columns_in, width)
    packed = call(
        functools.partial(pack_kernel, rows_in, columns_in),
        shape((grid_slots, width)),
        [grid_senders[0].T],
        [cells],
        flops=1000,
        name="pack",
    )
    grid_in = exchange(packed, patches)

    weights = [
        encoder_sender,
        encoder_output,
        update_summed,
        update_output,
        process_sender,
        process_output,
        refine_summed,
        refine_output,
    ]
    senders = mesh_senders[0].T
    received, self_all, self_sent, nodes_sent, match, *splits = call(
        before_kernel,
        [
            shape((grid_slots, width)),
            shape((number, width)),
            shape((mesh_slots, width)),
            shape((mesh_slots, width)),
            shape((mesh_slots, grid_slots), BF16),
        ]
        + [shape((width, width), BF16)] * (2 * len(weights)),
        [grid_targets, senders],
        [
            grid_targets,
            grid_geometry,
            mesh_latent,
            encoder_receiver,
            encoder_geometry,
            row(encoder_bias),
            update_self,
            row(update_bias),
        ]
        + weights,
        [
            pltpu.VMEM((grid_slots, width), F32),
            pltpu.VMEM((number, grid_slots), F32),
            pltpu.VMEM((mesh_slots, grid_slots), F32),
        ],
        flops=(number + grid_slots) * square * 3,
        name="before",
    )
    sent, parts = call(
        encode_kernel,
        [shape((mesh_slots, width)), shape((grid_slots, width))],
        [],
        [grid_in, received, self_sent, nodes_sent, match]
        + splits[0:4]
        + [row(encoder_outbias)]
        + splits[4:8]
        + [row(update_outbias)],
        flops=(3 * grid_slots + mesh_slots) * square * 3,
        name="encode",
    )
    mesh_in = exchange(sent, patches)
    received, self_near, near, match, base = call(
        between_kernel,
        [
            shape((mesh_slots, width)),
            shape((mesh_slots, width)),
            shape((mesh_slots, width)),
            shape((mesh_slots, mesh_slots), BF16),
            shape((number, width)),
        ],
        [mesh_targets],
        [
            grid_targets,
            mesh_targets,
            mesh_geometry,
            mesh_latent,
            self_all,
            parts,
            splits[6],
            splits[7],
            row(update_outbias),
            process_receiver,
            process_geometry,
            row(process_bias),
            refine_self,
            row(refine_bias),
            splits[14],
            splits[15],
            row(refine_outbias),
        ],
        [
            pltpu.VMEM((number, width), F32),
            pltpu.VMEM((number, width), F32),
            pltpu.VMEM((number, mesh_slots), F32),
            pltpu.VMEM((mesh_slots, mesh_slots), F32),
        ],
        flops=(3 * number + mesh_slots) * square * 3,
        name="between",
    )
    return call(
        refine_kernel,
        shape((number, width)),
        [mesh_targets],
        [mesh_in, received, self_near, near, match, base]
        + splits[8:12]
        + [row(process_outbias)]
        + splits[12:16]
        + [row(refine_outbias)],
        [pltpu.VMEM((mesh_slots, width), F32)],
        flops=4 * mesh_slots * square * 3,
        name="refine",
    )


def solution(mesh):
    patch = P(("lat", "lon"), None)
    block = P(("lat", "lon"), None, None)
    feature = P(None, ("lat", "lon"), None)
    return jax.shard_map(
        per_device,
        mesh=mesh,
        in_specs=(P("lat", "lon", None), patch, block, patch, feature, block, patch, feature)
        + (P(),) * 22,
        out_specs=patch,
        check_vma=False,
    )
```

```python
import functools

import jax
import jax.numpy as jnp
from jax import lax
from jax.experimental import pallas as pl
from jax.experimental.pallas import tpu as pltpu
from jax.sharding import PartitionSpec as P

F32 = jnp.float32
BF16 = jnp.bfloat16
VMEM = pl.BlockSpec(memory_space=pltpu.VMEM)
SMEM = pl.BlockSpec(memory_space=pltpu.SMEM)
HBM = pl.BlockSpec(memory_space=pltpu.HBM)


def split(values):
    high = values.astype(BF16)
    low = (values - high.astype(F32)).astype(BF16)
    return high, low


def dot(left, right):
    return jnp.dot(left, right, preferred_element_type=F32)


def dot3(left, high, low):
    left_high, left_low = split(left)
    return dot(left_high, high) + (dot(left_low, high) + dot(left_high, low))


def pick(one_hot, values):
    high, low = split(values)
    return dot(one_hot, high) + dot(one_hot, low)


def silu(values):
    return values * (1.0 / (1.0 + jnp.exp(-values)))


def norm_rows(values):
    average = jnp.mean(values, axis=-1, keepdims=True)
    centred = values - average
    spread = jnp.mean(centred * centred, axis=-1, keepdims=True)
    return centred * lax.rsqrt(spread + 1e-05)


def gather_rows(first, count, row_of, pairs, unroll=16):
    def step(i, carry):
        row = row_of(i)
        for source, target in pairs:
            target[pl.ds(i, 1), :] = source[pl.ds(row, 1), :]
        return carry

    lax.fori_loop(first, first + count, step, 0, unroll=unroll)


def geometry_rows(geometry_ref, weight_ref):
    features, _, slots = geometry_ref.shape
    rows = jnp.concatenate([geometry_ref[k] for k in range(features)], axis=0)
    padded = jnp.concatenate([rows, jnp.zeros((8 - features % 8, slots), F32)], axis=0)
    columns = padded.T
    total = columns[:, 0:1] * weight_ref[0:1, :]
    for k in range(1, features):
        total += columns[:, k : k + 1] * weight_ref[k : k + 1, :]
    return total


def target_matrix(number, targets_ref):
    slots = targets_ref.shape[1]
    nodes = lax.broadcasted_iota(jnp.int32, (number, slots), 0)
    return jnp.where(nodes == targets_ref[...], 1.0, 0.0).astype(F32)


def slot_order(index_ref):
    capacity = index_ref.shape[0]
    bits = capacity.bit_length() - 1
    assert capacity == 1 << bits
    return lambda i: index_ref[i & (capacity - 1), i >> bits]


class Copies:
    def __init__(self, semaphores):
        self.semaphores = semaphores
        self.used = 0

    def start(self, source, target):
        copy = pltpu.make_async_copy(source, target, self.semaphores.at[self.used])
        self.used += 1
        copy.start()
        return copy


def wait(*copies):
    for copy in copies:
        copy.wait()


def pack_kernel(
    rows_in, columns_in, senders_ref, cells_ref, out_ref, cells, out, senders, semaphores
):
    copies = Copies(semaphores)
    load_senders = copies.start(senders_ref, senders)
    load = copies.start(cells_ref, cells)
    shift = 20
    factor = -(-(1 << shift) // columns_in)
    assert all((i * factor) >> shift == i // columns_in for i in range(rows_in * columns_in))
    order = slot_order(senders)

    def row_of(i):
        cell = order(i)
        row = (cell * factor) >> shift
        return (cell - row * columns_in) * rows_in + row

    wait(load_senders, load)
    chunk = out.shape[0] // 4
    stores = []
    for first in range(0, out.shape[0], chunk):
        gather_rows(first, chunk, row_of, [(cells, out)])
        stores.append(
            copies.start(out.at[pl.ds(first, chunk)], out_ref.at[pl.ds(first, chunk)])
        )
    wait(*stores)


def before_kernel(
    grid_targets_s,
    mesh_senders_s,
    grid_targets,
    geometry,
    weight_geometry,
    edge_bias,
    node_bias,
    bias_one,
    bias_two,
    nodes_ref,
    weight_self_ref,
    weight_receiver_ref,
    *refs,
):
    count = 8
    weight_refs, refs = refs[:count], refs[count:]
    inner, refs = refs[:5], refs[5:]
    received_ref, self_all_ref, self_sent_ref, nodes_sent_ref, match_ref = refs[:5]
    split_refs, refs = refs[5 : 2 * count + 1], refs[2 * count + 1 :]
    nodes, weight_self, weight_receiver, weights, refs = *refs[:3], refs[3 : 3 + count], refs[3 + count :]
    received, self_all, self_sent, nodes_sent, match = refs[:5]
    splits, refs = refs[5 : 2 * count + 1], refs[2 * count + 1 :]
    near, table, chosen, semaphores = refs
    copies = Copies(semaphores)
    load_nodes = copies.start(nodes_ref, nodes)
    load_self = copies.start(weight_self_ref, weight_self)
    load_receiver = copies.start(weight_receiver_ref, weight_receiver)
    loads = [copies.start(ref, weight) for ref, weight in zip(weight_refs, weights, strict=True)]
    inner[4][0:1, :] = bias_one[...]
    inner[4][1:2, :] = bias_two[...]
    table[...] = target_matrix(nodes.shape[0], grid_targets)
    stores = []
    wait(load_nodes, load_self)
    self_all[...] = dot3(nodes[...], *split(weight_self[...])) + node_bias[...]
    stores.append(copies.start(self_all, self_all_ref))
    gather_rows(
        0,
        mesh_senders_s.shape[0] * mesh_senders_s.shape[1],
        slot_order(mesh_senders_s),
        [(nodes, nodes_sent), (self_all, self_sent), (table, chosen)],
    )
    match[...] = chosen[...].astype(BF16)
    stores.append(copies.start(self_sent, self_sent_ref))
    stores.append(copies.start(nodes_sent, nodes_sent_ref))
    stores.append(copies.start(match, match_ref))
    gather_rows(
        0, near.shape[0], lambda i: jnp.maximum(grid_targets_s[0, i], 0), [(nodes, near)]
    )
    wait(load_receiver)
    received[...] = (
        dot3(near[...], *split(weight_receiver[...]))
        + geometry_rows(geometry, weight_geometry)
        + edge_bias[...]
    )
    stores.append(copies.start(received, received_ref))
    for k in range(count):
        wait(loads[k])
        if k < 2:
            inner[2 * k][...], inner[2 * k + 1][...] = split(weights[k][...])
        else:
            at = 2 * (k - 2)
            splits[at][...], splits[at + 1][...] = split(weights[k][...])
            stores.append(copies.start(splits[at], split_refs[at]))
            stores.append(copies.start(splits[at + 1], split_refs[at + 1]))
    wait(*stores)


def encode_kernel(
    arrived,
    sender_high,
    sender_low,
    output_high,
    output_low,
    biases,
    received_ref,
    summed_high_ref,
    summed_low_ref,
    self_sent_ref,
    match_ref,
    update_high_ref,
    update_low_ref,
    nodes_sent_ref,
    sent_ref,
    parts_ref,
    received,
    summed_high,
    summed_low,
    self_sent,
    match,
    update_high,
    update_low,
    nodes_sent,
    sent,
    parts,
    semaphores,
):
    copies = Copies(semaphores)
    load_received = copies.start(received_ref, received)
    load_summed_high = copies.start(summed_high_ref, summed_high)
    load_summed_low = copies.start(summed_low_ref, summed_low)
    load_match = copies.start(match_ref, match)
    load_self = copies.start(self_sent_ref, self_sent)
    load_update_high = copies.start(update_high_ref, update_high)
    load_update_low = copies.start(update_low_ref, update_low)
    load_nodes = copies.start(nodes_sent_ref, nodes_sent)
    hidden = dot3(arrived[...], sender_high[...], sender_low[...])
    wait(load_received)
    hidden = silu(hidden + received[...])
    messages = norm_rows(dot3(hidden, output_high[...], output_low[...]) + biases[0:1, :])
    wait(load_summed_high, load_summed_low)
    part = dot3(messages, summed_high[...], summed_low[...])
    parts[...] = part
    store_parts = copies.start(parts, parts_ref)
    wait(load_match, load_self)
    hidden = silu(self_sent[...] + pick(match[...], part))
    wait(load_update_high, load_update_low, load_nodes)
    sent[...] = nodes_sent[...] + norm_rows(
        dot3(hidden, update_high[...], update_low[...]) + biases[1:2, :]
    )
    store_sent = copies.start(sent, sent_ref)
    wait(store_parts, store_sent)


def between_kernel(
    mesh_targets_s,
    grid_targets,
    mesh_targets,
    geometry,
    weight_geometry,
    edge_bias,
    node_bias,
    update_bias,
    refine_bias,
    bias_one,
    sender_high_ref,
    sender_low_ref,
    output_high_ref,
    output_low_ref,
    parts_ref,
    self_all_ref,
    nodes_ref,
    update_high_ref,
    update_low_ref,
    weight_self_ref,
    weight_receiver_ref,
    refine_high_ref,
    refine_low_ref,
    sender_high,
    sender_low,
    output_high,
    output_low,
    biases,
    received_ref,
    self_near_ref,
    near_ref,
    match_ref,
    base_ref,
    parts,
    self_all,
    nodes,
    update_high,
    update_low,
    weight_self,
    weight_receiver,
    refine_high,
    refine_low,
    received,
    self_near,
    near,
    match,
    base,
    encoded,
    self_next,
    table,
    chosen,
    semaphores,
):
    copies = Copies(semaphores)
    load_parts = copies.start(parts_ref, parts)
    load_all = copies.start(self_all_ref, self_all)
    load_update_high = copies.start(update_high_ref, update_high)
    load_update_low = copies.start(update_low_ref, update_low)
    load_nodes = copies.start(nodes_ref, nodes)
    load_self = copies.start(weight_self_ref, weight_self)
    load_receiver = copies.start(weight_receiver_ref, weight_receiver)
    load_refine_high = copies.start(refine_high_ref, refine_high)
    load_refine_low = copies.start(refine_low_ref, refine_low)
    passed = [
        copies.start(sender_high_ref, sender_high),
        copies.start(sender_low_ref, sender_low),
        copies.start(output_high_ref, output_high),
        copies.start(output_low_ref, output_low),
    ]
    stores = []
    biases[0:1, :] = bias_one[...]
    biases[1:2, :] = refine_bias[...]
    one_hot = target_matrix(nodes.shape[0], grid_targets).astype(BF16)
    table[...] = target_matrix(nodes.shape[0], mesh_targets)
    wait(load_parts, load_all)
    hidden = silu(self_all[...] + pick(one_hot, parts[...]))
    wait(load_update_high, load_update_low, load_nodes)
    encoded[...] = nodes[...] + norm_rows(
        dot3(hidden, update_high[...], update_low[...]) + update_bias[...]
    )
    wait(load_self)
    self_next[...] = dot3(encoded[...], *split(weight_self[...])) + node_bias[...]
    gather_rows(
        0,
        near.shape[0],
        lambda i: jnp.maximum(mesh_targets_s[0, i], 0),
        [(encoded, near), (self_next, self_near), (table, chosen)],
    )
    match[...] = chosen[...].astype(BF16)
    stores.append(copies.start(near, near_ref))
    stores.append(copies.start(self_near, self_near_ref))
    stores.append(copies.start(match, match_ref))
    wait(load_receiver)
    received[...] = (
        dot3(near[...], *split(weight_receiver[...]))
        + geometry_rows(geometry, weight_geometry)
        + edge_bias[...]
    )
    stores.append(copies.start(received, received_ref))
    wait(load_refine_high, load_refine_low)
    base[...] = encoded[...] + norm_rows(
        dot3(silu(self_next[...]), refine_high[...], refine_low[...]) + refine_bias[...]
    )
    stores.append(copies.start(base, base_ref))
    wait(*passed, *stores)


def refine_kernel(
    mesh_targets_s,
    arrived,
    sender_high,
    sender_low,
    output_high,
    output_low,
    biases,
    received_ref,
    summed_high_ref,
    summed_low_ref,
    match_ref,
    self_near_ref,
    refine_high_ref,
    refine_low_ref,
    near_ref,
    base_ref,
    out_ref,
    received,
    summed_high,
    summed_low,
    match,
    self_near,
    refine_high,
    refine_low,
    near,
    base,
    rows,
    semaphores,
):
    copies = Copies(semaphores)
    number = base_ref.shape[0]
    load_received = copies.start(received_ref, received)
    load_summed_high = copies.start(summed_high_ref, summed_high)
    load_summed_low = copies.start(summed_low_ref, summed_low)
    load_match = copies.start(match_ref, match)
    load_self = copies.start(self_near_ref, self_near)
    load_refine_high = copies.start(refine_high_ref, refine_high)
    load_refine_low = copies.start(refine_low_ref, refine_low)
    load_near = copies.start(near_ref, near)
    load_base = copies.start(base_ref, base.at[pl.ds(0, number)])
    hidden = dot3(arrived[...], sender_high[...], sender_low[...])
    wait(load_received)
    hidden = silu(hidden + received[...])
    messages = norm_rows(dot3(hidden, output_high[...], output_low[...]) + biases[0:1, :])
    wait(load_summed_high, load_summed_low)
    part = dot3(messages, summed_high[...], summed_low[...])
    wait(load_match, load_self)
    hidden = silu(self_near[...] + pick(match[...], part))
    wait(load_refine_high, load_refine_low, load_near)
    rows[...] = near[...] + norm_rows(
        dot3(hidden, refine_high[...], refine_low[...]) + biases[1:2, :]
    )
    wait(load_base)

    def place(i, carry):
        target = mesh_targets_s[0, i]
        target = jnp.where(target < 0, number, target)
        base[pl.ds(target, 1), :] = rows[pl.ds(i, 1), :]
        return carry

    lax.fori_loop(0, rows.shape[0], place, 0, unroll=16)
    wait(copies.start(base.at[pl.ds(0, number)], out_ref))


def flat(dims, kind=F32):
    return jax.ShapeDtypeStruct(dims, kind)


def call(
    kernel, name, flops, scalars, small, kept, large, results, held=(), scratch=(), direct=()
):
    direct = [pltpu.with_memory_space_constraint(array, pltpu.HBM) for array in direct]
    kept = [pltpu.with_memory_space_constraint(array, pltpu.VMEM) for array in kept]
    large = [pltpu.with_memory_space_constraint(array, pltpu.HBM) for array in large]
    twins = [pltpu.VMEM(array.shape, array.dtype) for array in [*large, *results]]
    twins += list(scratch)
    size = sum(4 * spec.inner_aval.size for spec in twins)
    return pl.pallas_call(
        kernel,
        out_shape=[pltpu.VMEM(array.shape, array.dtype) for array in held]
        + [pltpu.HBM(array.shape, array.dtype) for array in results],
        in_specs=[SMEM] * len(scalars)
        + [VMEM] * (len(small) + len(kept))
        + [HBM] * (len(direct) + len(large)),
        out_specs=[VMEM] * len(held) + [HBM] * len(results),
        scratch_shapes=[
            *twins,
            pltpu.SemaphoreType.DMA((len(direct) + len(large) + len(results) + 8,)),
        ],
        cost_estimate=pl.CostEstimate(flops=flops, bytes_accessed=4 * 2**20, transcendentals=0),
        compiler_params=pltpu.CompilerParams(vmem_limit_bytes=size + 12 * 2**20),
        name=name,
    )(*scalars, *small, *kept, *direct, *large)


def exchange(rows, patches):
    blocks = rows.reshape(patches, -1, rows.shape[1])
    blocks = lax.all_to_all(blocks, ("lat", "lon"), split_axis=0, concat_axis=0, tiled=True)
    return blocks.reshape(rows.shape)


def per_device(
    grid_latent,
    mesh_latent,
    grid_senders,
    grid_targets,
    grid_geometry,
    mesh_senders,
    mesh_targets,
    mesh_geometry,
    encoder_sender,
    encoder_receiver,
    encoder_geometry,
    encoder_bias,
    encoder_output,
    encoder_outbias,
    update_self,
    update_summed,
    update_bias,
    update_output,
    update_outbias,
    process_sender,
    process_receiver,
    process_geometry,
    process_bias,
    process_output,
    process_outbias,
    refine_self,
    refine_summed,
    refine_bias,
    refine_output,
    refine_outbias,
):
    number, width = mesh_latent.shape
    patches = grid_senders.shape[1]
    grid_slots = grid_targets.shape[1]
    mesh_slots = mesh_targets.shape[1]
    rows_in, columns_in = grid_latent.shape[:2]
    square = 2 * width * width
    row = lambda bias: bias.reshape(1, width)
    halves = [flat((width, width), BF16)] * 2

    cells = grid_latent.transpose(1, 0, 2).reshape(rows_in * columns_in, width)
    (packed,) = call(
        functools.partial(pack_kernel, rows_in, columns_in),
        "pack",
        1000,
        [],
        [],
        [],
        [cells],
        [flat((grid_slots, width))],
        scratch=[pltpu.SMEM((grid_slots // patches, patches), jnp.int32)],
        direct=[grid_senders[0].T],
    )
    grid_in = exchange(packed, patches)

    weights = [
        encoder_sender,
        encoder_output,
        update_summed,
        update_output,
        process_sender,
        process_output,
        refine_summed,
        refine_output,
    ]
    (
        *first,
        biases,
        received,
        self_all,
        self_sent,
        nodes_sent,
        match,
        summed_high,
        summed_low,
        update_high,
        update_low,
        sender_high,
        sender_low,
        output_high,
        output_low,
        second_high,
        second_low,
        refine_high,
        refine_low,
    ) = call(
        before_kernel,
        "before",
        (number + grid_slots) * square * 3,
        [grid_targets, mesh_senders[0].T],
        [
            grid_targets,
            grid_geometry,
            encoder_geometry,
            row(encoder_bias),
            row(update_bias),
            row(encoder_outbias),
            row(update_outbias),
        ],
        [],
        [mesh_latent, update_self, encoder_receiver] + weights,
        [
            flat((grid_slots, width)),
            flat((number, width)),
            flat((mesh_slots, width)),
            flat((mesh_slots, width)),
            flat((mesh_slots, grid_slots), BF16),
        ]
        + halves * 6,
        halves * 2 + [flat((8, width))],
        [
            pltpu.VMEM((grid_slots, width), F32),
            pltpu.VMEM((number, grid_slots), F32),
            pltpu.VMEM((mesh_slots, grid_slots), F32),
        ],
    )
    sent, parts = call(
        encode_kernel,
        "encode",
        (3 * grid_slots + mesh_slots) * square * 3,
        [],
        [],
        [grid_in, *first, biases],
        [received, summed_high, summed_low, self_sent, match, update_high, update_low, nodes_sent],
        [flat((mesh_slots, width)), flat((grid_slots, width))],
    )
    mesh_in = exchange(sent, patches)
    *first, biases, received, self_near, near, match, base = call(
        between_kernel,
        "between",
        (3 * number + mesh_slots) * square * 3,
        [mesh_targets],
        [
            grid_targets,
            mesh_targets,
            mesh_geometry,
            process_geometry,
            row(process_bias),
            row(refine_bias),
            row(update_outbias),
            row(refine_outbias),
            row(process_outbias),
        ],
        [],
        [
            parts,
            self_all,
            mesh_latent,
            update_high,
            update_low,
            refine_self,
            process_receiver,
            refine_high,
            refine_low,
        ],
        [
            flat((mesh_slots, width)),
            flat((mesh_slots, width)),
            flat((mesh_slots, width)),
            flat((mesh_slots, mesh_slots), BF16),
            flat((number, width)),
        ],
        halves * 2 + [flat((8, width))],
        [
            pltpu.VMEM((number, width), F32),
            pltpu.VMEM((number, width), F32),
            pltpu.VMEM((number, mesh_slots), F32),
            pltpu.VMEM((mesh_slots, mesh_slots), F32),
        ],
        [sender_high, sender_low, output_high, output_low],
    )
    return refine_call(
        mesh_targets, mesh_in, first, biases, received, second_high, second_low, match, self_near,
        refine_high, refine_low, near, base,
    )


def refine_call(targets, arrived, first, biases, *large):
    base = large[-1]
    number, width = base.shape
    slots = targets.shape[1]
    kept = [pltpu.with_memory_space_constraint(x, pltpu.VMEM) for x in [arrived, *first, biases]]
    large = [pltpu.with_memory_space_constraint(x, pltpu.HBM) for x in large]
    twins = [pltpu.VMEM(x.shape, x.dtype) for x in large[:-1]]
    twins += [pltpu.VMEM((number + 8, width), F32), pltpu.VMEM((slots, width), F32)]
    size = sum(4 * spec.inner_aval.size for spec in twins)
    return pl.pallas_call(
        refine_kernel,
        out_shape=flat((number, width)),
        in_specs=[SMEM] + [VMEM] * len(kept) + [HBM] * len(large),
        out_specs=HBM,
        scratch_shapes=[*twins, pltpu.SemaphoreType.DMA((len(large) + 1,))],
        compiler_params=pltpu.CompilerParams(vmem_limit_bytes=size + 12 * 2**20),
        name="refine",
    )(targets, *kept, *large)


def solution(mesh):
    patch = P(("lat", "lon"), None)
    block = P(("lat", "lon"), None, None)
    feature = P(None, ("lat", "lon"), None)
    return jax.shard_map(
        per_device,
        mesh=mesh,
        in_specs=(P("lat", "lon", None), patch, block, patch, feature, block, patch, feature)
        + (P(),) * 22,
        out_specs=patch,
        check_vma=False,
    )
```

```python
import functools

import jax
import jax.numpy as jnp
from jax import lax
from jax.experimental import pallas as pl
from jax.experimental.pallas import tpu as pltpu
from jax.sharding import PartitionSpec as P

F32 = jnp.float32
BF16 = jnp.bfloat16
VMEM = pl.BlockSpec(memory_space=pltpu.VMEM)
SMEM = pl.BlockSpec(memory_space=pltpu.SMEM)
HBM = pl.BlockSpec(memory_space=pltpu.HBM)


def split(values):
    high = values.astype(BF16)
    low = (values - high.astype(F32)).astype(BF16)
    return high, low


def dot(left, right):
    return jnp.dot(left, right, preferred_element_type=F32)


def dot3(left, high, low):
    left_high, left_low = split(left)
    return dot(left_high, high) + (dot(left_low, high) + dot(left_high, low))


def pick(one_hot, values):
    high, low = split(values)
    return dot(one_hot, high) + dot(one_hot, low)


def silu(values):
    half = 0.5 * values
    return half + half * jnp.tanh(half)


def centre(values):
    return values - jnp.mean(values, axis=-1, keepdims=True)


def scale(centred):
    return lax.rsqrt(jnp.mean(centred * centred, axis=-1, keepdims=True) + 1e-05)


def norm_centred(centred):
    return centred * scale(centred)


def gather_rows(first, count, row_of, pairs, unroll=16):
    def step(i, carry):
        row = row_of(i)
        for source, target in pairs:
            target[pl.ds(i, 1), :] = source[pl.ds(row, 1), :]
        return carry

    if count <= unroll:
        for i in range(first, first + count):
            step(i, 0)
    else:
        lax.fori_loop(first, first + count, step, 0, unroll=unroll)


def geometry_rows(geometry_ref, weight_ref):
    features, _, slots = geometry_ref.shape
    rows = jnp.concatenate([geometry_ref[k] for k in range(features)], axis=0)
    padded = jnp.concatenate([rows, jnp.zeros((8 - features % 8, slots), F32)], axis=0)
    columns = padded.T
    total = columns[:, 0:1] * weight_ref[0:1, :]
    for k in range(1, features):
        total += columns[:, k : k + 1] * weight_ref[k : k + 1, :]
    return total


def target_matrix(number, targets_ref):
    slots = targets_ref.shape[1]
    nodes = lax.broadcasted_iota(jnp.int32, (number, slots), 0)
    return jnp.where(nodes == targets_ref[...], 1.0, 0.0).astype(F32)


def slot_order(index_ref):
    capacity = index_ref.shape[0]
    bits = capacity.bit_length() - 1
    assert capacity == 1 << bits
    return lambda i: index_ref[i & (capacity - 1), i >> bits]


class Copies:
    def __init__(self, semaphores):
        self.semaphores = semaphores
        self.used = 0

    def start(self, source, target):
        copy = pltpu.make_async_copy(source, target, self.semaphores.at[self.used])
        self.used += 1
        copy.start()
        return copy


def wait(*copies):
    for copy in copies:
        copy.wait()


def started():
    pl.delay(1)


def pack_kernel(
    rows_in, columns_in, senders_ref, cells_ref, out_ref, cells, out, senders, semaphores
):
    copies = Copies(semaphores)
    load_senders = copies.start(senders_ref, senders)
    load = copies.start(cells_ref, cells)
    shift = 20
    factor = -(-(1 << shift) // columns_in)
    assert all((i * factor) >> shift == i // columns_in for i in range(rows_in * columns_in))
    order = slot_order(senders)

    def row_of(i):
        cell = order(i)
        row = (cell * factor) >> shift
        return (cell - row * columns_in) * rows_in + row

    wait(load_senders, load)
    chunk = out.shape[0] // 4
    stores = []
    for first in range(0, out.shape[0], chunk):
        gather_rows(first, chunk, row_of, [(cells, out)], 64)
        stores.append(
            copies.start(out.at[pl.ds(first, chunk)], out_ref.at[pl.ds(first, chunk)])
        )
    wait(*stores)


def before_kernel(
    grid_targets_s,
    mesh_senders_s,
    grid_targets,
    geometry,
    weight_geometry,
    edge_bias,
    node_bias,
    bias_one,
    bias_two,
    nodes_ref,
    weight_self_ref,
    weight_receiver_ref,
    *refs,
):
    count = 8
    weight_refs, refs = refs[:count], refs[count:]
    inner, refs = refs[:6], refs[6:]
    self_all_ref, self_sent_ref, nodes_sent_ref, match_ref = refs[:4]
    split_refs, refs = refs[4 : 2 * count], refs[2 * count :]
    nodes, weight_self, weight_receiver, weights, refs = *refs[:3], refs[3 : 3 + count], refs[3 + count :]
    self_all, self_sent, nodes_sent, match = refs[:4]
    splits, refs = refs[4 : 2 * count], refs[2 * count :]
    near, table, chosen, semaphores = refs
    copies = Copies(semaphores)
    load_nodes = copies.start(nodes_ref, nodes)
    load_self = copies.start(weight_self_ref, weight_self)
    load_receiver = copies.start(weight_receiver_ref, weight_receiver)
    loads = [copies.start(ref, weight) for ref, weight in zip(weight_refs, weights, strict=True)]
    started()
    received, biases = inner[4:]
    biases[0:1, :] = centre(bias_one[...])
    biases[1:2, :] = centre(bias_two[...])
    table[...] = target_matrix(nodes.shape[0], grid_targets)
    stores = []
    wait(load_nodes, load_self)
    self_all[...] = dot3(nodes[...], *split(weight_self[...])) + node_bias[...]
    stores.append(copies.start(self_all, self_all_ref))
    gather_rows(
        0,
        mesh_senders_s.shape[0] * mesh_senders_s.shape[1],
        slot_order(mesh_senders_s),
        [(nodes, nodes_sent), (self_all, self_sent), (table, chosen)],
    )
    match[...] = chosen[...].astype(BF16)
    stores.append(copies.start(self_sent, self_sent_ref))
    stores.append(copies.start(nodes_sent, nodes_sent_ref))
    stores.append(copies.start(match, match_ref))
    gather_rows(
        0, near.shape[0], lambda i: jnp.maximum(grid_targets_s[0, i], 0), [(nodes, near)]
    )
    wait(load_receiver)
    received[...] = (
        dot3(near[...], *split(weight_receiver[...]))
        + geometry_rows(geometry, weight_geometry)
        + edge_bias[...]
    )
    for k in range(count):
        wait(loads[k])
        weight = weights[k][...]
        if k % 2:
            weight = centre(weight)
        if k < 2:
            inner[2 * k][...], inner[2 * k + 1][...] = split(weight)
        else:
            at = 2 * (k - 2)
            splits[at][...], splits[at + 1][...] = split(weight)
            stores.append(copies.start(splits[at], split_refs[at]))
            stores.append(copies.start(splits[at + 1], split_refs[at + 1]))
    wait(*stores)


def edges(arrived, sender_high, sender_low, received, output_high, output_low, bias):
    hidden = silu(dot3(arrived[...], sender_high[...], sender_low[...]) + received[...])
    return dot3(hidden, output_high[...], output_low[...]) + bias


def encode_kernel(
    arrived,
    sender_high,
    sender_low,
    output_high,
    output_low,
    received,
    biases,
    summed_high_ref,
    summed_low_ref,
    match_ref,
    self_sent_ref,
    update_high_ref,
    update_low_ref,
    nodes_sent_ref,
    sent_ref,
    parts_ref,
    summed_high,
    summed_low,
    match,
    self_sent,
    update_high,
    update_low,
    nodes_sent,
    sent,
    parts,
    semaphores,
):
    copies = Copies(semaphores)
    load_summed_high = copies.start(summed_high_ref, summed_high)
    load_summed_low = copies.start(summed_low_ref, summed_low)
    load_match = copies.start(match_ref, match)
    load_self = copies.start(self_sent_ref, self_sent)
    load_update_high = copies.start(update_high_ref, update_high)
    load_update_low = copies.start(update_low_ref, update_low)
    load_nodes = copies.start(nodes_sent_ref, nodes_sent)
    started()
    rows = edges(
        arrived, sender_high, sender_low, received, output_high, output_low, biases[0:1, :]
    )
    wait(load_summed_high, load_summed_low)
    part = dot3(rows, summed_high[...], summed_low[...]) * scale(rows)
    parts[...] = part
    store_parts = copies.start(parts, parts_ref)
    wait(load_match, load_self)
    hidden = silu(self_sent[...] + pick(match[...], part))
    wait(load_update_high, load_update_low, load_nodes)
    sent[...] = nodes_sent[...] + norm_centred(
        dot3(hidden, update_high[...], update_low[...]) + biases[1:2, :]
    )
    store_sent = copies.start(sent, sent_ref)
    wait(store_parts, store_sent)


def between_kernel(
    mesh_targets_s,
    grid_targets,
    mesh_targets,
    geometry,
    weight_geometry,
    edge_bias,
    node_bias,
    update_bias,
    refine_bias,
    bias_one,
    sender_high_ref,
    sender_low_ref,
    output_high_ref,
    output_low_ref,
    parts_ref,
    self_all_ref,
    nodes_ref,
    update_high_ref,
    update_low_ref,
    weight_self_ref,
    weight_receiver_ref,
    refine_high_ref,
    refine_low_ref,
    sender_high,
    sender_low,
    output_high,
    output_low,
    received,
    biases,
    self_near_ref,
    normed_ref,
    match_ref,
    base_ref,
    firsts_ref,
    parts,
    self_all,
    nodes,
    update_high,
    update_low,
    weight_self,
    weight_receiver,
    refine_high,
    refine_low,
    self_near,
    normed_near,
    match,
    base,
    firsts,
    near,
    encoded,
    self_next,
    normed,
    table,
    chosen,
    semaphores,
):
    copies = Copies(semaphores)
    load_parts = copies.start(parts_ref, parts)
    load_all = copies.start(self_all_ref, self_all)
    load_update_high = copies.start(update_high_ref, update_high)
    load_update_low = copies.start(update_low_ref, update_low)
    load_nodes = copies.start(nodes_ref, nodes)
    load_self = copies.start(weight_self_ref, weight_self)
    load_receiver = copies.start(weight_receiver_ref, weight_receiver)
    load_refine_high = copies.start(refine_high_ref, refine_high)
    load_refine_low = copies.start(refine_low_ref, refine_low)
    passed = [
        copies.start(sender_high_ref, sender_high),
        copies.start(sender_low_ref, sender_low),
        copies.start(output_high_ref, output_high),
        copies.start(output_low_ref, output_low),
    ]
    started()
    stores = []
    biases[0:1, :] = centre(bias_one[...])
    biases[1:2, :] = centre(refine_bias[...])
    one_hot = target_matrix(nodes.shape[0], grid_targets).astype(BF16)
    table[...] = target_matrix(table.shape[0], mesh_targets)
    number = nodes.shape[0]

    def node_or_empty(i):
        target = mesh_targets_s[0, i]
        return jnp.where(target < 0, number, target)

    wait(load_parts, load_all)
    hidden = silu(self_all[...] + pick(one_hot, parts[...]))
    wait(load_update_high, load_update_low, load_nodes)
    encoded[...] = nodes[...] + norm_centred(
        dot3(hidden, update_high[...], update_low[...]) + centre(update_bias[...])
    )
    wait(load_self)
    self_next[...] = dot3(encoded[...], *split(weight_self[...])) + node_bias[...]
    wait(load_refine_high, load_refine_low)
    normed[...] = norm_centred(
        dot3(silu(self_next[...]), refine_high[...], refine_low[...]) + centre(refine_bias[...])
    )
    base[...] = encoded[...] + normed[...]
    stores.append(copies.start(base, base_ref))
    gather_rows(
        0,
        near.shape[0],
        lambda i: jnp.maximum(mesh_targets_s[0, i], 0),
        [(encoded, near), (self_next, self_near), (normed, normed_near)],
    )
    gather_rows(0, near.shape[0], node_or_empty, [(table, chosen)])
    slots = near.shape[0]
    same = chosen[...]
    match[...] = same.astype(BF16)
    earlier = lax.broadcasted_iota(jnp.int32, (slots, slots), 0) < lax.broadcasted_iota(
        jnp.int32, (slots, slots), 1
    )
    repeats = jnp.sum(jnp.where(earlier, same, 0.0), axis=0, keepdims=True)
    firsts[...] = jnp.where(repeats == 0.0, table[0:number, :], 0.0).astype(BF16)
    stores.append(copies.start(self_near, self_near_ref))
    stores.append(copies.start(normed_near, normed_ref))
    stores.append(copies.start(match, match_ref))
    stores.append(copies.start(firsts, firsts_ref))
    wait(load_receiver)
    received[...] = (
        dot3(near[...], *split(weight_receiver[...]))
        + geometry_rows(geometry, weight_geometry)
        + edge_bias[...]
    )
    wait(*passed, *stores)


def refine_kernel(
    arrived,
    sender_high,
    sender_low,
    output_high,
    output_low,
    received,
    biases,
    summed_high_ref,
    summed_low_ref,
    match_ref,
    self_near_ref,
    refine_high_ref,
    refine_low_ref,
    normed_ref,
    firsts_ref,
    base_ref,
    out_ref,
    summed_high,
    summed_low,
    match,
    self_near,
    refine_high,
    refine_low,
    normed,
    firsts,
    base,
    out,
    semaphores,
):
    copies = Copies(semaphores)
    load_summed_high = copies.start(summed_high_ref, summed_high)
    load_summed_low = copies.start(summed_low_ref, summed_low)
    load_match = copies.start(match_ref, match)
    load_self = copies.start(self_near_ref, self_near)
    load_refine_high = copies.start(refine_high_ref, refine_high)
    load_refine_low = copies.start(refine_low_ref, refine_low)
    load_normed = copies.start(normed_ref, normed)
    load_firsts = copies.start(firsts_ref, firsts)
    load_base = copies.start(base_ref, base)
    started()
    rows = edges(
        arrived, sender_high, sender_low, received, output_high, output_low, biases[0:1, :]
    )
    wait(load_summed_high, load_summed_low)
    part = dot3(rows, summed_high[...], summed_low[...]) * scale(rows)
    wait(load_match, load_self)
    hidden = silu(self_near[...] + pick(match[...], part))
    wait(load_refine_high, load_refine_low, load_normed)
    change = norm_centred(dot3(hidden, refine_high[...], refine_low[...]) + biases[1:2, :])
    high, low = split(change - normed[...])
    wait(load_firsts, load_base)
    number = out.shape[0]
    chunk = number // 2
    stores = []
    for first in range(0, number, chunk):
        at = pl.ds(first, chunk)
        out[at, :] = base[at, :] + (dot(firsts[at, :], high) + dot(firsts[at, :], low))
        stores.append(copies.start(out.at[at], out_ref.at[at]))
        if first + chunk < number:
            started()
    wait(*stores)


def flat(dims, kind=F32):
    return jax.ShapeDtypeStruct(dims, kind)


def call(
    kernel, name, flops, scalars, small, kept, large, results, held=(), scratch=(), direct=()
):
    direct = [pltpu.with_memory_space_constraint(array, pltpu.HBM) for array in direct]
    kept = [pltpu.with_memory_space_constraint(array, pltpu.VMEM) for array in kept]
    large = [pltpu.with_memory_space_constraint(array, pltpu.HBM) for array in large]
    twins = [pltpu.VMEM(array.shape, array.dtype) for array in [*large, *results]]
    twins += list(scratch)
    size = sum(4 * spec.inner_aval.size for spec in twins)
    return pl.pallas_call(
        kernel,
        out_shape=[pltpu.VMEM(array.shape, array.dtype) for array in held]
        + [pltpu.HBM(array.shape, array.dtype) for array in results],
        in_specs=[SMEM] * len(scalars)
        + [VMEM] * (len(small) + len(kept))
        + [HBM] * (len(direct) + len(large)),
        out_specs=[VMEM] * len(held) + [HBM] * len(results),
        scratch_shapes=[
            *twins,
            pltpu.SemaphoreType.DMA((len(direct) + len(large) + len(results) + 8,)),
        ],
        cost_estimate=pl.CostEstimate(flops=flops, bytes_accessed=4 * 2**20, transcendentals=0),
        compiler_params=pltpu.CompilerParams(vmem_limit_bytes=size + 12 * 2**20),
        name=name,
    )(*scalars, *small, *kept, *direct, *large)


def exchange(rows, patches):
    blocks = rows.reshape(patches, -1, rows.shape[1])
    blocks = lax.all_to_all(blocks, ("lat", "lon"), split_axis=0, concat_axis=0, tiled=True)
    return blocks.reshape(rows.shape)


def per_device(
    grid_latent,
    mesh_latent,
    grid_senders,
    grid_targets,
    grid_geometry,
    mesh_senders,
    mesh_targets,
    mesh_geometry,
    encoder_sender,
    encoder_receiver,
    encoder_geometry,
    encoder_bias,
    encoder_output,
    encoder_outbias,
    update_self,
    update_summed,
    update_bias,
    update_output,
    update_outbias,
    process_sender,
    process_receiver,
    process_geometry,
    process_bias,
    process_output,
    process_outbias,
    refine_self,
    refine_summed,
    refine_bias,
    refine_output,
    refine_outbias,
):
    number, width = mesh_latent.shape
    patches = grid_senders.shape[1]
    grid_slots = grid_targets.shape[1]
    mesh_slots = mesh_targets.shape[1]
    rows_in, columns_in = grid_latent.shape[:2]
    square = 2 * width * width
    row = lambda bias: bias.reshape(1, width)
    halves = [flat((width, width), BF16)] * 2

    cells = grid_latent.transpose(1, 0, 2).reshape(rows_in * columns_in, width)
    (packed,) = call(
        functools.partial(pack_kernel, rows_in, columns_in),
        "pack",
        1000,
        [],
        [],
        [],
        [cells],
        [flat((grid_slots, width))],
        scratch=[pltpu.SMEM((grid_slots // patches, patches), jnp.int32)],
        direct=[grid_senders[0].T],
    )
    grid_in = exchange(packed, patches)

    weights = [
        encoder_sender,
        encoder_output,
        update_summed,
        update_output,
        process_sender,
        process_output,
        refine_summed,
        refine_output,
    ]
    (
        *first,
        self_all,
        self_sent,
        nodes_sent,
        match,
        summed_high,
        summed_low,
        update_high,
        update_low,
        sender_high,
        sender_low,
        output_high,
        output_low,
        second_high,
        second_low,
        refine_high,
        refine_low,
    ) = call(
        before_kernel,
        "before",
        (number + grid_slots) * square * 3,
        [grid_targets, mesh_senders[0].T],
        [
            grid_targets,
            grid_geometry,
            encoder_geometry,
            row(encoder_bias),
            row(update_bias),
            row(encoder_outbias),
            row(update_outbias),
        ],
        [],
        [mesh_latent, update_self, encoder_receiver] + weights,
        [
            flat((number, width)),
            flat((mesh_slots, width)),
            flat((mesh_slots, width)),
            flat((mesh_slots, grid_slots), BF16),
        ]
        + halves * 6,
        halves * 2 + [flat((grid_slots, width)), flat((8, width))],
        [
            pltpu.VMEM((grid_slots, width), F32),
            pltpu.VMEM((number, grid_slots), F32),
            pltpu.VMEM((mesh_slots, grid_slots), F32),
        ],
    )
    sent, parts = call(
        encode_kernel,
        "encode",
        (3 * grid_slots + mesh_slots) * square * 3,
        [],
        [],
        [grid_in, *first],
        [summed_high, summed_low, match, self_sent, update_high, update_low, nodes_sent],
        [flat((mesh_slots, width)), flat((grid_slots, width))],
    )
    mesh_in = exchange(sent, patches)
    *first, self_near, normed, match, base, firsts = call(
        between_kernel,
        "between",
        (3 * number + mesh_slots) * square * 3,
        [mesh_targets],
        [
            grid_targets,
            mesh_targets,
            mesh_geometry,
            process_geometry,
            row(process_bias),
            row(refine_bias),
            row(update_outbias),
            row(refine_outbias),
            row(process_outbias),
        ],
        [],
        [
            parts,
            self_all,
            mesh_latent,
            update_high,
            update_low,
            refine_self,
            process_receiver,
            refine_high,
            refine_low,
        ],
        [
            flat((mesh_slots, width)),
            flat((mesh_slots, width)),
            flat((mesh_slots, mesh_slots), BF16),
            flat((number, width)),
            flat((number, mesh_slots), BF16),
        ],
        halves * 2 + [flat((mesh_slots, width)), flat((8, width))],
        [
            pltpu.VMEM((mesh_slots, width), F32),
            pltpu.VMEM((number, width), F32),
            pltpu.VMEM((number, width), F32),
            pltpu.VMEM((number, width), F32),
            pltpu.VMEM((number + 8, mesh_slots), F32),
            pltpu.VMEM((mesh_slots, mesh_slots), F32),
        ],
        [sender_high, sender_low, output_high, output_low],
    )
    (out,) = call(
        refine_kernel,
        "refine",
        4 * mesh_slots * square * 3,
        [],
        [],
        [mesh_in, *first],
        [
            second_high,
            second_low,
            match,
            self_near,
            refine_high,
            refine_low,
            normed,
            firsts,
            base,
        ],
        [flat((number, width))],
    )
    return out


def solution(mesh):
    patch = P(("lat", "lon"), None)
    block = P(("lat", "lon"), None, None)
    feature = P(None, ("lat", "lon"), None)
    return jax.shard_map(
        per_device,
        mesh=mesh,
        in_specs=(P("lat", "lon", None), patch, block, patch, feature, block, patch, feature)
        + (P(),) * 22,
        out_specs=patch,
        check_vma=False,
    )
```

```python
import functools

import jax
import jax.numpy as jnp
from jax import lax
from jax.experimental import pallas as pl
from jax.experimental.pallas import tpu as pltpu
from jax.sharding import PartitionSpec as P

F32 = jnp.float32
BF16 = jnp.bfloat16
VMEM = pl.BlockSpec(memory_space=pltpu.VMEM)
SMEM = pl.BlockSpec(memory_space=pltpu.SMEM)
HBM = pl.BlockSpec(memory_space=pltpu.HBM)


def split(values):
    high = values.astype(BF16)
    low = (values - high.astype(F32)).astype(BF16)
    return high, low


def dot(left, right):
    return jnp.dot(left, right, preferred_element_type=F32)


def dot3(left, high, low):
    left_high, left_low = split(left)
    return dot(left_high, high) + (dot(left_low, high) + dot(left_high, low))


def pick(one_hot, values):
    high, low = split(values)
    return dot(one_hot, high) + dot(one_hot, low)


def silu(values):
    half = 0.5 * values
    return half + half * jnp.tanh(half)


def centre(values):
    return values - jnp.mean(values, axis=-1, keepdims=True)


def scale(centred):
    return lax.rsqrt(jnp.mean(centred * centred, axis=-1, keepdims=True) + 1e-05)


def norm_centred(centred):
    return centred * scale(centred)


def gather_rows(first, count, row_of, pairs, unroll=16):
    def step(i, carry):
        row = row_of(i)
        for source, target in pairs:
            target[pl.ds(i, 1), :] = source[pl.ds(row, 1), :]
        return carry

    if count <= 256:
        for i in range(first, first + count):
            step(i, 0)
    else:
        lax.fori_loop(first, first + count, step, 0, unroll=unroll)


def geometry_rows(geometry_ref, weight_ref):
    features, _, slots = geometry_ref.shape
    rows = jnp.concatenate([geometry_ref[k] for k in range(features)], axis=0)
    padded = jnp.concatenate([rows, jnp.zeros((8 - features % 8, slots), F32)], axis=0)
    columns = padded.T
    total = columns[:, 0:1] * weight_ref[0:1, :]
    for k in range(1, features):
        total += columns[:, k : k + 1] * weight_ref[k : k + 1, :]
    return total


def target_matrix(number, targets_ref):
    slots = targets_ref.shape[1]
    nodes = lax.broadcasted_iota(jnp.int32, (number, slots), 0)
    return jnp.where(nodes == targets_ref[...], 1.0, 0.0).astype(F32)


def slot_order(index_ref):
    capacity = index_ref.shape[0]
    bits = capacity.bit_length() - 1
    assert capacity == 1 << bits
    return lambda i: index_ref[i & (capacity - 1), i >> bits]


class Copies:
    def __init__(self, semaphores):
        self.semaphores = semaphores
        self.used = 0

    def start(self, source, target):
        copy = pltpu.make_async_copy(source, target, self.semaphores.at[self.used])
        self.used += 1
        copy.start()
        return copy


def wait(*copies):
    for copy in copies:
        copy.wait()


def started():
    pl.delay(1)


def pack_kernel(
    rows_in, columns_in, senders_ref, cells_ref, out_ref, cells, out, senders, semaphores
):
    copies = Copies(semaphores)
    load_senders = copies.start(senders_ref, senders)
    load = copies.start(cells_ref, cells)
    shift = 20
    factor = -(-(1 << shift) // columns_in)
    assert all((i * factor) >> shift == i // columns_in for i in range(rows_in * columns_in))
    order = slot_order(senders)

    def row_of(i):
        cell = order(i)
        row = (cell * factor) >> shift
        return (cell - row * columns_in) * rows_in + row

    wait(load_senders, load)
    chunk = out.shape[0] // 4
    stores = []
    for first in range(0, out.shape[0], chunk):
        gather_rows(first, chunk, row_of, [(cells, out)])
        stores.append(
            copies.start(out.at[pl.ds(first, chunk)], out_ref.at[pl.ds(first, chunk)])
        )
    wait(*stores)


def rows_of(*biases):
    width = biases[0].shape[1]
    return jnp.concatenate([*biases, jnp.zeros((8 - len(biases), width), F32)], axis=0)


def before_kernel(
    grid_targets_s,
    mesh_senders_s,
    grid_targets,
    geometry,
    weight_geometry,
    edge_bias,
    node_bias,
    output_bias,
    update_bias,
    output_bias_2,
    refine_bias,
    nodes_ref,
    weight_self_ref,
    weight_receiver_ref,
    output_ref,
    summed_ref,
    sender_ref,
    update_ref,
    sender_ref_2,
    output_ref_2,
    summed_ref_2,
    refine_ref,
    sender_high,
    sender_low,
    merged_high,
    merged_low,
    received,
    biases,
    self_all_ref,
    self_sent_ref,
    nodes_sent_ref,
    match_ref,
    output_high_ref,
    onward_high_ref,
    onward_low_ref,
    update_high_ref,
    update_low_ref,
    merged_high_ref_2,
    merged_low_ref_2,
    output_high_ref_2,
    refine_high_ref,
    refine_low_ref,
    biases_ref_2,
    nodes,
    weight_self,
    weight_receiver,
    output,
    summed,
    sender,
    update,
    sender_2,
    output_2,
    summed_2,
    refine,
    self_all,
    self_sent,
    nodes_sent,
    match,
    output_high,
    onward_high,
    onward_low,
    update_high,
    update_low,
    merged_high_2,
    merged_low_2,
    output_high_2,
    refine_high,
    refine_low,
    biases_2,
    near,
    picked,
    table,
    chosen,
    semaphores,
):
    copies = Copies(semaphores)
    load_nodes = copies.start(nodes_ref, nodes)
    load_self = copies.start(weight_self_ref, weight_self)
    load_output = copies.start(output_ref, output)
    load_summed = copies.start(summed_ref, summed)
    load_receiver = copies.start(weight_receiver_ref, weight_receiver)
    load_sender = copies.start(sender_ref, sender)
    load_update = copies.start(update_ref, update)
    load_sender_2 = copies.start(sender_ref_2, sender_2)
    load_output_2 = copies.start(output_ref_2, output_2)
    load_summed_2 = copies.start(summed_ref_2, summed_2)
    load_refine = copies.start(refine_ref, refine)
    started()
    stores = []

    def store(*pairs):
        stores.extend(copies.start(source, target) for source, target in pairs)

    table[...] = target_matrix(nodes.shape[0], grid_targets)
    wait(load_nodes, load_self)
    self_all[...] = dot3(nodes[...], *split(weight_self[...])) + node_bias[...]
    store((self_all, self_all_ref))
    gather_rows(
        0,
        picked.shape[0],
        slot_order(mesh_senders_s),
        [(nodes, picked), (self_all, self_sent), (table, chosen)],
    )
    match[...] = chosen[...].astype(BF16)
    store((self_sent, self_sent_ref), (match, match_ref))
    wait(load_output, load_summed)
    centred = centre(output[...])
    high, low = split(summed[...])
    merged_high[...], merged_low[...] = split(dot3(centred, high, low))
    output_high[...] = centred.astype(BF16)
    store((output_high, output_high_ref))
    first_bias = centre(output_bias[...])
    first_bias_on = dot3(rows_of(first_bias), high, low)[0:1, :]
    gather_rows(
        0, near.shape[0], lambda i: jnp.maximum(grid_targets_s[0, i], 0), [(nodes, near)]
    )
    wait(load_receiver)
    received[...] = (
        dot3(near[...], *split(weight_receiver[...]))
        + geometry_rows(geometry, weight_geometry)
        + edge_bias[...]
    )
    wait(load_sender)
    sender_high[...], sender_low[...] = split(sender[...])
    wait(load_update, load_sender_2)
    centred = centre(update[...])
    update_high[...], update_low[...] = split(centred)
    high, low = split(sender_2[...])
    onward_high[...], onward_low[...] = split(dot3(centred, high, low))
    nodes_sent[...] = dot3(picked[...], high, low)
    store(
        (update_high, update_high_ref),
        (update_low, update_low_ref),
        (onward_high, onward_high_ref),
        (onward_low, onward_low_ref),
        (nodes_sent, nodes_sent_ref),
    )
    second_bias = centre(update_bias[...])
    second_bias_on = dot3(rows_of(second_bias), high, low)[0:1, :]
    biases[...] = rows_of(first_bias, first_bias_on, second_bias, second_bias_on)
    wait(load_output_2, load_summed_2, load_refine)
    centred = centre(output_2[...])
    high, low = split(summed_2[...])
    merged_high_2[...], merged_low_2[...] = split(dot3(centred, high, low))
    output_high_2[...] = centred.astype(BF16)
    third_bias = centre(output_bias_2[...])
    third_bias_on = dot3(rows_of(third_bias), high, low)[0:1, :]
    biases_2[...] = rows_of(third_bias, third_bias_on, centre(refine_bias[...]))
    refine_high[...], refine_low[...] = split(centre(refine[...]))
    store(
        (merged_high_2, merged_high_ref_2),
        (merged_low_2, merged_low_ref_2),
        (output_high_2, output_high_ref_2),
        (refine_high, refine_high_ref),
        (refine_low, refine_low_ref),
        (biases_2, biases_ref_2),
    )
    wait(*stores)


def edges(hidden, merged_high, merged_low, output_high, bias, bias_on):
    hidden_high, hidden_low = split(hidden)
    high = merged_high[...]
    total = dot(hidden_high, high) + (
        dot(hidden_low, high) + dot(hidden_high, merged_low[...])
    )
    return (total + bias_on) * scale(dot(hidden_high, output_high[...]) + bias)


def encode_kernel(
    arrived,
    sender_high,
    sender_low,
    merged_high,
    merged_low,
    received,
    biases,
    output_high_ref,
    match_ref,
    self_sent_ref,
    onward_high_ref,
    onward_low_ref,
    update_high_ref,
    nodes_sent_ref,
    sent_ref,
    parts_ref,
    output_high,
    match,
    self_sent,
    onward_high,
    onward_low,
    update_high,
    nodes_sent,
    sent,
    parts,
    semaphores,
):
    copies = Copies(semaphores)
    load_output = copies.start(output_high_ref, output_high)
    load_match = copies.start(match_ref, match)
    load_self = copies.start(self_sent_ref, self_sent)
    load_onward_high = copies.start(onward_high_ref, onward_high)
    load_onward_low = copies.start(onward_low_ref, onward_low)
    load_update = copies.start(update_high_ref, update_high)
    load_nodes = copies.start(nodes_sent_ref, nodes_sent)
    started()
    hidden = silu(dot3(arrived[...], sender_high[...], sender_low[...]) + received[...])
    wait(load_output)
    part = edges(
        hidden, merged_high, merged_low, output_high, biases[0:1, :], biases[1:2, :]
    )
    parts[...] = part
    store_parts = copies.start(parts, parts_ref)
    wait(load_match, load_self)
    hidden = silu(self_sent[...] + pick(match[...], part))
    wait(load_onward_high, load_onward_low, load_update, load_nodes)
    sent[...] = nodes_sent[...] + edges(
        hidden, onward_high, onward_low, update_high, biases[2:3, :], biases[3:4, :]
    )
    store_sent = copies.start(sent, sent_ref)
    wait(store_parts, store_sent)


def between_kernel(
    mesh_targets_s,
    grid_targets,
    mesh_targets,
    geometry,
    weight_geometry,
    edge_bias,
    node_bias,
    update_bias,
    refine_bias,
    merged_high_ref,
    merged_low_ref,
    output_high_ref,
    biases_ref,
    parts_ref,
    self_all_ref,
    nodes_ref,
    update_high_ref,
    update_low_ref,
    weight_self_ref,
    weight_receiver_ref,
    refine_high_ref,
    refine_low_ref,
    merged_high,
    merged_low,
    output_high,
    received,
    self_near,
    match,
    biases,
    normed_ref,
    base_ref,
    firsts_ref,
    parts,
    self_all,
    nodes,
    update_high,
    update_low,
    weight_self,
    weight_receiver,
    refine_high,
    refine_low,
    normed_near,
    base,
    firsts,
    near,
    encoded,
    self_next,
    normed,
    table,
    chosen,
    semaphores,
):
    copies = Copies(semaphores)
    load_parts = copies.start(parts_ref, parts)
    load_all = copies.start(self_all_ref, self_all)
    load_update_high = copies.start(update_high_ref, update_high)
    load_update_low = copies.start(update_low_ref, update_low)
    load_nodes = copies.start(nodes_ref, nodes)
    load_self = copies.start(weight_self_ref, weight_self)
    load_receiver = copies.start(weight_receiver_ref, weight_receiver)
    load_refine_high = copies.start(refine_high_ref, refine_high)
    load_refine_low = copies.start(refine_low_ref, refine_low)
    passed = [
        copies.start(merged_high_ref, merged_high),
        copies.start(merged_low_ref, merged_low),
        copies.start(output_high_ref, output_high),
        copies.start(biases_ref, biases),
    ]
    started()
    stores = []
    one_hot = target_matrix(nodes.shape[0], grid_targets).astype(BF16)
    table[...] = target_matrix(table.shape[0], mesh_targets)
    number = nodes.shape[0]

    def node_or_empty(i):
        target = mesh_targets_s[0, i]
        return jnp.where(target < 0, number, target)

    wait(load_parts, load_all)
    hidden = silu(self_all[...] + pick(one_hot, parts[...]))
    wait(load_update_high, load_update_low, load_nodes)
    encoded[...] = nodes[...] + norm_centred(
        dot3(hidden, update_high[...], update_low[...]) + centre(update_bias[...])
    )
    wait(load_self)
    self_next[...] = dot3(encoded[...], *split(weight_self[...])) + node_bias[...]
    wait(load_refine_high, load_refine_low)
    normed[...] = norm_centred(
        dot3(silu(self_next[...]), refine_high[...], refine_low[...]) + centre(refine_bias[...])
    )
    base[...] = encoded[...] + normed[...]
    stores.append(copies.start(base, base_ref))
    gather_rows(
        0,
        near.shape[0],
        lambda i: jnp.maximum(mesh_targets_s[0, i], 0),
        [(encoded, near), (self_next, self_near), (normed, normed_near)],
    )
    gather_rows(0, near.shape[0], node_or_empty, [(table, chosen)])
    slots = near.shape[0]
    same = chosen[...]
    match[...] = same.astype(BF16)
    earlier = lax.broadcasted_iota(jnp.int32, (slots, slots), 0) < lax.broadcasted_iota(
        jnp.int32, (slots, slots), 1
    )
    repeats = jnp.sum(jnp.where(earlier, same, 0.0), axis=0, keepdims=True)
    firsts[...] = jnp.where(repeats == 0.0, table[0:number, :], 0.0).astype(BF16)
    stores.append(copies.start(normed_near, normed_ref))
    stores.append(copies.start(firsts, firsts_ref))
    wait(load_receiver)
    received[...] = (
        dot3(near[...], *split(weight_receiver[...]))
        + geometry_rows(geometry, weight_geometry)
        + edge_bias[...]
    )
    wait(*passed, *stores)


def refine_kernel(
    arrived,
    merged_high,
    merged_low,
    output_high,
    received,
    self_near,
    match,
    biases,
    refine_high_ref,
    refine_low_ref,
    normed_ref,
    firsts_ref,
    base_ref,
    out_ref,
    refine_high,
    refine_low,
    normed,
    firsts,
    base,
    out,
    semaphores,
):
    copies = Copies(semaphores)
    load_refine_high = copies.start(refine_high_ref, refine_high)
    load_refine_low = copies.start(refine_low_ref, refine_low)
    load_normed = copies.start(normed_ref, normed)
    load_firsts = copies.start(firsts_ref, firsts)
    load_base = copies.start(base_ref, base)
    started()
    part = edges(
        silu(arrived[...] + received[...]),
        merged_high,
        merged_low,
        output_high,
        biases[0:1, :],
        biases[1:2, :],
    )
    hidden = silu(self_near[...] + pick(match[...], part))
    wait(load_refine_high, load_refine_low, load_normed)
    change = norm_centred(dot3(hidden, refine_high[...], refine_low[...]) + biases[2:3, :])
    high, low = split(change - normed[...])
    wait(load_firsts, load_base)
    number = out.shape[0]
    chunk = number // 2
    stores = []
    for first in range(0, number, chunk):
        at = pl.ds(first, chunk)
        out[at, :] = base[at, :] + (dot(firsts[at, :], high) + dot(firsts[at, :], low))
        stores.append(copies.start(out.at[at], out_ref.at[at]))
        if first + chunk < number:
            started()
    wait(*stores)


def flat(dims, kind=F32):
    return jax.ShapeDtypeStruct(dims, kind)


def call(
    kernel, name, flops, scalars, small, kept, large, results, held=(), scratch=(), direct=()
):
    direct = [pltpu.with_memory_space_constraint(array, pltpu.HBM) for array in direct]
    kept = [pltpu.with_memory_space_constraint(array, pltpu.VMEM) for array in kept]
    large = [pltpu.with_memory_space_constraint(array, pltpu.HBM) for array in large]
    twins = [pltpu.VMEM(array.shape, array.dtype) for array in [*large, *results]]
    twins += list(scratch)
    size = sum(4 * spec.inner_aval.size for spec in twins)
    return pl.pallas_call(
        kernel,
        out_shape=[pltpu.VMEM(array.shape, array.dtype) for array in held]
        + [pltpu.HBM(array.shape, array.dtype) for array in results],
        in_specs=[SMEM] * len(scalars)
        + [VMEM] * (len(small) + len(kept))
        + [HBM] * (len(direct) + len(large)),
        out_specs=[VMEM] * len(held) + [HBM] * len(results),
        scratch_shapes=[
            *twins,
            pltpu.SemaphoreType.DMA((len(direct) + len(large) + len(results) + 8,)),
        ],
        cost_estimate=pl.CostEstimate(flops=flops, bytes_accessed=4 * 2**20, transcendentals=0),
        compiler_params=pltpu.CompilerParams(vmem_limit_bytes=size + 12 * 2**20),
        name=name,
    )(*scalars, *small, *kept, *direct, *large)


def exchange(rows, patches):
    blocks = rows.reshape(patches, -1, rows.shape[1])
    blocks = lax.all_to_all(blocks, ("lat", "lon"), split_axis=0, concat_axis=0, tiled=True)
    return blocks.reshape(rows.shape)


def per_device(
    grid_latent,
    mesh_latent,
    grid_senders,
    grid_targets,
    grid_geometry,
    mesh_senders,
    mesh_targets,
    mesh_geometry,
    encoder_sender,
    encoder_receiver,
    encoder_geometry,
    encoder_bias,
    encoder_output,
    encoder_outbias,
    update_self,
    update_summed,
    update_bias,
    update_output,
    update_outbias,
    process_sender,
    process_receiver,
    process_geometry,
    process_bias,
    process_output,
    process_outbias,
    refine_self,
    refine_summed,
    refine_bias,
    refine_output,
    refine_outbias,
):
    number, width = mesh_latent.shape
    patches = grid_senders.shape[1]
    grid_slots = grid_targets.shape[1]
    mesh_slots = mesh_targets.shape[1]
    rows_in, columns_in = grid_latent.shape[:2]
    square = 2 * width * width
    row = lambda bias: bias.reshape(1, width)
    halves = [flat((width, width), BF16)] * 2

    cells = grid_latent.transpose(1, 0, 2).reshape(rows_in * columns_in, width)
    (packed,) = call(
        functools.partial(pack_kernel, rows_in, columns_in),
        "pack",
        1000,
        [],
        [],
        [],
        [cells],
        [flat((grid_slots, width))],
        scratch=[pltpu.SMEM((grid_slots // patches, patches), jnp.int32)],
        direct=[grid_senders[0].T],
    )
    grid_in = exchange(packed, patches)

    (
        *first,
        self_all,
        self_sent,
        nodes_sent,
        match,
        output_high,
        onward_high,
        onward_low,
        update_high,
        update_low,
        merged_high,
        merged_low,
        second_high,
        refine_high,
        refine_low,
        biases,
    ) = call(
        before_kernel,
        "before",
        (number + grid_slots) * square * 3,
        [grid_targets, mesh_senders[0].T],
        [
            grid_targets,
            grid_geometry,
            encoder_geometry,
            row(encoder_bias),
            row(update_bias),
            row(encoder_outbias),
            row(update_outbias),
            row(process_outbias),
            row(refine_outbias),
        ],
        [],
        [
            mesh_latent,
            update_self,
            encoder_receiver,
            encoder_output,
            update_summed,
            encoder_sender,
            update_output,
            process_sender,
            process_output,
            refine_summed,
            refine_output,
        ],
        [
            flat((number, width)),
            flat((mesh_slots, width)),
            flat((mesh_slots, width)),
            flat((mesh_slots, grid_slots), BF16),
        ]
        + halves * 5
        + [flat((8, width))],
        halves * 2 + [flat((grid_slots, width)), flat((8, width))],
        [
            pltpu.VMEM((grid_slots, width), F32),
            pltpu.VMEM((mesh_slots, width), F32),
            pltpu.VMEM((number, grid_slots), F32),
            pltpu.VMEM((mesh_slots, grid_slots), F32),
        ],
    )
    sent, parts = call(
        encode_kernel,
        "encode",
        (3 * grid_slots + mesh_slots) * square * 3,
        [],
        [],
        [grid_in, *first],
        [output_high, match, self_sent, onward_high, onward_low, update_high, nodes_sent],
        [flat((mesh_slots, width)), flat((grid_slots, width))],
    )
    mesh_in = exchange(sent, patches)
    *first, normed, base, firsts = call(
        between_kernel,
        "between",
        (3 * number + mesh_slots) * square * 3,
        [mesh_targets],
        [
            grid_targets,
            mesh_targets,
            mesh_geometry,
            process_geometry,
            row(process_bias),
            row(refine_bias),
            row(update_outbias),
            row(refine_outbias),
        ],
        [],
        [
            parts,
            self_all,
            mesh_latent,
            update_high,
            update_low,
            refine_self,
            process_receiver,
            refine_high,
            refine_low,
        ],
        [
            flat((mesh_slots, width)),
            flat((number, width)),
            flat((number, mesh_slots), BF16),
        ],
        [
            *halves,
            halves[0],
            flat((mesh_slots, width)),
            flat((mesh_slots, width)),
            flat((mesh_slots, mesh_slots), BF16),
            flat((8, width)),
        ],
        [
            pltpu.VMEM((mesh_slots, width), F32),
            pltpu.VMEM((number, width), F32),
            pltpu.VMEM((number, width), F32),
            pltpu.VMEM((number, width), F32),
            pltpu.VMEM((number + 8, mesh_slots), F32),
            pltpu.VMEM((mesh_slots, mesh_slots), F32),
        ],
        [merged_high, merged_low, second_high, biases],
    )
    (out,) = call(
        refine_kernel,
        "refine",
        4 * mesh_slots * square * 3,
        [],
        [],
        [mesh_in, *first],
        [
            refine_high,
            refine_low,
            normed,
            firsts,
            base,
        ],
        [flat((number, width))],
    )
    return out


def solution(mesh):
    patch = P(("lat", "lon"), None)
    block = P(("lat", "lon"), None, None)
    feature = P(None, ("lat", "lon"), None)
    return jax.shard_map(
        per_device,
        mesh=mesh,
        in_specs=(P("lat", "lon", None), patch, block, patch, feature, block, patch, feature)
        + (P(),) * 22,
        out_specs=patch,
        check_vma=False,
    )
```

```python
import functools

import jax
import jax.numpy as jnp
from jax import lax
from jax.experimental import pallas as pl
from jax.experimental.pallas import tpu as pltpu
from jax.sharding import PartitionSpec as P

F32 = jnp.float32
BF16 = jnp.bfloat16
VMEM = pl.BlockSpec(memory_space=pltpu.VMEM)
SMEM = pl.BlockSpec(memory_space=pltpu.SMEM)
HBM = pl.BlockSpec(memory_space=pltpu.HBM)


def split(values):
    high = values.astype(BF16)
    low = (values - high.astype(F32)).astype(BF16)
    return high, low


def dot(left, right):
    return jnp.dot(left, right, preferred_element_type=F32)


def dot3(left, high, low):
    left_high, left_low = split(left)
    return dot(left_high, high) + (dot(left_low, high) + dot(left_high, low))


def pick(one_hot, values):
    high, low = split(values)
    return dot(one_hot, high) + dot(one_hot, low)


def silu(values):
    half = 0.5 * values
    return half + half * jnp.tanh(half)


def centre(values):
    return values - jnp.mean(values, axis=-1, keepdims=True)


def scale(centred):
    return lax.rsqrt(jnp.mean(centred * centred, axis=-1, keepdims=True) + 1e-05)


def norm_centred(centred):
    return centred * scale(centred)


def gather_rows(first, count, row_of, pairs, unroll=16):
    def step(i, carry):
        row = row_of(i)
        for source, target in pairs:
            target[pl.ds(i, 1), :] = source[pl.ds(row, 1), :]
        return carry

    if count <= 256:
        for i in range(first, first + count):
            step(i, 0)
    else:
        lax.fori_loop(first, first + count, step, 0, unroll=unroll)


def geometry_rows(geometry_ref, weight_ref):
    features, _, slots = geometry_ref.shape
    rows = jnp.concatenate([geometry_ref[k] for k in range(features)], axis=0)
    padded = jnp.concatenate([rows, jnp.zeros((8 - features % 8, slots), F32)], axis=0)
    columns = padded.T
    total = columns[:, 0:1] * weight_ref[0:1, :]
    for k in range(1, features):
        total += columns[:, k : k + 1] * weight_ref[k : k + 1, :]
    return total


def target_matrix(number, targets_ref):
    slots = targets_ref.shape[1]
    nodes = lax.broadcasted_iota(jnp.int32, (number, slots), 0)
    return jnp.where(nodes == targets_ref[...], 1.0, 0.0).astype(F32)


def slot_order(index_ref):
    capacity = index_ref.shape[0]
    bits = capacity.bit_length() - 1
    assert capacity == 1 << bits
    return lambda i: index_ref[i & (capacity - 1), i >> bits]


class Copies:
    def __init__(self, semaphores):
        self.semaphores = semaphores
        self.used = 0

    def start(self, source, target):
        copy = pltpu.make_async_copy(source, target, self.semaphores.at[self.used])
        self.used += 1
        copy.start()
        return copy


def wait(*copies):
    for copy in copies:
        copy.wait()


def started():
    pl.delay(1)


def pack_kernel(
    rows_in, columns_in, senders_ref, cells_ref, out_ref, cells, out, senders, semaphores
):
    copies = Copies(semaphores)
    load_senders = copies.start(senders_ref, senders)
    load = copies.start(cells_ref, cells)
    shift = 20
    factor = -(-(1 << shift) // columns_in)
    assert all((i * factor) >> shift == i // columns_in for i in range(rows_in * columns_in))
    order = slot_order(senders)

    def row_of(i):
        cell = order(i)
        row = (cell * factor) >> shift
        return (cell - row * columns_in) * rows_in + row

    wait(load_senders, load)
    chunk = out.shape[0] // 4
    stores = []
    for first in range(0, out.shape[0], chunk):
        gather_rows(first, chunk, row_of, [(cells, out)])
        stores.append(
            copies.start(out.at[pl.ds(first, chunk)], out_ref.at[pl.ds(first, chunk)])
        )
    wait(*stores)


def rows_of(*biases):
    width = biases[0].shape[1]
    return jnp.concatenate([*biases, jnp.zeros((8 - len(biases), width), F32)], axis=0)


def before_kernel(
    grid_targets_s,
    mesh_senders_s,
    grid_targets,
    geometry,
    weight_geometry,
    edge_bias,
    node_bias,
    output_bias,
    update_bias,
    output_bias_2,
    refine_bias,
    nodes_ref,
    weight_self_ref,
    weight_receiver_ref,
    output_ref,
    summed_ref,
    sender_ref,
    update_ref,
    sender_ref_2,
    output_ref_2,
    summed_ref_2,
    refine_ref,
    sender_high,
    sender_low,
    merged_high,
    merged_low,
    received,
    biases,
    self_all_ref,
    self_sent_ref,
    nodes_sent_ref,
    match_ref,
    output_high_ref,
    onward_high_ref,
    onward_low_ref,
    update_high_ref,
    update_low_ref,
    merged_high_ref_2,
    merged_low_ref_2,
    output_high_ref_2,
    refine_high_ref,
    refine_low_ref,
    biases_ref_2,
    nodes,
    weight_self,
    weight_receiver,
    output,
    summed,
    sender,
    update,
    sender_2,
    output_2,
    summed_2,
    refine,
    self_all,
    self_sent,
    nodes_sent,
    match,
    output_high,
    onward_high,
    onward_low,
    update_high,
    update_low,
    merged_high_2,
    merged_low_2,
    output_high_2,
    refine_high,
    refine_low,
    biases_2,
    near,
    picked,
    table,
    chosen,
    semaphores,
):
    copies = Copies(semaphores)
    load_nodes = copies.start(nodes_ref, nodes)
    load_self = copies.start(weight_self_ref, weight_self)
    load_output = copies.start(output_ref, output)
    load_summed = copies.start(summed_ref, summed)
    load_receiver = copies.start(weight_receiver_ref, weight_receiver)
    load_sender = copies.start(sender_ref, sender)
    load_update = copies.start(update_ref, update)
    load_sender_2 = copies.start(sender_ref_2, sender_2)
    load_output_2 = copies.start(output_ref_2, output_2)
    load_summed_2 = copies.start(summed_ref_2, summed_2)
    load_refine = copies.start(refine_ref, refine)
    started()
    stores = []

    def store(*pairs):
        stores.extend(copies.start(source, target) for source, target in pairs)

    table[...] = target_matrix(nodes.shape[0], grid_targets)
    wait(load_nodes, load_self)
    self_all[...] = dot3(nodes[...], *split(weight_self[...])) + node_bias[...]
    store((self_all, self_all_ref))
    gather_rows(
        0,
        picked.shape[0],
        slot_order(mesh_senders_s),
        [(nodes, picked), (self_all, self_sent), (table, chosen)],
    )
    match[...] = chosen[...].astype(BF16)
    store((self_sent, self_sent_ref), (match, match_ref))
    wait(load_output, load_summed)
    centred = centre(output[...])
    high, low = split(summed[...])
    merged_high[...], merged_low[...] = split(dot3(centred, high, low))
    output_high[...] = centred.astype(BF16)
    store((output_high, output_high_ref))
    first_bias = centre(output_bias[...])
    first_bias_on = dot3(rows_of(first_bias), high, low)[0:1, :]
    gather_rows(
        0, near.shape[0], lambda i: jnp.maximum(grid_targets_s[0, i], 0), [(nodes, near)]
    )
    wait(load_receiver)
    received[...] = (
        dot3(near[...], *split(weight_receiver[...]))
        + geometry_rows(geometry, weight_geometry)
        + edge_bias[...]
    )
    wait(load_sender)
    sender_high[...], sender_low[...] = split(sender[...])
    wait(load_update, load_sender_2)
    centred = centre(update[...])
    update_high[...], update_low[...] = split(centred)
    high, low = split(sender_2[...])
    onward_high[...], onward_low[...] = split(dot3(centred, high, low))
    nodes_sent[...] = dot3(picked[...], high, low)
    store(
        (update_high, update_high_ref),
        (update_low, update_low_ref),
        (onward_high, onward_high_ref),
        (onward_low, onward_low_ref),
        (nodes_sent, nodes_sent_ref),
    )
    second_bias = centre(update_bias[...])
    second_bias_on = dot3(rows_of(second_bias), high, low)[0:1, :]
    biases[...] = rows_of(first_bias, first_bias_on, second_bias, second_bias_on)
    wait(load_output_2, load_summed_2, load_refine)
    centred = centre(output_2[...])
    high, low = split(summed_2[...])
    merged_high_2[...], merged_low_2[...] = split(dot3(centred, high, low))
    output_high_2[...] = centred.astype(BF16)
    third_bias = centre(output_bias_2[...])
    third_bias_on = dot3(rows_of(third_bias), high, low)[0:1, :]
    biases_2[...] = rows_of(third_bias, third_bias_on, centre(refine_bias[...]))
    refine_high[...], refine_low[...] = split(centre(refine[...]))
    store(
        (merged_high_2, merged_high_ref_2),
        (merged_low_2, merged_low_ref_2),
        (output_high_2, output_high_ref_2),
        (refine_high, refine_high_ref),
        (refine_low, refine_low_ref),
        (biases_2, biases_ref_2),
    )
    wait(*stores)


def edges(hidden, merged_high, merged_low, output_high, bias, bias_on, loads=()):
    hidden_high, hidden_low = split(hidden)
    high = merged_high[...]
    total = dot(hidden_high, high) + (
        dot(hidden_low, high) + dot(hidden_high, merged_low[...])
    )
    wait(*loads)
    return (total + bias_on) * scale(dot(hidden_high, output_high[...]) + bias)


def encode_kernel(
    arrived,
    sender_high,
    sender_low,
    merged_high,
    merged_low,
    received,
    biases,
    output_high_ref,
    match_ref,
    self_sent_ref,
    onward_high_ref,
    onward_low_ref,
    update_high_ref,
    nodes_sent_ref,
    sent_ref,
    parts_ref,
    output_high,
    match,
    self_sent,
    onward_high,
    onward_low,
    update_high,
    nodes_sent,
    sent,
    parts,
    semaphores,
):
    copies = Copies(semaphores)
    load_output = copies.start(output_high_ref, output_high)
    load_match = copies.start(match_ref, match)
    load_self = copies.start(self_sent_ref, self_sent)
    load_onward_high = copies.start(onward_high_ref, onward_high)
    load_onward_low = copies.start(onward_low_ref, onward_low)
    load_update = copies.start(update_high_ref, update_high)
    load_nodes = copies.start(nodes_sent_ref, nodes_sent)
    started()
    hidden = silu(dot3(arrived[...], sender_high[...], sender_low[...]) + received[...])
    part = edges(
        hidden, merged_high, merged_low, output_high, biases[0:1, :], biases[1:2, :], [load_output]
    )
    parts[...] = part
    store_parts = copies.start(parts, parts_ref)
    wait(load_match, load_self)
    hidden = silu(self_sent[...] + pick(match[...], part))
    wait(load_onward_high, load_onward_low, load_update, load_nodes)
    sent[...] = nodes_sent[...] + edges(
        hidden, onward_high, onward_low, update_high, biases[2:3, :], biases[3:4, :]
    )
    store_sent = copies.start(sent, sent_ref)
    wait(store_parts, store_sent)


def between_kernel(
    mesh_targets_s,
    grid_targets,
    mesh_targets,
    geometry,
    weight_geometry,
    edge_bias,
    node_bias,
    update_bias,
    refine_bias,
    merged_high_ref,
    merged_low_ref,
    output_high_ref,
    biases_ref,
    parts_ref,
    self_all_ref,
    nodes_ref,
    update_high_ref,
    update_low_ref,
    weight_self_ref,
    weight_receiver_ref,
    refine_high_ref,
    refine_low_ref,
    merged_high,
    merged_low,
    output_high,
    received,
    self_near,
    match,
    biases,
    normed_ref,
    base_ref,
    firsts_ref,
    parts,
    self_all,
    nodes,
    update_high,
    update_low,
    weight_self,
    weight_receiver,
    refine_high,
    refine_low,
    normed_near,
    base,
    firsts,
    near,
    encoded,
    self_next,
    normed,
    table,
    chosen,
    semaphores,
):
    copies = Copies(semaphores)
    load_parts = copies.start(parts_ref, parts)
    load_all = copies.start(self_all_ref, self_all)
    load_update_high = copies.start(update_high_ref, update_high)
    load_update_low = copies.start(update_low_ref, update_low)
    load_nodes = copies.start(nodes_ref, nodes)
    load_self = copies.start(weight_self_ref, weight_self)
    load_receiver = copies.start(weight_receiver_ref, weight_receiver)
    load_refine_high = copies.start(refine_high_ref, refine_high)
    load_refine_low = copies.start(refine_low_ref, refine_low)
    passed = [
        copies.start(merged_high_ref, merged_high),
        copies.start(merged_low_ref, merged_low),
        copies.start(output_high_ref, output_high),
        copies.start(biases_ref, biases),
    ]
    started()
    stores = []
    one_hot = target_matrix(nodes.shape[0], grid_targets).astype(BF16)
    table[...] = target_matrix(table.shape[0], mesh_targets)
    number = nodes.shape[0]

    def node_or_empty(i):
        target = mesh_targets_s[0, i]
        return jnp.where(target < 0, number, target)

    wait(load_parts, load_all)
    hidden = silu(self_all[...] + pick(one_hot, parts[...]))
    wait(load_update_high, load_update_low, load_nodes)
    encoded[...] = nodes[...] + norm_centred(
        dot3(hidden, update_high[...], update_low[...]) + centre(update_bias[...])
    )
    wait(load_self)
    self_next[...] = dot3(encoded[...], *split(weight_self[...])) + node_bias[...]
    wait(load_refine_high, load_refine_low)
    normed[...] = norm_centred(
        dot3(silu(self_next[...]), refine_high[...], refine_low[...]) + centre(refine_bias[...])
    )
    base[...] = encoded[...] + normed[...]
    stores.append(copies.start(base, base_ref))
    gather_rows(
        0,
        near.shape[0],
        lambda i: jnp.maximum(mesh_targets_s[0, i], 0),
        [(encoded, near), (self_next, self_near), (normed, normed_near)],
    )
    gather_rows(0, near.shape[0], node_or_empty, [(table, chosen)])
    slots = near.shape[0]
    same = chosen[...]
    match[...] = same.astype(BF16)
    earlier = lax.broadcasted_iota(jnp.int32, (slots, slots), 0) < lax.broadcasted_iota(
        jnp.int32, (slots, slots), 1
    )
    repeats = jnp.sum(jnp.where(earlier, same, 0.0), axis=0, keepdims=True)
    firsts[...] = jnp.where(repeats == 0.0, table[0:number, :], 0.0).astype(BF16)
    stores.append(copies.start(normed_near, normed_ref))
    stores.append(copies.start(firsts, firsts_ref))
    wait(load_receiver)
    received[...] = (
        dot3(near[...], *split(weight_receiver[...]))
        + geometry_rows(geometry, weight_geometry)
        + edge_bias[...]
    )
    wait(*passed, *stores)


def refine_kernel(
    arrived,
    merged_high,
    merged_low,
    output_high,
    received,
    self_near,
    match,
    biases,
    refine_high_ref,
    refine_low_ref,
    normed_ref,
    firsts_ref,
    base_ref,
    out_ref,
    refine_high,
    refine_low,
    normed,
    firsts,
    base,
    out,
    semaphores,
):
    copies = Copies(semaphores)
    load_refine_high = copies.start(refine_high_ref, refine_high)
    load_refine_low = copies.start(refine_low_ref, refine_low)
    load_normed = copies.start(normed_ref, normed)
    load_firsts = copies.start(firsts_ref, firsts)
    load_base = copies.start(base_ref, base)
    started()
    part = edges(
        silu(arrived[...] + received[...]),
        merged_high,
        merged_low,
        output_high,
        biases[0:1, :],
        biases[1:2, :],
    )
    hidden = silu(self_near[...] + pick(match[...], part))
    wait(load_refine_high, load_refine_low)
    change = norm_centred(dot3(hidden, refine_high[...], refine_low[...]) + biases[2:3, :])
    wait(load_normed, load_firsts, load_base)
    high, low = split(change - normed[...])
    number = out.shape[0]
    chunk = number // 2
    stores = []
    for first in range(0, number, chunk):
        at = pl.ds(first, chunk)
        out[at, :] = base[at, :] + (dot(firsts[at, :], high) + dot(firsts[at, :], low))
        stores.append(copies.start(out.at[at], out_ref.at[at]))
    wait(*stores)


def flat(dims, kind=F32):
    return jax.ShapeDtypeStruct(dims, kind)


def call(
    kernel, name, flops, scalars, small, kept, large, results, held=(), scratch=(), direct=()
):
    direct = [pltpu.with_memory_space_constraint(array, pltpu.HBM) for array in direct]
    kept = [pltpu.with_memory_space_constraint(array, pltpu.VMEM) for array in kept]
    large = [pltpu.with_memory_space_constraint(array, pltpu.HBM) for array in large]
    twins = [pltpu.VMEM(array.shape, array.dtype) for array in [*large, *results]]
    twins += list(scratch)
    size = sum(4 * spec.inner_aval.size for spec in twins)
    return pl.pallas_call(
        kernel,
        out_shape=[pltpu.VMEM(array.shape, array.dtype) for array in held]
        + [pltpu.HBM(array.shape, array.dtype) for array in results],
        in_specs=[SMEM] * len(scalars)
        + [VMEM] * (len(small) + len(kept))
        + [HBM] * (len(direct) + len(large)),
        out_specs=[VMEM] * len(held) + [HBM] * len(results),
        scratch_shapes=[
            *twins,
            pltpu.SemaphoreType.DMA((len(direct) + len(large) + len(results) + 8,)),
        ],
        cost_estimate=pl.CostEstimate(flops=flops, bytes_accessed=4 * 2**20, transcendentals=0),
        compiler_params=pltpu.CompilerParams(vmem_limit_bytes=size + 12 * 2**20),
        name=name,
    )(*scalars, *small, *kept, *direct, *large)


def exchange(rows, patches):
    blocks = rows.reshape(patches, -1, rows.shape[1])
    blocks = lax.all_to_all(blocks, ("lat", "lon"), split_axis=0, concat_axis=0, tiled=True)
    return blocks.reshape(rows.shape)


def per_device(
    grid_latent,
    mesh_latent,
    grid_senders,
    grid_targets,
    grid_geometry,
    mesh_senders,
    mesh_targets,
    mesh_geometry,
    encoder_sender,
    encoder_receiver,
    encoder_geometry,
    encoder_bias,
    encoder_output,
    encoder_outbias,
    update_self,
    update_summed,
    update_bias,
    update_output,
    update_outbias,
    process_sender,
    process_receiver,
    process_geometry,
    process_bias,
    process_output,
    process_outbias,
    refine_self,
    refine_summed,
    refine_bias,
    refine_output,
    refine_outbias,
):
    number, width = mesh_latent.shape
    patches = grid_senders.shape[1]
    grid_slots = grid_targets.shape[1]
    mesh_slots = mesh_targets.shape[1]
    rows_in, columns_in = grid_latent.shape[:2]
    square = 2 * width * width
    row = lambda bias: bias.reshape(1, width)
    halves = [flat((width, width), BF16)] * 2

    cells = grid_latent.transpose(1, 0, 2).reshape(rows_in * columns_in, width)
    (packed,) = call(
        functools.partial(pack_kernel, rows_in, columns_in),
        "pack",
        1000,
        [],
        [],
        [],
        [cells],
        [flat((grid_slots, width))],
        scratch=[pltpu.SMEM((grid_slots // patches, patches), jnp.int32)],
        direct=[grid_senders[0].T],
    )
    grid_in = exchange(packed, patches)

    (
        *first,
        self_all,
        self_sent,
        nodes_sent,
        match,
        output_high,
        onward_high,
        onward_low,
        update_high,
        update_low,
        merged_high,
        merged_low,
        second_high,
        refine_high,
        refine_low,
        biases,
    ) = call(
        before_kernel,
        "before",
        (number + grid_slots) * square * 3,
        [grid_targets, mesh_senders[0].T],
        [
            grid_targets,
            grid_geometry,
            encoder_geometry,
            row(encoder_bias),
            row(update_bias),
            row(encoder_outbias),
            row(update_outbias),
            row(process_outbias),
            row(refine_outbias),
        ],
        [],
        [
            mesh_latent,
            update_self,
            encoder_receiver,
            encoder_output,
            update_summed,
            encoder_sender,
            update_output,
            process_sender,
            process_output,
            refine_summed,
            refine_output,
        ],
        [
            flat((number, width)),
            flat((mesh_slots, width)),
            flat((mesh_slots, width)),
            flat((mesh_slots, grid_slots), BF16),
        ]
        + halves * 5
        + [flat((8, width))],
        halves * 2 + [flat((grid_slots, width)), flat((8, width))],
        [
            pltpu.VMEM((grid_slots, width), F32),
            pltpu.VMEM((mesh_slots, width), F32),
            pltpu.VMEM((number, grid_slots), F32),
            pltpu.VMEM((mesh_slots, grid_slots), F32),
        ],
    )
    sent, parts = call(
        encode_kernel,
        "encode",
        (3 * grid_slots + mesh_slots) * square * 3,
        [],
        [],
        [grid_in, *first],
        [output_high, match, self_sent, onward_high, onward_low, update_high, nodes_sent],
        [flat((mesh_slots, width)), flat((grid_slots, width))],
    )
    mesh_in = exchange(sent, patches)
    *first, normed, base, firsts = call(
        between_kernel,
        "between",
        (3 * number + mesh_slots) * square * 3,
        [mesh_targets],
        [
            grid_targets,
            mesh_targets,
            mesh_geometry,
            process_geometry,
            row(process_bias),
            row(refine_bias),
            row(update_outbias),
            row(refine_outbias),
        ],
        [],
        [
            parts,
            self_all,
            mesh_latent,
            update_high,
            update_low,
            refine_self,
            process_receiver,
            refine_high,
            refine_low,
        ],
        [
            flat((mesh_slots, width)),
            flat((number, width)),
            flat((number, mesh_slots), BF16),
        ],
        [
            *halves,
            halves[0],
            flat((mesh_slots, width)),
            flat((mesh_slots, width)),
            flat((mesh_slots, mesh_slots), BF16),
            flat((8, width)),
        ],
        [
            pltpu.VMEM((mesh_slots, width), F32),
            pltpu.VMEM((number, width), F32),
            pltpu.VMEM((number, width), F32),
            pltpu.VMEM((number, width), F32),
            pltpu.VMEM((number + 8, mesh_slots), F32),
            pltpu.VMEM((mesh_slots, mesh_slots), F32),
        ],
        [merged_high, merged_low, second_high, biases],
    )
    (out,) = call(
        refine_kernel,
        "refine",
        4 * mesh_slots * square * 3,
        [],
        [],
        [mesh_in, *first],
        [
            refine_high,
            refine_low,
            normed,
            firsts,
            base,
        ],
        [flat((number, width))],
    )
    return out


def solution(mesh):
    patch = P(("lat", "lon"), None)
    block = P(("lat", "lon"), None, None)
    feature = P(None, ("lat", "lon"), None)
    return jax.shard_map(
        per_device,
        mesh=mesh,
        in_specs=(P("lat", "lon", None), patch, block, patch, feature, block, patch, feature)
        + (P(),) * 22,
        out_specs=patch,
        check_vma=False,
    )
```

```python
import functools

import jax
import jax.numpy as jnp
from jax import lax
from jax.experimental import pallas as pl
from jax.experimental.pallas import tpu as pltpu
from jax.sharding import PartitionSpec as P

F32 = jnp.float32
BF16 = jnp.bfloat16
VMEM = pl.BlockSpec(memory_space=pltpu.VMEM)
SMEM = pl.BlockSpec(memory_space=pltpu.SMEM)
HBM = pl.BlockSpec(memory_space=pltpu.HBM)


def split(values):
    high = values.astype(BF16)
    low = (values - high.astype(F32)).astype(BF16)
    return high, low


def dot(left, right):
    return jnp.dot(left, right, preferred_element_type=F32)


def dot3(left, high, low):
    left_high, left_low = split(left)
    return dot(left_high, high) + (dot(left_low, high) + dot(left_high, low))


def pick(one_hot, values):
    high, low = split(values)
    return dot(one_hot, high) + dot(one_hot, low)


def silu(values):
    half = 0.5 * values
    return half + half * jnp.tanh(half)


def centre(values):
    return values - jnp.mean(values, axis=-1, keepdims=True)


def scale(centred):
    return lax.rsqrt(jnp.mean(centred * centred, axis=-1, keepdims=True) + 1e-05)


def norm_centred(centred):
    return centred * scale(centred)


def gather_rows(first, count, row_of, pairs, unroll=16):
    def step(i, carry):
        row = row_of(i)
        for source, target in pairs:
            target[pl.ds(i, 1), :] = source[pl.ds(row, 1), :]
        return carry

    if count <= 256:
        for i in range(first, first + count):
            step(i, 0)
    else:
        lax.fori_loop(first, first + count, step, 0, unroll=unroll)


def geometry_rows(geometry_ref, weight_ref):
    features, _, slots = geometry_ref.shape
    rows = jnp.concatenate([geometry_ref[k] for k in range(features)], axis=0)
    padded = jnp.concatenate([rows, jnp.zeros((8 - features % 8, slots), F32)], axis=0)
    columns = padded.T
    total = columns[:, 0:1] * weight_ref[0:1, :]
    for k in range(1, features):
        total += columns[:, k : k + 1] * weight_ref[k : k + 1, :]
    return total


def target_matrix(number, targets_ref):
    slots = targets_ref.shape[1]
    nodes = lax.broadcasted_iota(jnp.int32, (number, slots), 0)
    return jnp.where(nodes == targets_ref[...], 1.0, 0.0).astype(F32)


def slot_order(index_ref):
    capacity = index_ref.shape[0]
    bits = capacity.bit_length() - 1
    assert capacity == 1 << bits
    return lambda i: index_ref[i & (capacity - 1), i >> bits]


class Copies:
    def __init__(self, semaphores):
        self.semaphores = semaphores
        self.used = 0

    def start(self, source, target):
        copy = pltpu.make_async_copy(source, target, self.semaphores.at[self.used])
        self.used += 1
        copy.start()
        return copy


def wait(*copies):
    for copy in copies:
        copy.wait()


def started():
    pl.delay(1)


def pack_kernel(
    rows_in,
    columns_in,
    senders_ref,
    cells_ref,
    out_ref,
    cells,
    out,
    senders,
    senders_s,
    semaphores,
):
    copies = Copies(semaphores)
    load_senders = copies.start(senders_ref, senders)
    load_cells = copies.start(cells_ref, cells)
    shift = 20
    factor = -(-(1 << shift) // columns_in)
    assert all((i * factor) >> shift == i // columns_in for i in range(rows_in * columns_in))
    wait(load_senders)
    cell = senders[...]
    row = (cell * factor) >> shift
    senders[...] = (cell - row * columns_in) * rows_in + row
    wait(copies.start(senders, senders_s), load_cells)
    chunk = out.shape[0] // 2
    stores = []
    for first in range(0, out.shape[0], chunk):
        gather_rows(first, chunk, slot_order(senders_s), [(cells, out)])
        at = pl.ds(first, chunk)
        stores.append(copies.start(out.at[at], out_ref.at[at]))
        started()
    wait(*stores)


def rows_of(*biases):
    width = biases[0].shape[1]
    return jnp.concatenate([*biases, jnp.zeros((8 - len(biases), width), F32)], axis=0)


def before_kernel(
    grid_targets_s,
    mesh_senders_s,
    grid_targets,
    geometry,
    weight_geometry,
    edge_bias,
    node_bias,
    output_bias,
    update_bias,
    output_bias_2,
    refine_bias,
    nodes_ref,
    weight_self_ref,
    weight_receiver_ref,
    output_ref,
    summed_ref,
    sender_ref,
    update_ref,
    sender_ref_2,
    output_ref_2,
    summed_ref_2,
    refine_ref,
    sender_high,
    sender_low,
    merged_high,
    merged_low,
    received,
    biases,
    self_all_ref,
    self_sent_ref,
    nodes_sent_ref,
    match_ref,
    output_high_ref,
    onward_high_ref,
    onward_low_ref,
    update_high_ref,
    update_low_ref,
    merged_high_ref_2,
    merged_low_ref_2,
    output_high_ref_2,
    refine_high_ref,
    refine_low_ref,
    biases_ref_2,
    nodes,
    weight_self,
    weight_receiver,
    output,
    summed,
    sender,
    update,
    sender_2,
    output_2,
    summed_2,
    refine,
    self_all,
    self_sent,
    nodes_sent,
    match,
    output_high,
    onward_high,
    onward_low,
    update_high,
    update_low,
    merged_high_2,
    merged_low_2,
    output_high_2,
    refine_high,
    refine_low,
    biases_2,
    near,
    picked,
    table,
    chosen,
    semaphores,
):
    copies = Copies(semaphores)
    load_nodes = copies.start(nodes_ref, nodes)
    load_self = copies.start(weight_self_ref, weight_self)
    load_output = copies.start(output_ref, output)
    load_summed = copies.start(summed_ref, summed)
    load_receiver = copies.start(weight_receiver_ref, weight_receiver)
    load_sender = copies.start(sender_ref, sender)
    load_update = copies.start(update_ref, update)
    load_sender_2 = copies.start(sender_ref_2, sender_2)
    load_output_2 = copies.start(output_ref_2, output_2)
    load_summed_2 = copies.start(summed_ref_2, summed_2)
    load_refine = copies.start(refine_ref, refine)
    started()
    stores = []

    def store(*pairs):
        stores.extend(copies.start(source, target) for source, target in pairs)

    table[...] = target_matrix(nodes.shape[0], grid_targets)
    wait(load_nodes, load_self)
    self_all[...] = dot3(nodes[...], *split(weight_self[...])) + node_bias[...]
    store((self_all, self_all_ref))
    gather_rows(
        0,
        picked.shape[0],
        slot_order(mesh_senders_s),
        [(nodes, picked), (self_all, self_sent), (table, chosen)],
    )
    match[...] = chosen[...].astype(BF16)
    store((self_sent, self_sent_ref), (match, match_ref))
    wait(load_output, load_summed)
    centred = centre(output[...])
    high, low = split(summed[...])
    merged_high[...], merged_low[...] = split(dot3(centred, high, low))
    output_high[...] = centred.astype(BF16)
    store((output_high, output_high_ref))
    first_bias = centre(output_bias[...])
    first_bias_on = dot3(rows_of(first_bias), high, low)[0:1, :]
    gather_rows(
        0, near.shape[0], lambda i: jnp.maximum(grid_targets_s[0, i], 0), [(nodes, near)]
    )
    wait(load_receiver)
    received[...] = (
        dot3(near[...], *split(weight_receiver[...]))
        + geometry_rows(geometry, weight_geometry)
        + edge_bias[...]
    )
    wait(load_sender)
    sender_high[...], sender_low[...] = split(sender[...])
    wait(load_update, load_sender_2)
    centred = centre(update[...])
    update_high[...], update_low[...] = split(centred)
    high, low = split(sender_2[...])
    onward_high[...], onward_low[...] = split(dot3(centred, high, low))
    nodes_sent[...] = dot3(picked[...], high, low)
    store(
        (update_high, update_high_ref),
        (update_low, update_low_ref),
        (onward_high, onward_high_ref),
        (onward_low, onward_low_ref),
        (nodes_sent, nodes_sent_ref),
    )
    second_bias = centre(update_bias[...])
    second_bias_on = dot3(rows_of(second_bias), high, low)[0:1, :]
    biases[...] = rows_of(first_bias, first_bias_on, second_bias, second_bias_on)
    wait(load_output_2, load_summed_2, load_refine)
    centred = centre(output_2[...])
    high, low = split(summed_2[...])
    merged_high_2[...], merged_low_2[...] = split(dot3(centred, high, low))
    output_high_2[...] = centred.astype(BF16)
    third_bias = centre(output_bias_2[...])
    third_bias_on = dot3(rows_of(third_bias), high, low)[0:1, :]
    biases_2[...] = rows_of(third_bias, third_bias_on, centre(refine_bias[...]))
    refine_high[...], refine_low[...] = split(centre(refine[...]))
    store(
        (merged_high_2, merged_high_ref_2),
        (merged_low_2, merged_low_ref_2),
        (output_high_2, output_high_ref_2),
        (refine_high, refine_high_ref),
        (refine_low, refine_low_ref),
        (biases_2, biases_ref_2),
    )
    wait(*stores)


def edges(hidden, merged_high, merged_low, output_high, bias, bias_on, loads=()):
    hidden_high, hidden_low = split(hidden)
    high = merged_high[...]
    total = dot(hidden_high, high) + (
        dot(hidden_low, high) + dot(hidden_high, merged_low[...])
    )
    wait(*loads)
    return (total + bias_on) * scale(dot(hidden_high, output_high[...]) + bias)


def encode_kernel(
    arrived,
    sender_high,
    sender_low,
    merged_high,
    merged_low,
    received,
    biases,
    output_high_ref,
    match_ref,
    self_sent_ref,
    onward_high_ref,
    onward_low_ref,
    update_high_ref,
    nodes_sent_ref,
    sent_ref,
    parts_ref,
    output_high,
    match,
    self_sent,
    onward_high,
    onward_low,
    update_high,
    nodes_sent,
    sent,
    parts,
    semaphores,
):
    copies = Copies(semaphores)
    load_output = copies.start(output_high_ref, output_high)
    load_match = copies.start(match_ref, match)
    load_self = copies.start(self_sent_ref, self_sent)
    load_onward_high = copies.start(onward_high_ref, onward_high)
    load_onward_low = copies.start(onward_low_ref, onward_low)
    load_update = copies.start(update_high_ref, update_high)
    load_nodes = copies.start(nodes_sent_ref, nodes_sent)
    started()
    hidden = silu(dot3(arrived[...], sender_high[...], sender_low[...]) + received[...])
    part = edges(
        hidden, merged_high, merged_low, output_high, biases[0:1, :], biases[1:2, :], [load_output]
    )
    parts[...] = part
    store_parts = copies.start(parts, parts_ref)
    wait(load_match, load_self)
    hidden = silu(self_sent[...] + pick(match[...], part))
    wait(load_onward_high, load_onward_low, load_update, load_nodes)
    sent[...] = nodes_sent[...] + edges(
        hidden, onward_high, onward_low, update_high, biases[2:3, :], biases[3:4, :]
    )
    store_sent = copies.start(sent, sent_ref)
    wait(store_parts, store_sent)


def between_kernel(
    mesh_targets_s,
    grid_targets,
    mesh_targets,
    geometry,
    weight_geometry,
    edge_bias,
    node_bias,
    update_bias,
    refine_bias,
    merged_high_ref,
    merged_low_ref,
    output_high_ref,
    biases_ref,
    parts_ref,
    self_all_ref,
    nodes_ref,
    update_high_ref,
    update_low_ref,
    weight_self_ref,
    weight_receiver_ref,
    refine_high_ref,
    refine_low_ref,
    merged_high,
    merged_low,
    output_high,
    received,
    self_near,
    match,
    biases,
    normed_ref,
    base_ref,
    firsts_ref,
    parts,
    self_all,
    nodes,
    update_high,
    update_low,
    weight_self,
    weight_receiver,
    refine_high,
    refine_low,
    normed_near,
    base,
    firsts,
    near,
    encoded,
    self_next,
    normed,
    table,
    chosen,
    semaphores,
):
    copies = Copies(semaphores)
    load_parts = copies.start(parts_ref, parts)
    load_all = copies.start(self_all_ref, self_all)
    load_update_high = copies.start(update_high_ref, update_high)
    load_update_low = copies.start(update_low_ref, update_low)
    load_nodes = copies.start(nodes_ref, nodes)
    load_self = copies.start(weight_self_ref, weight_self)
    load_receiver = copies.start(weight_receiver_ref, weight_receiver)
    load_refine_high = copies.start(refine_high_ref, refine_high)
    load_refine_low = copies.start(refine_low_ref, refine_low)
    passed = [
        copies.start(merged_high_ref, merged_high),
        copies.start(merged_low_ref, merged_low),
        copies.start(output_high_ref, output_high),
        copies.start(biases_ref, biases),
    ]
    started()
    stores = []
    one_hot = target_matrix(nodes.shape[0], grid_targets).astype(BF16)
    table[...] = target_matrix(table.shape[0], mesh_targets)
    number = nodes.shape[0]

    def node_or_empty(i):
        target = mesh_targets_s[0, i]
        return jnp.where(target < 0, number, target)

    wait(load_parts, load_all)
    hidden = silu(self_all[...] + pick(one_hot, parts[...]))
    wait(load_update_high, load_update_low, load_nodes)
    encoded[...] = nodes[...] + norm_centred(
        dot3(hidden, update_high[...], update_low[...]) + centre(update_bias[...])
    )
    wait(load_self)
    self_next[...] = dot3(encoded[...], *split(weight_self[...])) + node_bias[...]
    wait(load_refine_high, load_refine_low)
    normed[...] = norm_centred(
        dot3(silu(self_next[...]), refine_high[...], refine_low[...]) + centre(refine_bias[...])
    )
    base[...] = encoded[...] + normed[...]
    stores.append(copies.start(base, base_ref))
    gather_rows(
        0,
        near.shape[0],
        lambda i: jnp.maximum(mesh_targets_s[0, i], 0),
        [(encoded, near), (self_next, self_near), (normed, normed_near)],
    )
    gather_rows(0, near.shape[0], node_or_empty, [(table, chosen)])
    slots = near.shape[0]
    same = chosen[...]
    match[...] = same.astype(BF16)
    earlier = lax.broadcasted_iota(jnp.int32, (slots, slots), 0) < lax.broadcasted_iota(
        jnp.int32, (slots, slots), 1
    )
    repeats = jnp.sum(jnp.where(earlier, same, 0.0), axis=0, keepdims=True)
    firsts[...] = jnp.where(repeats == 0.0, table[0:number, :], 0.0).astype(BF16)
    stores.append(copies.start(normed_near, normed_ref))
    stores.append(copies.start(firsts, firsts_ref))
    wait(load_receiver)
    received[...] = (
        dot3(near[...], *split(weight_receiver[...]))
        + geometry_rows(geometry, weight_geometry)
        + edge_bias[...]
    )
    wait(*passed, *stores)


def refine_kernel(
    arrived,
    merged_high,
    merged_low,
    output_high,
    received,
    self_near,
    match,
    biases,
    refine_high_ref,
    refine_low_ref,
    normed_ref,
    firsts_ref,
    base_ref,
    out_ref,
    refine_high,
    refine_low,
    normed,
    firsts,
    base,
    out,
    semaphores,
):
    copies = Copies(semaphores)
    load_refine_high = copies.start(refine_high_ref, refine_high)
    load_refine_low = copies.start(refine_low_ref, refine_low)
    load_normed = copies.start(normed_ref, normed)
    load_firsts = copies.start(firsts_ref, firsts)
    load_base = copies.start(base_ref, base)
    started()
    part = edges(
        silu(arrived[...] + received[...]),
        merged_high,
        merged_low,
        output_high,
        biases[0:1, :],
        biases[1:2, :],
    )
    hidden = silu(self_near[...] + pick(match[...], part))
    wait(load_refine_high, load_refine_low)
    change = norm_centred(dot3(hidden, refine_high[...], refine_low[...]) + biases[2:3, :])
    wait(load_normed, load_firsts, load_base)
    high, low = split(change - normed[...])
    number = out.shape[0]
    chunk = number // 2
    stores = []
    for first in range(0, number, chunk):
        at = pl.ds(first, chunk)
        out[at, :] = base[at, :] + (dot(firsts[at, :], high) + dot(firsts[at, :], low))
        stores.append(copies.start(out.at[at], out_ref.at[at]))
    wait(*stores)


def flat(dims, kind=F32):
    return jax.ShapeDtypeStruct(dims, kind)


def call(
    kernel, name, flops, scalars, small, kept, large, results, held=(), scratch=(), direct=()
):
    direct = [pltpu.with_memory_space_constraint(array, pltpu.HBM) for array in direct]
    kept = [pltpu.with_memory_space_constraint(array, pltpu.VMEM) for array in kept]
    large = [pltpu.with_memory_space_constraint(array, pltpu.HBM) for array in large]
    twins = [pltpu.VMEM(array.shape, array.dtype) for array in [*large, *results]]
    twins += list(scratch)
    size = sum(4 * spec.inner_aval.size for spec in twins)
    return pl.pallas_call(
        kernel,
        out_shape=[pltpu.VMEM(array.shape, array.dtype) for array in held]
        + [pltpu.HBM(array.shape, array.dtype) for array in results],
        in_specs=[SMEM] * len(scalars)
        + [VMEM] * (len(small) + len(kept))
        + [HBM] * (len(direct) + len(large)),
        out_specs=[VMEM] * len(held) + [HBM] * len(results),
        scratch_shapes=[
            *twins,
            pltpu.SemaphoreType.DMA((len(direct) + len(large) + len(results) + 8,)),
        ],
        cost_estimate=pl.CostEstimate(flops=flops, bytes_accessed=4 * 2**20, transcendentals=0),
        compiler_params=pltpu.CompilerParams(vmem_limit_bytes=size + 12 * 2**20),
        name=name,
    )(*scalars, *small, *kept, *direct, *large)


def exchange(rows, patches):
    blocks = rows.reshape(patches, -1, rows.shape[1])
    blocks = lax.all_to_all(blocks, ("lat", "lon"), split_axis=0, concat_axis=0, tiled=True)
    return blocks.reshape(rows.shape)


def per_device(
    grid_latent,
    mesh_latent,
    grid_senders,
    grid_targets,
    grid_geometry,
    mesh_senders,
    mesh_targets,
    mesh_geometry,
    encoder_sender,
    encoder_receiver,
    encoder_geometry,
    encoder_bias,
    encoder_output,
    encoder_outbias,
    update_self,
    update_summed,
    update_bias,
    update_output,
    update_outbias,
    process_sender,
    process_receiver,
    process_geometry,
    process_bias,
    process_output,
    process_outbias,
    refine_self,
    refine_summed,
    refine_bias,
    refine_output,
    refine_outbias,
):
    number, width = mesh_latent.shape
    patches = grid_senders.shape[1]
    grid_slots = grid_targets.shape[1]
    mesh_slots = mesh_targets.shape[1]
    rows_in, columns_in = grid_latent.shape[:2]
    square = 2 * width * width
    row = lambda bias: bias.reshape(1, width)
    halves = [flat((width, width), BF16)] * 2

    cells = grid_latent.transpose(1, 0, 2).reshape(rows_in * columns_in, width)
    (packed,) = call(
        functools.partial(pack_kernel, rows_in, columns_in),
        "pack",
        1000,
        [],
        [],
        [],
        [cells],
        [flat((grid_slots, width))],
        scratch=[
            pltpu.VMEM((grid_slots // patches, patches), jnp.int32),
            pltpu.SMEM((grid_slots // patches, patches), jnp.int32),
        ],
        direct=[grid_senders[0].T],
    )
    grid_in = exchange(packed, patches)

    (
        *first,
        self_all,
        self_sent,
        nodes_sent,
        match,
        output_high,
        onward_high,
        onward_low,
        update_high,
        update_low,
        merged_high,
        merged_low,
        second_high,
        refine_high,
        refine_low,
        biases,
    ) = call(
        before_kernel,
        "before",
        (number + grid_slots) * square * 3,
        [grid_targets, mesh_senders[0].T],
        [
            grid_targets,
            grid_geometry,
            encoder_geometry,
            row(encoder_bias),
            row(update_bias),
            row(encoder_outbias),
            row(update_outbias),
            row(process_outbias),
            row(refine_outbias),
        ],
        [],
        [
            mesh_latent,
            update_self,
            encoder_receiver,
            encoder_output,
            update_summed,
            encoder_sender,
            update_output,
            process_sender,
            process_output,
            refine_summed,
            refine_output,
        ],
        [
            flat((number, width)),
            flat((mesh_slots, width)),
            flat((mesh_slots, width)),
            flat((mesh_slots, grid_slots), BF16),
        ]
        + halves * 5
        + [flat((8, width))],
        halves * 2 + [flat((grid_slots, width)), flat((8, width))],
        [
            pltpu.VMEM((grid_slots, width), F32),
            pltpu.VMEM((mesh_slots, width), F32),
            pltpu.VMEM((number, grid_slots), F32),
            pltpu.VMEM((mesh_slots, grid_slots), F32),
        ],
    )
    sent, parts = call(
        encode_kernel,
        "encode",
        (3 * grid_slots + mesh_slots) * square * 3,
        [],
        [],
        [grid_in, *first],
        [output_high, match, self_sent, onward_high, onward_low, update_high, nodes_sent],
        [flat((mesh_slots, width)), flat((grid_slots, width))],
    )
    mesh_in = exchange(sent, patches)
    *first, normed, base, firsts = call(
        between_kernel,
        "between",
        (3 * number + mesh_slots) * square * 3,
        [mesh_targets],
        [
            grid_targets,
            mesh_targets,
            mesh_geometry,
            process_geometry,
            row(process_bias),
            row(refine_bias),
            row(update_outbias),
            row(refine_outbias),
        ],
        [],
        [
            parts,
            self_all,
            mesh_latent,
            update_high,
            update_low,
            refine_self,
            process_receiver,
            refine_high,
            refine_low,
        ],
        [
            flat((mesh_slots, width)),
            flat((number, width)),
            flat((number, mesh_slots), BF16),
        ],
        [
            *halves,
            halves[0],
            flat((mesh_slots, width)),
            flat((mesh_slots, width)),
            flat((mesh_slots, mesh_slots), BF16),
            flat((8, width)),
        ],
        [
            pltpu.VMEM((mesh_slots, width), F32),
            pltpu.VMEM((number, width), F32),
            pltpu.VMEM((number, width), F32),
            pltpu.VMEM((number, width), F32),
            pltpu.VMEM((number + 8, mesh_slots), F32),
            pltpu.VMEM((mesh_slots, mesh_slots), F32),
        ],
        [merged_high, merged_low, second_high, biases],
    )
    (out,) = call(
        refine_kernel,
        "refine",
        4 * mesh_slots * square * 3,
        [],
        [],
        [mesh_in, *first],
        [
            refine_high,
            refine_low,
            normed,
            firsts,
            base,
        ],
        [flat((number, width))],
    )
    return out


def solution(mesh):
    patch = P(("lat", "lon"), None)
    block = P(("lat", "lon"), None, None)
    feature = P(None, ("lat", "lon"), None)
    return jax.shard_map(
        per_device,
        mesh=mesh,
        in_specs=(P("lat", "lon", None), patch, block, patch, feature, block, patch, feature)
        + (P(),) * 22,
        out_specs=patch,
        check_vma=False,
    )
```

```python
import functools

import jax
import jax.numpy as jnp
from jax import lax
from jax.experimental import pallas as pl
from jax.experimental.pallas import tpu as pltpu
from jax.sharding import PartitionSpec as P

F32 = jnp.float32
BF16 = jnp.bfloat16
VMEM = pl.BlockSpec(memory_space=pltpu.VMEM)
SMEM = pl.BlockSpec(memory_space=pltpu.SMEM)
HBM = pl.BlockSpec(memory_space=pltpu.HBM)


def split(values):
    high = values.astype(BF16)
    low = (values - high.astype(F32)).astype(BF16)
    return high, low


def dot(left, right):
    return jnp.dot(left, right, preferred_element_type=F32)


def dot3(left, high, low):
    left_high, left_low = split(left)
    return dot(left_high, high) + (dot(left_low, high) + dot(left_high, low))


def pick(one_hot, values):
    high, low = split(values)
    return dot(one_hot, high) + dot(one_hot, low)


def silu(values):
    half = 0.5 * values
    return half + half * jnp.tanh(half)


def centre(values):
    return values - jnp.mean(values, axis=-1, keepdims=True)


def scale(centred):
    return lax.rsqrt(jnp.mean(centred * centred, axis=-1, keepdims=True) + 1e-05)


def norm_centred(centred):
    return centred * scale(centred)


def gather_rows(first, count, row_of, pairs, unroll=16):
    def step(i, carry):
        row = row_of(i)
        for source, target in pairs:
            target[pl.ds(i, 1), :] = source[pl.ds(row, 1), :]
        return carry

    if count <= 256:
        for i in range(first, first + count):
            step(i, 0)
    else:
        lax.fori_loop(first, first + count, step, 0, unroll=unroll)


def geometry_rows(geometry_ref, weight_ref):
    features, _, slots = geometry_ref.shape
    rows = jnp.concatenate([geometry_ref[k] for k in range(features)], axis=0)
    padded = jnp.concatenate([rows, jnp.zeros((8 - features % 8, slots), F32)], axis=0)
    columns = padded.T
    total = columns[:, 0:1] * weight_ref[0:1, :]
    for k in range(1, features):
        total += columns[:, k : k + 1] * weight_ref[k : k + 1, :]
    return total


def target_matrix(number, targets_ref):
    slots = targets_ref.shape[1]
    nodes = lax.broadcasted_iota(jnp.int32, (number, slots), 0)
    return jnp.where(nodes == targets_ref[...], 1.0, 0.0).astype(F32)


def slot_order(index_ref):
    capacity = index_ref.shape[0]
    bits = capacity.bit_length() - 1
    assert capacity == 1 << bits
    return lambda i: index_ref[i & (capacity - 1), i >> bits]


class Copies:
    def __init__(self, semaphores):
        self.semaphores = semaphores
        self.used = 0

    def start(self, source, target):
        copy = pltpu.make_async_copy(source, target, self.semaphores.at[self.used])
        self.used += 1
        copy.start()
        return copy


def wait(*copies):
    for copy in copies:
        copy.wait()


def started():
    pl.delay(1)


def pack_kernel(
    rows_in,
    columns_in,
    senders_ref,
    cells_ref,
    out_ref,
    cells,
    out,
    senders,
    senders_s,
    semaphores,
):
    copies = Copies(semaphores)
    load_senders = copies.start(senders_ref, senders)
    load_cells = copies.start(cells_ref, cells)
    shift = 20
    factor = -(-(1 << shift) // columns_in)
    assert all((i * factor) >> shift == i // columns_in for i in range(rows_in * columns_in))
    wait(load_senders)
    cell = senders[...]
    row = (cell * factor) >> shift
    senders[...] = (cell - row * columns_in) * rows_in + row
    wait(copies.start(senders, senders_s), load_cells)
    chunk = out.shape[0] // 2
    stores = []
    for first in range(0, out.shape[0], chunk):
        gather_rows(first, chunk, slot_order(senders_s), [(cells, out)])
        at = pl.ds(first, chunk)
        stores.append(copies.start(out.at[at], out_ref.at[at]))
        started()
    wait(*stores)


def rows_of(*biases):
    width = biases[0].shape[1]
    return jnp.concatenate([*biases, jnp.zeros((8 - len(biases), width), F32)], axis=0)


def before_kernel(
    grid_targets_s,
    mesh_senders_s,
    grid_targets,
    geometry,
    weight_geometry,
    edge_bias,
    node_bias,
    output_bias,
    update_bias,
    output_bias_2,
    refine_bias,
    nodes_ref,
    weight_self_ref,
    weight_receiver_ref,
    output_ref,
    summed_ref,
    sender_ref,
    update_ref,
    sender_ref_2,
    output_ref_2,
    summed_ref_2,
    refine_ref,
    sender_high,
    sender_low,
    merged_high,
    output_high,
    received,
    biases,
    self_all_ref,
    self_sent_ref,
    nodes_sent_ref,
    match_ref,
    merged_low_ref,
    onward_high_ref,
    onward_low_ref,
    update_high_ref,
    update_low_ref,
    merged_high_ref_2,
    merged_low_ref_2,
    output_high_ref_2,
    refine_high_ref,
    refine_low_ref,
    biases_ref_2,
    nodes,
    weight_self,
    weight_receiver,
    output,
    summed,
    sender,
    update,
    sender_2,
    output_2,
    summed_2,
    refine,
    self_all,
    self_sent,
    nodes_sent,
    match,
    merged_low,
    onward_high,
    onward_low,
    update_high,
    update_low,
    merged_high_2,
    merged_low_2,
    output_high_2,
    refine_high,
    refine_low,
    biases_2,
    near,
    picked,
    table,
    chosen,
    semaphores,
):
    copies = Copies(semaphores)
    load_nodes = copies.start(nodes_ref, nodes)
    load_self = copies.start(weight_self_ref, weight_self)
    load_output = copies.start(output_ref, output)
    load_summed = copies.start(summed_ref, summed)
    load_receiver = copies.start(weight_receiver_ref, weight_receiver)
    load_sender = copies.start(sender_ref, sender)
    load_update = copies.start(update_ref, update)
    load_sender_2 = copies.start(sender_ref_2, sender_2)
    load_output_2 = copies.start(output_ref_2, output_2)
    load_summed_2 = copies.start(summed_ref_2, summed_2)
    load_refine = copies.start(refine_ref, refine)
    started()
    stores = []

    def store(*pairs):
        stores.extend(copies.start(source, target) for source, target in pairs)

    table[...] = target_matrix(nodes.shape[0], grid_targets)
    wait(load_nodes, load_self)
    self_all[...] = dot3(nodes[...], *split(weight_self[...])) + node_bias[...]
    store((self_all, self_all_ref))
    gather_rows(
        0,
        picked.shape[0],
        slot_order(mesh_senders_s),
        [(nodes, picked), (self_all, self_sent), (table, chosen)],
    )
    match[...] = chosen[...].astype(BF16)
    store((self_sent, self_sent_ref), (match, match_ref))
    wait(load_output, load_summed)
    centred = centre(output[...])
    high, low = split(summed[...])
    merged_high[...], merged_low[...] = split(dot3(centred, high, low))
    output_high[...] = centred.astype(BF16)
    store((merged_low, merged_low_ref))
    first_bias = centre(output_bias[...])
    first_bias_on = dot3(rows_of(first_bias), high, low)[0:1, :]
    gather_rows(
        0, near.shape[0], lambda i: jnp.maximum(grid_targets_s[0, i], 0), [(nodes, near)]
    )
    wait(load_receiver)
    received[...] = (
        dot3(near[...], *split(weight_receiver[...]))
        + geometry_rows(geometry, weight_geometry)
        + edge_bias[...]
    )
    wait(load_sender)
    sender_high[...], sender_low[...] = split(sender[...])
    wait(load_update, load_sender_2)
    centred = centre(update[...])
    update_high[...], update_low[...] = split(centred)
    high, low = split(sender_2[...])
    onward_high[...], onward_low[...] = split(dot3(centred, high, low))
    nodes_sent[...] = dot3(picked[...], high, low)
    store(
        (update_high, update_high_ref),
        (update_low, update_low_ref),
        (onward_high, onward_high_ref),
        (onward_low, onward_low_ref),
        (nodes_sent, nodes_sent_ref),
    )
    second_bias = centre(update_bias[...])
    second_bias_on = dot3(rows_of(second_bias), high, low)[0:1, :]
    biases[...] = rows_of(first_bias, first_bias_on, second_bias, second_bias_on)
    wait(load_output_2, load_summed_2, load_refine)
    centred = centre(output_2[...])
    high, low = split(summed_2[...])
    merged_high_2[...], merged_low_2[...] = split(dot3(centred, high, low))
    output_high_2[...] = centred.astype(BF16)
    third_bias = centre(output_bias_2[...])
    third_bias_on = dot3(rows_of(third_bias), high, low)[0:1, :]
    biases_2[...] = rows_of(third_bias, third_bias_on, centre(refine_bias[...]))
    refine_high[...], refine_low[...] = split(centre(refine[...]))
    store(
        (merged_high_2, merged_high_ref_2),
        (merged_low_2, merged_low_ref_2),
        (output_high_2, output_high_ref_2),
        (refine_high, refine_high_ref),
        (refine_low, refine_low_ref),
        (biases_2, biases_ref_2),
    )
    wait(*stores)


def edges(hidden, merged_high, merged_low, output_high, bias, bias_on, load_low=()):
    hidden_high, hidden_low = split(hidden)
    normed = scale(dot(hidden_high, output_high[...]) + bias)
    high = merged_high[...]
    total = dot(hidden_high, high) + dot(hidden_low, high)
    wait(*load_low)
    return (total + dot(hidden_high, merged_low[...]) + bias_on) * normed


def encode_kernel(
    arrived,
    sender_high,
    sender_low,
    merged_high,
    output_high,
    received,
    biases,
    merged_low_ref,
    match_ref,
    self_sent_ref,
    onward_high_ref,
    onward_low_ref,
    update_high_ref,
    nodes_sent_ref,
    sent_ref,
    parts_ref,
    merged_low,
    match,
    self_sent,
    onward_high,
    onward_low,
    update_high,
    nodes_sent,
    sent,
    parts,
    semaphores,
):
    copies = Copies(semaphores)
    load_merged = copies.start(merged_low_ref, merged_low)
    load_match = copies.start(match_ref, match)
    load_self = copies.start(self_sent_ref, self_sent)
    load_onward_high = copies.start(onward_high_ref, onward_high)
    load_onward_low = copies.start(onward_low_ref, onward_low)
    load_update = copies.start(update_high_ref, update_high)
    load_nodes = copies.start(nodes_sent_ref, nodes_sent)
    started()
    hidden = silu(dot3(arrived[...], sender_high[...], sender_low[...]) + received[...])
    part = edges(
        hidden, merged_high, merged_low, output_high, biases[0:1, :], biases[1:2, :], [load_merged]
    )
    parts[...] = part
    store_parts = copies.start(parts, parts_ref)
    wait(load_match, load_self)
    hidden = silu(self_sent[...] + pick(match[...], part))
    wait(load_onward_high, load_update)
    sent[...] = (
        edges(
            hidden,
            onward_high,
            onward_low,
            update_high,
            biases[2:3, :],
            biases[3:4, :],
            [load_onward_low, load_nodes],
        )
        + nodes_sent[...]
    )
    store_sent = copies.start(sent, sent_ref)
    wait(store_parts, store_sent)


def between_kernel(
    mesh_targets_s,
    grid_targets,
    mesh_targets,
    geometry,
    weight_geometry,
    edge_bias,
    node_bias,
    update_bias,
    refine_bias,
    merged_high_ref,
    merged_low_ref,
    output_high_ref,
    biases_ref,
    parts_ref,
    self_all_ref,
    nodes_ref,
    update_high_ref,
    update_low_ref,
    weight_self_ref,
    weight_receiver_ref,
    refine_high_ref,
    refine_low_ref,
    merged_high,
    merged_low,
    output_high,
    received,
    self_near,
    match,
    biases,
    normed_ref,
    base_ref,
    firsts_ref,
    parts,
    self_all,
    nodes,
    update_high,
    update_low,
    weight_self,
    weight_receiver,
    refine_high,
    refine_low,
    normed_near,
    base,
    firsts,
    near,
    encoded,
    self_next,
    normed,
    table,
    chosen,
    semaphores,
):
    copies = Copies(semaphores)
    load_parts = copies.start(parts_ref, parts)
    load_all = copies.start(self_all_ref, self_all)
    load_update_high = copies.start(update_high_ref, update_high)
    load_update_low = copies.start(update_low_ref, update_low)
    load_nodes = copies.start(nodes_ref, nodes)
    load_self = copies.start(weight_self_ref, weight_self)
    load_receiver = copies.start(weight_receiver_ref, weight_receiver)
    load_refine_high = copies.start(refine_high_ref, refine_high)
    load_refine_low = copies.start(refine_low_ref, refine_low)
    passed = [
        copies.start(merged_high_ref, merged_high),
        copies.start(merged_low_ref, merged_low),
        copies.start(output_high_ref, output_high),
        copies.start(biases_ref, biases),
    ]
    started()
    stores = []
    one_hot = target_matrix(nodes.shape[0], grid_targets).astype(BF16)
    table[...] = target_matrix(table.shape[0], mesh_targets)
    number = nodes.shape[0]

    def node_or_empty(i):
        target = mesh_targets_s[0, i]
        return jnp.where(target < 0, number, target)

    wait(load_parts, load_all)
    hidden = silu(self_all[...] + pick(one_hot, parts[...]))
    wait(load_update_high, load_update_low, load_nodes)
    encoded[...] = nodes[...] + norm_centred(
        dot3(hidden, update_high[...], update_low[...]) + centre(update_bias[...])
    )
    wait(load_self)
    self_next[...] = dot3(encoded[...], *split(weight_self[...])) + node_bias[...]
    wait(load_refine_high, load_refine_low)
    normed[...] = norm_centred(
        dot3(silu(self_next[...]), refine_high[...], refine_low[...]) + centre(refine_bias[...])
    )
    base[...] = encoded[...] + normed[...]
    stores.append(copies.start(base, base_ref))
    gather_rows(
        0,
        near.shape[0],
        lambda i: jnp.maximum(mesh_targets_s[0, i], 0),
        [(encoded, near), (self_next, self_near), (normed, normed_near)],
    )
    gather_rows(0, near.shape[0], node_or_empty, [(table, chosen)])
    slots = near.shape[0]
    same = chosen[...]
    match[...] = same.astype(BF16)
    earlier = lax.broadcasted_iota(jnp.int32, (slots, slots), 0) < lax.broadcasted_iota(
        jnp.int32, (slots, slots), 1
    )
    repeats = jnp.sum(jnp.where(earlier, same, 0.0), axis=0, keepdims=True)
    firsts[...] = jnp.where(repeats == 0.0, table[0:number, :], 0.0).astype(BF16)
    stores.append(copies.start(normed_near, normed_ref))
    stores.append(copies.start(firsts, firsts_ref))
    wait(load_receiver)
    received[...] = (
        dot3(near[...], *split(weight_receiver[...]))
        + geometry_rows(geometry, weight_geometry)
        + edge_bias[...]
    )
    wait(*passed, *stores)


def refine_kernel(
    arrived,
    merged_high,
    merged_low,
    output_high,
    received,
    self_near,
    match,
    biases,
    refine_high_ref,
    refine_low_ref,
    normed_ref,
    firsts_ref,
    base_ref,
    out_ref,
    refine_high,
    refine_low,
    normed,
    firsts,
    base,
    out,
    semaphores,
):
    copies = Copies(semaphores)
    load_refine_high = copies.start(refine_high_ref, refine_high)
    load_refine_low = copies.start(refine_low_ref, refine_low)
    load_normed = copies.start(normed_ref, normed)
    load_firsts = copies.start(firsts_ref, firsts)
    load_base = copies.start(base_ref, base)
    started()
    part = edges(
        silu(arrived[...] + received[...]),
        merged_high,
        merged_low,
        output_high,
        biases[0:1, :],
        biases[1:2, :],
    )
    hidden = silu(self_near[...] + pick(match[...], part))
    wait(load_refine_high, load_refine_low)
    change = norm_centred(dot3(hidden, refine_high[...], refine_low[...]) + biases[2:3, :])
    wait(load_normed, load_firsts, load_base)
    high, low = split(change - normed[...])
    number = out.shape[0]
    chunk = number // 2
    stores = []
    for first in range(0, number, chunk):
        at = pl.ds(first, chunk)
        out[at, :] = base[at, :] + (dot(firsts[at, :], high) + dot(firsts[at, :], low))
        stores.append(copies.start(out.at[at], out_ref.at[at]))
    wait(*stores)


def flat(dims, kind=F32):
    return jax.ShapeDtypeStruct(dims, kind)


def call(
    kernel, name, flops, scalars, small, kept, large, results, held=(), scratch=(), direct=()
):
    direct = [pltpu.with_memory_space_constraint(array, pltpu.HBM) for array in direct]
    kept = [pltpu.with_memory_space_constraint(array, pltpu.VMEM) for array in kept]
    large = [pltpu.with_memory_space_constraint(array, pltpu.HBM) for array in large]
    twins = [pltpu.VMEM(array.shape, array.dtype) for array in [*large, *results]]
    twins += list(scratch)
    size = sum(4 * spec.inner_aval.size for spec in twins)
    return pl.pallas_call(
        kernel,
        out_shape=[pltpu.VMEM(array.shape, array.dtype) for array in held]
        + [pltpu.HBM(array.shape, array.dtype) for array in results],
        in_specs=[SMEM] * len(scalars)
        + [VMEM] * (len(small) + len(kept))
        + [HBM] * (len(direct) + len(large)),
        out_specs=[VMEM] * len(held) + [HBM] * len(results),
        scratch_shapes=[
            *twins,
            pltpu.SemaphoreType.DMA((len(direct) + len(large) + len(results) + 8,)),
        ],
        cost_estimate=pl.CostEstimate(flops=flops, bytes_accessed=4 * 2**20, transcendentals=0),
        compiler_params=pltpu.CompilerParams(vmem_limit_bytes=size + 12 * 2**20),
        name=name,
    )(*scalars, *small, *kept, *direct, *large)


def exchange(rows, patches):
    blocks = rows.reshape(patches, -1, rows.shape[1])
    blocks = lax.all_to_all(blocks, ("lat", "lon"), split_axis=0, concat_axis=0, tiled=True)
    return blocks.reshape(rows.shape)


def per_device(
    grid_latent,
    mesh_latent,
    grid_senders,
    grid_targets,
    grid_geometry,
    mesh_senders,
    mesh_targets,
    mesh_geometry,
    encoder_sender,
    encoder_receiver,
    encoder_geometry,
    encoder_bias,
    encoder_output,
    encoder_outbias,
    update_self,
    update_summed,
    update_bias,
    update_output,
    update_outbias,
    process_sender,
    process_receiver,
    process_geometry,
    process_bias,
    process_output,
    process_outbias,
    refine_self,
    refine_summed,
    refine_bias,
    refine_output,
    refine_outbias,
):
    number, width = mesh_latent.shape
    patches = grid_senders.shape[1]
    grid_slots = grid_targets.shape[1]
    mesh_slots = mesh_targets.shape[1]
    rows_in, columns_in = grid_latent.shape[:2]
    square = 2 * width * width
    row = lambda bias: bias.reshape(1, width)
    halves = [flat((width, width), BF16)] * 2

    cells = grid_latent.transpose(1, 0, 2).reshape(rows_in * columns_in, width)
    (packed,) = call(
        functools.partial(pack_kernel, rows_in, columns_in),
        "pack",
        1000,
        [],
        [],
        [],
        [cells],
        [flat((grid_slots, width))],
        scratch=[
            pltpu.VMEM((grid_slots // patches, patches), jnp.int32),
            pltpu.SMEM((grid_slots // patches, patches), jnp.int32),
        ],
        direct=[grid_senders[0].T],
    )
    grid_in = exchange(packed, patches)

    (
        *first,
        self_all,
        self_sent,
        nodes_sent,
        match,
        first_low,
        onward_high,
        onward_low,
        update_high,
        update_low,
        merged_high,
        merged_low,
        second_high,
        refine_high,
        refine_low,
        biases,
    ) = call(
        before_kernel,
        "before",
        (number + grid_slots) * square * 3,
        [grid_targets, mesh_senders[0].T],
        [
            grid_targets,
            grid_geometry,
            encoder_geometry,
            row(encoder_bias),
            row(update_bias),
            row(encoder_outbias),
            row(update_outbias),
            row(process_outbias),
            row(refine_outbias),
        ],
        [],
        [
            mesh_latent,
            update_self,
            encoder_receiver,
            encoder_output,
            update_summed,
            encoder_sender,
            update_output,
            process_sender,
            process_output,
            refine_summed,
            refine_output,
        ],
        [
            flat((number, width)),
            flat((mesh_slots, width)),
            flat((mesh_slots, width)),
            flat((mesh_slots, grid_slots), BF16),
        ]
        + halves * 5
        + [flat((8, width))],
        halves * 2 + [flat((grid_slots, width)), flat((8, width))],
        [
            pltpu.VMEM((grid_slots, width), F32),
            pltpu.VMEM((mesh_slots, width), F32),
            pltpu.VMEM((number, grid_slots), F32),
            pltpu.VMEM((mesh_slots, grid_slots), F32),
        ],
    )
    sent, parts = call(
        encode_kernel,
        "encode",
        (3 * grid_slots + mesh_slots) * square * 3,
        [],
        [],
        [grid_in, *first],
        [first_low, match, self_sent, onward_high, onward_low, update_high, nodes_sent],
        [flat((mesh_slots, width)), flat((grid_slots, width))],
    )
    mesh_in = exchange(sent, patches)
    *first, normed, base, firsts = call(
        between_kernel,
        "between",
        (3 * number + mesh_slots) * square * 3,
        [mesh_targets],
        [
            grid_targets,
            mesh_targets,
            mesh_geometry,
            process_geometry,
            row(process_bias),
            row(refine_bias),
            row(update_outbias),
            row(refine_outbias),
        ],
        [],
        [
            parts,
            self_all,
            mesh_latent,
            update_high,
            update_low,
            refine_self,
            process_receiver,
            refine_high,
            refine_low,
        ],
        [
            flat((mesh_slots, width)),
            flat((number, width)),
            flat((number, mesh_slots), BF16),
        ],
        [
            *halves,
            halves[0],
            flat((mesh_slots, width)),
            flat((mesh_slots, width)),
            flat((mesh_slots, mesh_slots), BF16),
            flat((8, width)),
        ],
        [
            pltpu.VMEM((mesh_slots, width), F32),
            pltpu.VMEM((number, width), F32),
            pltpu.VMEM((number, width), F32),
            pltpu.VMEM((number, width), F32),
            pltpu.VMEM((number + 8, mesh_slots), F32),
            pltpu.VMEM((mesh_slots, mesh_slots), F32),
        ],
        [merged_high, merged_low, second_high, biases],
    )
    (out,) = call(
        refine_kernel,
        "refine",
        4 * mesh_slots * square * 3,
        [],
        [],
        [mesh_in, *first],
        [
            refine_high,
            refine_low,
            normed,
            firsts,
            base,
        ],
        [flat((number, width))],
    )
    return out


def solution(mesh):
    patch = P(("lat", "lon"), None)
    block = P(("lat", "lon"), None, None)
    feature = P(None, ("lat", "lon"), None)
    return jax.shard_map(
        per_device,
        mesh=mesh,
        in_specs=(P("lat", "lon", None), patch, block, patch, feature, block, patch, feature)
        + (P(),) * 22,
        out_specs=patch,
        check_vma=False,
    )
```

```python
import functools

import jax
import jax.numpy as jnp
from jax import lax
from jax.experimental import pallas as pl
from jax.experimental.pallas import tpu as pltpu
from jax.sharding import PartitionSpec as P

F32 = jnp.float32
BF16 = jnp.bfloat16
VMEM = pl.BlockSpec(memory_space=pltpu.VMEM)
HBM = pl.BlockSpec(memory_space=pltpu.HBM)


def split(values):
    high = values.astype(BF16)
    low = (values - high.astype(F32)).astype(BF16)
    return high, low


def dot(left, right):
    return jnp.dot(left, right, preferred_element_type=F32)


def dot3(left, high, low):
    left_high, left_low = split(left)
    return dot(left_high, high) + (dot(left_low, high) + dot(left_high, low))


def pick(one_hot, values):
    high, low = split(values)
    return dot(one_hot, high) + dot(one_hot, low)


def silu(values):
    half = 0.5 * values
    return half + half * jnp.tanh(half)


def centre(values):
    return values - jnp.mean(values, axis=-1, keepdims=True)


def scale(centred):
    return lax.rsqrt(jnp.mean(centred * centred, axis=-1, keepdims=True) + 1e-05)


def norm_centred(centred):
    return centred * scale(centred)


def gather_rows(first, count, row_of, pairs, unroll=16):
    def step(i, carry):
        row = row_of(i)
        for source, target in pairs:
            target[pl.ds(i, 1), :] = source[pl.ds(row, 1), :]
        return carry

    if count <= 256:
        for i in range(first, first + count):
            step(i, 0)
    else:
        lax.fori_loop(first, first + count, step, 0, unroll=unroll)


def geometry_rows(geometry_ref, weight_ref):
    features, _, slots = geometry_ref.shape
    rows = jnp.concatenate([geometry_ref[k] for k in range(features)], axis=0)
    padded = jnp.concatenate([rows, jnp.zeros((8 - features % 8, slots), F32)], axis=0)
    columns = padded.T
    total = columns[:, 0:1] * weight_ref[0:1, :]
    for k in range(1, features):
        total += columns[:, k : k + 1] * weight_ref[k : k + 1, :]
    return total


def target_matrix(number, targets_ref):
    slots = targets_ref.shape[1]
    nodes = lax.broadcasted_iota(jnp.int32, (number, slots), 0)
    return jnp.where(nodes == targets_ref[...], 1.0, 0.0).astype(F32)


def slot_order(index_ref):
    capacity = index_ref.shape[0]
    bits = capacity.bit_length() - 1
    assert capacity == 1 << bits
    return lambda i: index_ref[i & (capacity - 1), i >> bits]


class Copies:
    def __init__(self, semaphores):
        self.semaphores = semaphores
        self.used = 0

    def start(self, source, target):
        copy = pltpu.make_async_copy(source, target, self.semaphores.at[self.used])
        self.used += 1
        copy.start()
        return copy


def wait(*copies):
    for copy in copies:
        copy.wait()


def started():
    pl.delay(1)


def pack_kernel(
    rows_in,
    columns_in,
    senders_ref,
    cells_ref,
    out_ref,
    cells,
    out,
    senders,
    senders_s,
    semaphores,
):
    copies = Copies(semaphores)
    load_senders = copies.start(senders_ref, senders)
    load_cells = copies.start(cells_ref, cells)
    shift = 20
    factor = -(-(1 << shift) // columns_in)
    assert all((i * factor) >> shift == i // columns_in for i in range(rows_in * columns_in))
    wait(load_senders)
    cell = senders[...]
    row = (cell * factor) >> shift
    senders[...] = (cell - row * columns_in) * rows_in + row
    wait(copies.start(senders, senders_s), load_cells)
    chunk = out.shape[0] // 2
    stores = []
    for first in range(0, out.shape[0], chunk):
        gather_rows(first, chunk, slot_order(senders_s), [(cells, out)])
        at = pl.ds(first, chunk)
        stores.append(copies.start(out.at[at], out_ref.at[at]))
        started()
    wait(*stores)


def rows_of(*biases):
    width = biases[0].shape[1]
    return jnp.concatenate([*biases, jnp.zeros((8 - len(biases), width), F32)], axis=0)


def before_kernel(
    grid_targets_s,
    mesh_senders_s,
    grid_targets,
    geometry,
    weight_geometry,
    edge_bias,
    node_bias,
    output_bias,
    update_bias,
    output_bias_2,
    refine_bias,
    nodes_ref,
    weight_self_ref,
    weight_receiver_ref,
    output_ref,
    summed_ref,
    sender_ref,
    update_ref,
    sender_ref_2,
    output_ref_2,
    summed_ref_2,
    refine_ref,
    sender_high,
    sender_low,
    merged_high,
    output_high,
    received,
    biases,
    self_all_ref,
    self_sent_ref,
    nodes_sent_ref,
    match_ref,
    merged_low_ref,
    onward_high_ref,
    onward_low_ref,
    update_high_ref,
    update_low_ref,
    merged_high_ref_2,
    merged_low_ref_2,
    output_high_ref_2,
    refine_high_ref,
    refine_low_ref,
    biases_ref_2,
    nodes,
    weight_self,
    weight_receiver,
    output,
    summed,
    sender,
    update,
    sender_2,
    output_2,
    summed_2,
    refine,
    self_all,
    self_sent,
    nodes_sent,
    match,
    merged_low,
    onward_high,
    onward_low,
    update_high,
    update_low,
    merged_high_2,
    merged_low_2,
    output_high_2,
    refine_high,
    refine_low,
    biases_2,
    near,
    picked,
    table,
    chosen,
    semaphores,
    pending,
):
    copies = Copies(semaphores)
    load_nodes = copies.start(nodes_ref, nodes)
    load_self = copies.start(weight_self_ref, weight_self)
    load_output = copies.start(output_ref, output)
    load_summed = copies.start(summed_ref, summed)
    load_receiver = copies.start(weight_receiver_ref, weight_receiver)
    load_sender = copies.start(sender_ref, sender)
    load_update = copies.start(update_ref, update)
    load_sender_2 = copies.start(sender_ref_2, sender_2)
    load_output_2 = copies.start(output_ref_2, output_2)
    load_summed_2 = copies.start(summed_ref_2, summed_2)
    load_refine = copies.start(refine_ref, refine)
    started()
    wait(*pending)
    stores = []

    def store(*pairs):
        stores.extend(copies.start(source, target) for source, target in pairs)

    table[...] = target_matrix(nodes.shape[0], grid_targets)
    wait(load_nodes, load_self)
    self_all[...] = dot3(nodes[...], *split(weight_self[...])) + node_bias[...]
    store((self_all, self_all_ref))
    gather_rows(
        0,
        picked.shape[0],
        slot_order(mesh_senders_s),
        [(nodes, picked), (self_all, self_sent), (table, chosen)],
    )
    match[...] = chosen[...].astype(BF16)
    store((self_sent, self_sent_ref), (match, match_ref))
    wait(load_output, load_summed)
    centred = centre(output[...])
    high, low = split(summed[...])
    merged_high[...], merged_low[...] = split(dot3(centred, high, low))
    output_high[...] = centred.astype(BF16)
    store((merged_low, merged_low_ref))
    first_bias = centre(output_bias[...])
    first_bias_on = dot3(rows_of(first_bias), high, low)[0:1, :]
    gather_rows(
        0, near.shape[0], lambda i: jnp.maximum(grid_targets_s[0, i], 0), [(nodes, near)]
    )
    wait(load_receiver)
    received[...] = (
        dot3(near[...], *split(weight_receiver[...]))
        + geometry_rows(geometry, weight_geometry)
        + edge_bias[...]
    )
    wait(load_sender)
    sender_high[...], sender_low[...] = split(sender[...])
    wait(load_update, load_sender_2)
    centred = centre(update[...])
    update_high[...], update_low[...] = split(centred)
    high, low = split(sender_2[...])
    onward_high[...], onward_low[...] = split(dot3(centred, high, low))
    nodes_sent[...] = dot3(picked[...], high, low)
    store(
        (update_high, update_high_ref),
        (update_low, update_low_ref),
        (onward_high, onward_high_ref),
        (onward_low, onward_low_ref),
        (nodes_sent, nodes_sent_ref),
    )
    second_bias = centre(update_bias[...])
    second_bias_on = dot3(rows_of(second_bias), high, low)[0:1, :]
    biases[...] = rows_of(first_bias, first_bias_on, second_bias, second_bias_on)
    wait(load_output_2, load_summed_2, load_refine)
    centred = centre(output_2[...])
    high, low = split(summed_2[...])
    merged_high_2[...], merged_low_2[...] = split(dot3(centred, high, low))
    output_high_2[...] = centred.astype(BF16)
    third_bias = centre(output_bias_2[...])
    third_bias_on = dot3(rows_of(third_bias), high, low)[0:1, :]
    biases_2[...] = rows_of(third_bias, third_bias_on, centre(refine_bias[...]))
    refine_high[...], refine_low[...] = split(centre(refine[...]))
    store(
        (merged_high_2, merged_high_ref_2),
        (merged_low_2, merged_low_ref_2),
        (output_high_2, output_high_ref_2),
        (refine_high, refine_high_ref),
        (refine_low, refine_low_ref),
        (biases_2, biases_ref_2),
    )
    wait(*stores)


def edges(hidden, merged_high, merged_low, output_high, bias, bias_on, load_low=()):
    hidden_high, hidden_low = split(hidden)
    normed = scale(dot(hidden_high, output_high[...]) + bias)
    high = merged_high[...]
    total = dot(hidden_high, high) + dot(hidden_low, high)
    wait(*load_low)
    return (total + dot(hidden_high, merged_low[...]) + bias_on) * normed


def encode_kernel(
    arrived,
    sender_high,
    sender_low,
    merged_high,
    output_high,
    received,
    biases,
    merged_low_ref,
    match_ref,
    self_sent_ref,
    onward_high_ref,
    onward_low_ref,
    update_high_ref,
    nodes_sent_ref,
    sent_ref,
    parts_ref,
    merged_low,
    match,
    self_sent,
    onward_high,
    onward_low,
    update_high,
    nodes_sent,
    sent,
    parts,
    semaphores,
):
    copies = Copies(semaphores)
    load_merged = copies.start(merged_low_ref, merged_low)
    load_match = copies.start(match_ref, match)
    load_self = copies.start(self_sent_ref, self_sent)
    load_onward_high = copies.start(onward_high_ref, onward_high)
    load_onward_low = copies.start(onward_low_ref, onward_low)
    load_update = copies.start(update_high_ref, update_high)
    load_nodes = copies.start(nodes_sent_ref, nodes_sent)
    started()
    hidden = silu(dot3(arrived[...], sender_high[...], sender_low[...]) + received[...])
    part = edges(
        hidden, merged_high, merged_low, output_high, biases[0:1, :], biases[1:2, :], [load_merged]
    )
    parts[...] = part
    store_parts = copies.start(parts, parts_ref)
    wait(load_match, load_self)
    hidden = silu(self_sent[...] + pick(match[...], part))
    wait(load_onward_high, load_update)
    sent[...] = (
        edges(
            hidden,
            onward_high,
            onward_low,
            update_high,
            biases[2:3, :],
            biases[3:4, :],
            [load_onward_low, load_nodes],
        )
        + nodes_sent[...]
    )
    store_sent = copies.start(sent, sent_ref)
    wait(store_parts, store_sent)


def between_kernel(
    mesh_targets_s,
    grid_targets,
    mesh_targets,
    geometry,
    weight_geometry,
    edge_bias,
    node_bias,
    update_bias,
    refine_bias,
    merged_high_ref,
    merged_low_ref,
    output_high_ref,
    biases_ref,
    parts_ref,
    self_all_ref,
    nodes_ref,
    update_high_ref,
    update_low_ref,
    weight_self_ref,
    weight_receiver_ref,
    refine_high_ref,
    refine_low_ref,
    merged_high,
    merged_low,
    output_high,
    received,
    self_near,
    match,
    biases,
    normed_ref,
    base_ref,
    firsts_ref,
    parts,
    self_all,
    nodes,
    update_high,
    update_low,
    weight_self,
    weight_receiver,
    refine_high,
    refine_low,
    normed_near,
    base,
    firsts,
    near,
    encoded,
    self_next,
    normed,
    table,
    chosen,
    semaphores,
    pending,
):
    copies = Copies(semaphores)
    load_parts = copies.start(parts_ref, parts)
    load_all = copies.start(self_all_ref, self_all)
    load_update_high = copies.start(update_high_ref, update_high)
    load_update_low = copies.start(update_low_ref, update_low)
    load_nodes = copies.start(nodes_ref, nodes)
    load_self = copies.start(weight_self_ref, weight_self)
    load_receiver = copies.start(weight_receiver_ref, weight_receiver)
    load_refine_high = copies.start(refine_high_ref, refine_high)
    load_refine_low = copies.start(refine_low_ref, refine_low)
    passed = [
        copies.start(merged_high_ref, merged_high),
        copies.start(merged_low_ref, merged_low),
        copies.start(output_high_ref, output_high),
        copies.start(biases_ref, biases),
    ]
    started()
    wait(*pending)
    stores = []
    one_hot = target_matrix(nodes.shape[0], grid_targets).astype(BF16)
    table[...] = target_matrix(table.shape[0], mesh_targets)
    number = nodes.shape[0]

    def node_or_empty(i):
        target = mesh_targets_s[0, i]
        return jnp.where(target < 0, number, target)

    wait(load_parts, load_all)
    hidden = silu(self_all[...] + pick(one_hot, parts[...]))
    wait(load_update_high, load_update_low, load_nodes)
    encoded[...] = nodes[...] + norm_centred(
        dot3(hidden, update_high[...], update_low[...]) + centre(update_bias[...])
    )
    wait(load_self)
    self_next[...] = dot3(encoded[...], *split(weight_self[...])) + node_bias[...]
    wait(load_refine_high, load_refine_low)
    normed[...] = norm_centred(
        dot3(silu(self_next[...]), refine_high[...], refine_low[...]) + centre(refine_bias[...])
    )
    base[...] = encoded[...] + normed[...]
    stores.append(copies.start(base, base_ref))
    gather_rows(
        0,
        near.shape[0],
        lambda i: jnp.maximum(mesh_targets_s[0, i], 0),
        [(encoded, near), (self_next, self_near), (normed, normed_near)],
    )
    gather_rows(0, near.shape[0], node_or_empty, [(table, chosen)])
    slots = near.shape[0]
    same = chosen[...]
    match[...] = same.astype(BF16)
    earlier = lax.broadcasted_iota(jnp.int32, (slots, slots), 0) < lax.broadcasted_iota(
        jnp.int32, (slots, slots), 1
    )
    repeats = jnp.sum(jnp.where(earlier, same, 0.0), axis=0, keepdims=True)
    firsts[...] = jnp.where(repeats == 0.0, table[0:number, :], 0.0).astype(BF16)
    stores.append(copies.start(normed_near, normed_ref))
    stores.append(copies.start(firsts, firsts_ref))
    wait(load_receiver)
    received[...] = (
        dot3(near[...], *split(weight_receiver[...]))
        + geometry_rows(geometry, weight_geometry)
        + edge_bias[...]
    )
    wait(*passed, *stores)


def refine_kernel(
    arrived,
    merged_high,
    merged_low,
    output_high,
    received,
    self_near,
    match,
    biases,
    refine_high_ref,
    refine_low_ref,
    normed_ref,
    firsts_ref,
    base_ref,
    out_ref,
    refine_high,
    refine_low,
    normed,
    firsts,
    base,
    out,
    semaphores,
):
    copies = Copies(semaphores)
    load_refine_high = copies.start(refine_high_ref, refine_high)
    load_refine_low = copies.start(refine_low_ref, refine_low)
    load_normed = copies.start(normed_ref, normed)
    load_firsts = copies.start(firsts_ref, firsts)
    load_base = copies.start(base_ref, base)
    started()
    part = edges(
        silu(arrived[...] + received[...]),
        merged_high,
        merged_low,
        output_high,
        biases[0:1, :],
        biases[1:2, :],
    )
    hidden = silu(self_near[...] + pick(match[...], part))
    wait(load_refine_high, load_refine_low)
    change = norm_centred(dot3(hidden, refine_high[...], refine_low[...]) + biases[2:3, :])
    wait(load_normed, load_firsts, load_base)
    high, low = split(change - normed[...])
    number = out.shape[0]
    chunk = number // 2
    stores = []
    for first in range(0, number, chunk):
        at = pl.ds(first, chunk)
        out[at, :] = base[at, :] + (dot(firsts[at, :], high) + dot(firsts[at, :], low))
        stores.append(copies.start(out.at[at], out_ref.at[at]))
    wait(*stores)


def flat(dims, kind=F32):
    return jax.ShapeDtypeStruct(dims, kind)


def call(
    kernel, name, flops, scalars, small, kept, large, results, held=(), scratch=(), direct=()
):
    hbm = lambda arrays: [pltpu.with_memory_space_constraint(x, pltpu.HBM) for x in arrays]
    ahead = hbm([*scalars, *small])
    kept = [pltpu.with_memory_space_constraint(array, pltpu.VMEM) for array in kept]
    direct = hbm(direct)
    large = hbm(large)
    landing = [pltpu.SMEM(x.shape, x.dtype) for x in scalars]
    landing += [pltpu.VMEM(x.shape, x.dtype) for x in small]
    twins = [pltpu.VMEM(array.shape, array.dtype) for array in [*large, *results]]
    twins += list(scratch)
    size = sum(4 * spec.inner_aval.size for spec in twins)
    count = len(ahead)

    def with_pending(*refs):
        *landed, semaphores = refs[len(refs) - count - 1 :]
        copies = Copies(semaphores)
        pending = [copies.start(*pair) for pair in zip(refs[:count], landed, strict=True)]
        kernel(*landed, *refs[count : len(refs) - count - 1], pending)

    if count:
        landing.append(pltpu.SemaphoreType.DMA((count,)))
    return pl.pallas_call(
        with_pending if count else kernel,
        out_shape=[pltpu.VMEM(array.shape, array.dtype) for array in held]
        + [pltpu.HBM(array.shape, array.dtype) for array in results],
        in_specs=[HBM] * count + [VMEM] * len(kept) + [HBM] * (len(direct) + len(large)),
        out_specs=[VMEM] * len(held) + [HBM] * len(results),
        scratch_shapes=[
            *twins,
            pltpu.SemaphoreType.DMA((len(direct) + len(large) + len(results) + 8,)),
            *landing,
        ],
        cost_estimate=pl.CostEstimate(flops=flops, bytes_accessed=4 * 2**20, transcendentals=0),
        compiler_params=pltpu.CompilerParams(vmem_limit_bytes=size + 12 * 2**20),
        name=name,
    )(*ahead, *kept, *direct, *large)


def exchange(rows, patches):
    blocks = rows.reshape(patches, -1, rows.shape[1])
    blocks = lax.all_to_all(blocks, ("lat", "lon"), split_axis=0, concat_axis=0, tiled=True)
    return blocks.reshape(rows.shape)


def per_device(
    grid_latent,
    mesh_latent,
    grid_senders,
    grid_targets,
    grid_geometry,
    mesh_senders,
    mesh_targets,
    mesh_geometry,
    encoder_sender,
    encoder_receiver,
    encoder_geometry,
    encoder_bias,
    encoder_output,
    encoder_outbias,
    update_self,
    update_summed,
    update_bias,
    update_output,
    update_outbias,
    process_sender,
    process_receiver,
    process_geometry,
    process_bias,
    process_output,
    process_outbias,
    refine_self,
    refine_summed,
    refine_bias,
    refine_output,
    refine_outbias,
):
    number, width = mesh_latent.shape
    patches = grid_senders.shape[1]
    grid_slots = grid_targets.shape[1]
    mesh_slots = mesh_targets.shape[1]
    rows_in, columns_in = grid_latent.shape[:2]
    square = 2 * width * width
    row = lambda bias: bias.reshape(1, width)
    halves = [flat((width, width), BF16)] * 2

    cells = grid_latent.transpose(1, 0, 2).reshape(rows_in * columns_in, width)
    (packed,) = call(
        functools.partial(pack_kernel, rows_in, columns_in),
        "pack",
        1000,
        [],
        [],
        [],
        [cells],
        [flat((grid_slots, width))],
        scratch=[
            pltpu.VMEM((grid_slots // patches, patches), jnp.int32),
            pltpu.SMEM((grid_slots // patches, patches), jnp.int32),
        ],
        direct=[grid_senders[0].T],
    )
    grid_in = exchange(packed, patches)

    (
        *first,
        self_all,
        self_sent,
        nodes_sent,
        match,
        first_low,
        onward_high,
        onward_low,
        update_high,
        update_low,
        merged_high,
        merged_low,
        second_high,
        refine_high,
        refine_low,
        biases,
    ) = call(
        before_kernel,
        "before",
        (number + grid_slots) * square * 3,
        [grid_targets, mesh_senders[0].T],
        [
            grid_targets,
            grid_geometry,
            encoder_geometry,
            row(encoder_bias),
            row(update_bias),
            row(encoder_outbias),
            row(update_outbias),
            row(process_outbias),
            row(refine_outbias),
        ],
        [],
        [
            mesh_latent,
            update_self,
            encoder_receiver,
            encoder_output,
            update_summed,
            encoder_sender,
            update_output,
            process_sender,
            process_output,
            refine_summed,
            refine_output,
        ],
        [
            flat((number, width)),
            flat((mesh_slots, width)),
            flat((mesh_slots, width)),
            flat((mesh_slots, grid_slots), BF16),
        ]
        + halves * 5
        + [flat((8, width))],
        halves * 2 + [flat((grid_slots, width)), flat((8, width))],
        [
            pltpu.VMEM((grid_slots, width), F32),
            pltpu.VMEM((mesh_slots, width), F32),
            pltpu.VMEM((number, grid_slots), F32),
            pltpu.VMEM((mesh_slots, grid_slots), F32),
        ],
    )
    sent, parts = call(
        encode_kernel,
        "encode",
        (3 * grid_slots + mesh_slots) * square * 3,
        [],
        [],
        [grid_in, *first],
        [first_low, match, self_sent, onward_high, onward_low, update_high, nodes_sent],
        [flat((mesh_slots, width)), flat((grid_slots, width))],
    )
    mesh_in = exchange(sent, patches)
    *first, normed, base, firsts = call(
        between_kernel,
        "between",
        (3 * number + mesh_slots) * square * 3,
        [mesh_targets],
        [
            grid_targets,
            mesh_targets,
            mesh_geometry,
            process_geometry,
            row(process_bias),
            row(refine_bias),
            row(update_outbias),
            row(refine_outbias),
        ],
        [],
        [
            parts,
            self_all,
            mesh_latent,
            update_high,
            update_low,
            refine_self,
            process_receiver,
            refine_high,
            refine_low,
        ],
        [
            flat((mesh_slots, width)),
            flat((number, width)),
            flat((number, mesh_slots), BF16),
        ],
        [
            *halves,
            halves[0],
            flat((mesh_slots, width)),
            flat((mesh_slots, width)),
            flat((mesh_slots, mesh_slots), BF16),
            flat((8, width)),
        ],
        [
            pltpu.VMEM((mesh_slots, width), F32),
            pltpu.VMEM((number, width), F32),
            pltpu.VMEM((number, width), F32),
            pltpu.VMEM((number, width), F32),
            pltpu.VMEM((number + 8, mesh_slots), F32),
            pltpu.VMEM((mesh_slots, mesh_slots), F32),
        ],
        [merged_high, merged_low, second_high, biases],
    )
    (out,) = call(
        refine_kernel,
        "refine",
        4 * mesh_slots * square * 3,
        [],
        [],
        [mesh_in, *first],
        [
            refine_high,
            refine_low,
            normed,
            firsts,
            base,
        ],
        [flat((number, width))],
    )
    return out


def solution(mesh):
    patch = P(("lat", "lon"), None)
    block = P(("lat", "lon"), None, None)
    feature = P(None, ("lat", "lon"), None)
    return jax.shard_map(
        per_device,
        mesh=mesh,
        in_specs=(P("lat", "lon", None), patch, block, patch, feature, block, patch, feature)
        + (P(),) * 22,
        out_specs=patch,
        check_vma=False,
    )
```

```python
import functools

import jax
import jax.numpy as jnp
from jax import lax
from jax.experimental import pallas as pl
from jax.experimental.pallas import tpu as pltpu
from jax.sharding import PartitionSpec as P

F32 = jnp.float32
BF16 = jnp.bfloat16
VMEM = pl.BlockSpec(memory_space=pltpu.VMEM)
HBM = pl.BlockSpec(memory_space=pltpu.HBM)


def split(values):
    high = values.astype(BF16)
    low = (values - high.astype(F32)).astype(BF16)
    return high, low


def dot(left, right):
    return jnp.dot(left, right, preferred_element_type=F32)


def dot3(left, high, low):
    left_high, left_low = split(left)
    return dot(left_high, high) + (dot(left_low, high) + dot(left_high, low))


def pick(one_hot, values):
    high, low = split(values)
    return dot(one_hot, high) + dot(one_hot, low)


def silu(values):
    half = 0.5 * values
    return half + half * jnp.tanh(half)


def centre(values):
    return values - jnp.mean(values, axis=-1, keepdims=True)


def scale(centred):
    return lax.rsqrt(jnp.mean(centred * centred, axis=-1, keepdims=True) + 1e-05)


def norm_centred(centred):
    return centred * scale(centred)


def gather_rows(first, count, row_of, pairs, unroll=16):
    def step(i, carry):
        row = row_of(i)
        for source, target in pairs:
            target[pl.ds(i, 1), :] = source[pl.ds(row, 1), :]
        return carry

    if count <= 256:
        for i in range(first, first + count):
            step(i, 0)
    else:
        lax.fori_loop(first, first + count, step, 0, unroll=unroll)


def geometry_rows(geometry_ref, weight_ref):
    features, _, slots = geometry_ref.shape
    rows = jnp.concatenate([geometry_ref[k] for k in range(features)], axis=0)
    padded = jnp.concatenate([rows, jnp.zeros((8 - features % 8, slots), F32)], axis=0)
    columns = padded.T
    total = columns[:, 0:1] * weight_ref[0:1, :]
    for k in range(1, features):
        total += columns[:, k : k + 1] * weight_ref[k : k + 1, :]
    return total


def target_matrix(number, targets_ref):
    slots = targets_ref.shape[1]
    nodes = lax.broadcasted_iota(jnp.int32, (number, slots), 0)
    return jnp.where(nodes == targets_ref[...], 1.0, 0.0).astype(F32)


def slot_order(index_ref):
    capacity = index_ref.shape[0]
    bits = capacity.bit_length() - 1
    assert capacity == 1 << bits
    return lambda i: index_ref[i & (capacity - 1), i >> bits]


class Copies:
    def __init__(self, semaphores):
        self.semaphores = semaphores
        self.used = 0

    def start(self, source, target):
        copy = pltpu.make_async_copy(source, target, self.semaphores.at[self.used])
        self.used += 1
        copy.start()
        return copy


def wait(*copies):
    for copy in copies:
        copy.wait()


def started():
    pl.delay(1)


def pack_kernel(
    rows_in,
    columns_in,
    senders_ref,
    cells_ref,
    out_ref,
    cells,
    out,
    senders,
    senders_s,
    semaphores,
):
    copies = Copies(semaphores)
    load_senders = copies.start(senders_ref, senders)
    load_cells = copies.start(cells_ref, cells)
    shift = 20
    factor = -(-(1 << shift) // columns_in)
    assert all((i * factor) >> shift == i // columns_in for i in range(rows_in * columns_in))
    wait(load_senders)
    cell = senders[...]
    row = (cell * factor) >> shift
    senders[...] = (cell - row * columns_in) * rows_in + row
    wait(copies.start(senders, senders_s), load_cells)
    chunk = out.shape[0] // 2
    stores = []
    for first in range(0, out.shape[0], chunk):
        gather_rows(first, chunk, slot_order(senders_s), [(cells, out)])
        at = pl.ds(first, chunk)
        stores.append(copies.start(out.at[at], out_ref.at[at]))
        started()
    wait(*stores)


def rows_of(*biases):
    width = biases[0].shape[1]
    return jnp.concatenate([*biases, jnp.zeros((8 - len(biases), width), F32)], axis=0)


def before_kernel(
    grid_targets_s,
    mesh_senders_s,
    grid_targets,
    geometry,
    weight_geometry,
    edge_bias,
    node_bias,
    output_bias,
    update_bias,
    output_bias_2,
    refine_bias,
    nodes_ref,
    weight_self_ref,
    weight_receiver_ref,
    output_ref,
    summed_ref,
    sender_ref,
    update_ref,
    sender_ref_2,
    output_ref_2,
    summed_ref_2,
    refine_ref,
    sender_high,
    sender_low,
    merged_high,
    output_high,
    received,
    biases,
    self_all_ref,
    self_sent_ref,
    nodes_sent_ref,
    match_ref,
    merged_low_ref,
    onward_high_ref,
    onward_low_ref,
    update_high_ref,
    update_low_ref,
    merged_high_ref_2,
    merged_low_ref_2,
    output_high_ref_2,
    refine_high_ref,
    refine_low_ref,
    biases_ref_2,
    nodes,
    weight_self,
    weight_receiver,
    output,
    summed,
    sender,
    update,
    sender_2,
    output_2,
    summed_2,
    refine,
    self_all,
    self_sent,
    nodes_sent,
    match,
    merged_low,
    onward_high,
    onward_low,
    update_high,
    update_low,
    merged_high_2,
    merged_low_2,
    output_high_2,
    refine_high,
    refine_low,
    biases_2,
    near,
    picked,
    table,
    chosen,
    semaphores,
    pending,
):
    copies = Copies(semaphores)
    load_nodes = copies.start(nodes_ref, nodes)
    load_self = copies.start(weight_self_ref, weight_self)
    load_output = copies.start(output_ref, output)
    load_summed = copies.start(summed_ref, summed)
    load_receiver = copies.start(weight_receiver_ref, weight_receiver)
    load_sender = copies.start(sender_ref, sender)
    load_update = copies.start(update_ref, update)
    load_sender_2 = copies.start(sender_ref_2, sender_2)
    load_output_2 = copies.start(output_ref_2, output_2)
    load_summed_2 = copies.start(summed_ref_2, summed_2)
    load_refine = copies.start(refine_ref, refine)
    started()
    stores = []

    def store(*pairs):
        stores.extend(copies.start(source, target) for source, target in pairs)

    wait(load_nodes, load_self)
    self_all[...] = dot3(nodes[...], *split(weight_self[...]))
    wait(*pending)
    self_all[...] = self_all[...] + node_bias[...]
    table[...] = target_matrix(nodes.shape[0], grid_targets)
    store((self_all, self_all_ref))
    gather_rows(
        0,
        picked.shape[0],
        slot_order(mesh_senders_s),
        [(nodes, picked), (self_all, self_sent), (table, chosen)],
    )
    match[...] = chosen[...].astype(BF16)
    store((self_sent, self_sent_ref), (match, match_ref))
    wait(load_output, load_summed)
    centred = centre(output[...])
    high, low = split(summed[...])
    merged_high[...], merged_low[...] = split(dot3(centred, high, low))
    output_high[...] = centred.astype(BF16)
    store((merged_low, merged_low_ref))
    first_bias = centre(output_bias[...])
    first_bias_on = dot3(rows_of(first_bias), high, low)[0:1, :]
    gather_rows(
        0, near.shape[0], lambda i: jnp.maximum(grid_targets_s[0, i], 0), [(nodes, near)]
    )
    wait(load_receiver)
    received[...] = (
        dot3(near[...], *split(weight_receiver[...]))
        + geometry_rows(geometry, weight_geometry)
        + edge_bias[...]
    )
    wait(load_sender)
    sender_high[...], sender_low[...] = split(sender[...])
    wait(load_update, load_sender_2)
    centred = centre(update[...])
    update_high[...], update_low[...] = split(centred)
    high, low = split(sender_2[...])
    onward_high[...], onward_low[...] = split(dot3(centred, high, low))
    nodes_sent[...] = dot3(picked[...], high, low)
    store(
        (update_high, update_high_ref),
        (update_low, update_low_ref),
        (onward_high, onward_high_ref),
        (onward_low, onward_low_ref),
        (nodes_sent, nodes_sent_ref),
    )
    second_bias = centre(update_bias[...])
    second_bias_on = dot3(rows_of(second_bias), high, low)[0:1, :]
    biases[...] = rows_of(first_bias, first_bias_on, second_bias, second_bias_on)
    wait(load_output_2, load_summed_2, load_refine)
    centred = centre(output_2[...])
    high, low = split(summed_2[...])
    merged_high_2[...], merged_low_2[...] = split(dot3(centred, high, low))
    output_high_2[...] = centred.astype(BF16)
    third_bias = centre(output_bias_2[...])
    third_bias_on = dot3(rows_of(third_bias), high, low)[0:1, :]
    biases_2[...] = rows_of(third_bias, third_bias_on, centre(refine_bias[...]))
    refine_high[...], refine_low[...] = split(centre(refine[...]))
    store(
        (merged_high_2, merged_high_ref_2),
        (merged_low_2, merged_low_ref_2),
        (output_high_2, output_high_ref_2),
        (refine_high, refine_high_ref),
        (refine_low, refine_low_ref),
        (biases_2, biases_ref_2),
    )
    wait(*stores)


def edges(hidden, merged_high, merged_low, output_high, bias, bias_on, load_low=()):
    hidden_high, hidden_low = split(hidden)
    normed = scale(dot(hidden_high, output_high[...]) + bias)
    high = merged_high[...]
    total = dot(hidden_high, high) + dot(hidden_low, high)
    wait(*load_low)
    return (total + dot(hidden_high, merged_low[...]) + bias_on) * normed


def encode_kernel(
    arrived,
    sender_high,
    sender_low,
    merged_high,
    output_high,
    received,
    biases,
    merged_low_ref,
    match_ref,
    self_sent_ref,
    onward_high_ref,
    onward_low_ref,
    update_high_ref,
    nodes_sent_ref,
    sent_ref,
    parts_ref,
    merged_low,
    match,
    self_sent,
    onward_high,
    onward_low,
    update_high,
    nodes_sent,
    sent,
    parts,
    semaphores,
):
    copies = Copies(semaphores)
    load_merged = copies.start(merged_low_ref, merged_low)
    load_match = copies.start(match_ref, match)
    load_self = copies.start(self_sent_ref, self_sent)
    load_onward_high = copies.start(onward_high_ref, onward_high)
    load_onward_low = copies.start(onward_low_ref, onward_low)
    load_update = copies.start(update_high_ref, update_high)
    load_nodes = copies.start(nodes_sent_ref, nodes_sent)
    started()
    hidden = silu(dot3(arrived[...], sender_high[...], sender_low[...]) + received[...])
    part = edges(
        hidden, merged_high, merged_low, output_high, biases[0:1, :], biases[1:2, :], [load_merged]
    )
    parts[...] = part
    store_parts = copies.start(parts, parts_ref)
    wait(load_match, load_self)
    hidden = silu(self_sent[...] + pick(match[...], part))
    wait(load_onward_high, load_update)
    sent[...] = (
        edges(
            hidden,
            onward_high,
            onward_low,
            update_high,
            biases[2:3, :],
            biases[3:4, :],
            [load_onward_low, load_nodes],
        )
        + nodes_sent[...]
    )
    store_sent = copies.start(sent, sent_ref)
    wait(store_parts, store_sent)


def between_kernel(
    mesh_targets_s,
    grid_targets,
    mesh_targets,
    geometry,
    weight_geometry,
    edge_bias,
    node_bias,
    update_bias,
    refine_bias,
    merged_high_ref,
    merged_low_ref,
    output_high_ref,
    biases_ref,
    parts_ref,
    self_all_ref,
    nodes_ref,
    update_high_ref,
    update_low_ref,
    weight_self_ref,
    weight_receiver_ref,
    refine_high_ref,
    refine_low_ref,
    merged_high,
    merged_low,
    output_high,
    received,
    self_near,
    match,
    biases,
    normed_ref,
    base_ref,
    firsts_ref,
    parts,
    self_all,
    nodes,
    update_high,
    update_low,
    weight_self,
    weight_receiver,
    refine_high,
    refine_low,
    normed_near,
    base,
    firsts,
    near,
    encoded,
    self_next,
    normed,
    table,
    chosen,
    semaphores,
    pending,
):
    copies = Copies(semaphores)
    load_parts = copies.start(parts_ref, parts)
    load_all = copies.start(self_all_ref, self_all)
    load_update_high = copies.start(update_high_ref, update_high)
    load_update_low = copies.start(update_low_ref, update_low)
    load_nodes = copies.start(nodes_ref, nodes)
    load_self = copies.start(weight_self_ref, weight_self)
    load_receiver = copies.start(weight_receiver_ref, weight_receiver)
    load_refine_high = copies.start(refine_high_ref, refine_high)
    load_refine_low = copies.start(refine_low_ref, refine_low)
    passed = [
        copies.start(merged_high_ref, merged_high),
        copies.start(merged_low_ref, merged_low),
        copies.start(output_high_ref, output_high),
        copies.start(biases_ref, biases),
    ]
    started()
    wait(*pending)
    stores = []
    one_hot = target_matrix(nodes.shape[0], grid_targets).astype(BF16)
    table[...] = target_matrix(table.shape[0], mesh_targets)
    number = nodes.shape[0]

    def node_or_empty(i):
        target = mesh_targets_s[0, i]
        return jnp.where(target < 0, number, target)

    wait(load_parts, load_all)
    hidden = silu(self_all[...] + pick(one_hot, parts[...]))
    wait(load_update_high, load_update_low, load_nodes)
    encoded[...] = nodes[...] + norm_centred(
        dot3(hidden, update_high[...], update_low[...]) + centre(update_bias[...])
    )
    wait(load_self)
    self_next[...] = dot3(encoded[...], *split(weight_self[...])) + node_bias[...]
    wait(load_refine_high, load_refine_low)
    normed[...] = norm_centred(
        dot3(silu(self_next[...]), refine_high[...], refine_low[...]) + centre(refine_bias[...])
    )
    base[...] = encoded[...] + normed[...]
    stores.append(copies.start(base, base_ref))
    gather_rows(
        0,
        near.shape[0],
        lambda i: jnp.maximum(mesh_targets_s[0, i], 0),
        [(encoded, near), (self_next, self_near), (normed, normed_near)],
    )
    gather_rows(0, near.shape[0], node_or_empty, [(table, chosen)])
    slots = near.shape[0]
    same = chosen[...]
    match[...] = same.astype(BF16)
    earlier = lax.broadcasted_iota(jnp.int32, (slots, slots), 0) < lax.broadcasted_iota(
        jnp.int32, (slots, slots), 1
    )
    repeats = jnp.sum(jnp.where(earlier, same, 0.0), axis=0, keepdims=True)
    firsts[...] = jnp.where(repeats == 0.0, table[0:number, :], 0.0).astype(BF16)
    stores.append(copies.start(normed_near, normed_ref))
    stores.append(copies.start(firsts, firsts_ref))
    wait(load_receiver)
    received[...] = (
        dot3(near[...], *split(weight_receiver[...]))
        + geometry_rows(geometry, weight_geometry)
        + edge_bias[...]
    )
    wait(*passed, *stores)


def refine_kernel(
    arrived,
    merged_high,
    merged_low,
    output_high,
    received,
    self_near,
    match,
    biases,
    refine_high_ref,
    refine_low_ref,
    normed_ref,
    firsts_ref,
    base_ref,
    out_ref,
    refine_high,
    refine_low,
    normed,
    firsts,
    base,
    out,
    semaphores,
):
    copies = Copies(semaphores)
    load_refine_high = copies.start(refine_high_ref, refine_high)
    load_refine_low = copies.start(refine_low_ref, refine_low)
    load_normed = copies.start(normed_ref, normed)
    load_firsts = copies.start(firsts_ref, firsts)
    load_base = copies.start(base_ref, base)
    started()
    part = edges(
        silu(arrived[...] + received[...]),
        merged_high,
        merged_low,
        output_high,
        biases[0:1, :],
        biases[1:2, :],
    )
    hidden = silu(self_near[...] + pick(match[...], part))
    wait(load_refine_high, load_refine_low)
    change = norm_centred(dot3(hidden, refine_high[...], refine_low[...]) + biases[2:3, :])
    wait(load_normed, load_firsts, load_base)
    high, low = split(change - normed[...])
    number = out.shape[0]
    chunk = number // 2
    stores = []
    for first in range(0, number, chunk):
        at = pl.ds(first, chunk)
        out[at, :] = base[at, :] + (dot(firsts[at, :], high) + dot(firsts[at, :], low))
        stores.append(copies.start(out.at[at], out_ref.at[at]))
    wait(*stores)


def flat(dims, kind=F32):
    return jax.ShapeDtypeStruct(dims, kind)


def call(
    kernel, name, flops, scalars, small, kept, large, results, held=(), scratch=(), direct=()
):
    hbm = lambda arrays: [pltpu.with_memory_space_constraint(x, pltpu.HBM) for x in arrays]
    ahead = hbm([*scalars, *small])
    kept = [pltpu.with_memory_space_constraint(array, pltpu.VMEM) for array in kept]
    direct = hbm(direct)
    large = hbm(large)
    landing = [pltpu.SMEM(x.shape, x.dtype) for x in scalars]
    landing += [pltpu.VMEM(x.shape, x.dtype) for x in small]
    twins = [pltpu.VMEM(array.shape, array.dtype) for array in [*large, *results]]
    twins += list(scratch)
    size = sum(4 * spec.inner_aval.size for spec in twins)
    count = len(ahead)

    def with_pending(*refs):
        *landed, semaphores = refs[len(refs) - count - 1 :]
        copies = Copies(semaphores)
        pending = [copies.start(*pair) for pair in zip(refs[:count], landed, strict=True)]
        kernel(*landed, *refs[count : len(refs) - count - 1], pending)

    if count:
        landing.append(pltpu.SemaphoreType.DMA((count,)))
    return pl.pallas_call(
        with_pending if count else kernel,
        out_shape=[pltpu.VMEM(array.shape, array.dtype) for array in held]
        + [pltpu.HBM(array.shape, array.dtype) for array in results],
        in_specs=[HBM] * count + [VMEM] * len(kept) + [HBM] * (len(direct) + len(large)),
        out_specs=[VMEM] * len(held) + [HBM] * len(results),
        scratch_shapes=[
            *twins,
            pltpu.SemaphoreType.DMA((len(direct) + len(large) + len(results) + 8,)),
            *landing,
        ],
        cost_estimate=pl.CostEstimate(flops=flops, bytes_accessed=4 * 2**20, transcendentals=0),
        compiler_params=pltpu.CompilerParams(vmem_limit_bytes=size + 12 * 2**20),
        name=name,
    )(*ahead, *kept, *direct, *large)


def exchange(rows, patches):
    blocks = rows.reshape(patches, -1, rows.shape[1])
    blocks = lax.all_to_all(blocks, ("lat", "lon"), split_axis=0, concat_axis=0, tiled=True)
    return blocks.reshape(rows.shape)


def per_device(
    grid_latent,
    mesh_latent,
    grid_senders,
    grid_targets,
    grid_geometry,
    mesh_senders,
    mesh_targets,
    mesh_geometry,
    encoder_sender,
    encoder_receiver,
    encoder_geometry,
    encoder_bias,
    encoder_output,
    encoder_outbias,
    update_self,
    update_summed,
    update_bias,
    update_output,
    update_outbias,
    process_sender,
    process_receiver,
    process_geometry,
    process_bias,
    process_output,
    process_outbias,
    refine_self,
    refine_summed,
    refine_bias,
    refine_output,
    refine_outbias,
):
    number, width = mesh_latent.shape
    patches = grid_senders.shape[1]
    grid_slots = grid_targets.shape[1]
    mesh_slots = mesh_targets.shape[1]
    rows_in, columns_in = grid_latent.shape[:2]
    square = 2 * width * width
    row = lambda bias: bias.reshape(1, width)
    halves = [flat((width, width), BF16)] * 2

    cells = grid_latent.transpose(1, 0, 2).reshape(rows_in * columns_in, width)
    (packed,) = call(
        functools.partial(pack_kernel, rows_in, columns_in),
        "pack",
        1000,
        [],
        [],
        [],
        [cells],
        [flat((grid_slots, width))],
        scratch=[
            pltpu.VMEM((grid_slots // patches, patches), jnp.int32),
            pltpu.SMEM((grid_slots // patches, patches), jnp.int32),
        ],
        direct=[grid_senders[0].T],
    )
    grid_in = exchange(packed, patches)

    (
        *first,
        self_all,
        self_sent,
        nodes_sent,
        match,
        first_low,
        onward_high,
        onward_low,
        update_high,
        update_low,
        merged_high,
        merged_low,
        second_high,
        refine_high,
        refine_low,
        biases,
    ) = call(
        before_kernel,
        "before",
        (number + grid_slots) * square * 3,
        [grid_targets, mesh_senders[0].T],
        [
            grid_targets,
            grid_geometry,
            encoder_geometry,
            row(encoder_bias),
            row(update_bias),
            row(encoder_outbias),
            row(update_outbias),
            row(process_outbias),
            row(refine_outbias),
        ],
        [],
        [
            mesh_latent,
            update_self,
            encoder_receiver,
            encoder_output,
            update_summed,
            encoder_sender,
            update_output,
            process_sender,
            process_output,
            refine_summed,
            refine_output,
        ],
        [
            flat((number, width)),
            flat((mesh_slots, width)),
            flat((mesh_slots, width)),
            flat((mesh_slots, grid_slots), BF16),
        ]
        + halves * 5
        + [flat((8, width))],
        halves * 2 + [flat((grid_slots, width)), flat((8, width))],
        [
            pltpu.VMEM((grid_slots, width), F32),
            pltpu.VMEM((mesh_slots, width), F32),
            pltpu.VMEM((number, grid_slots), F32),
            pltpu.VMEM((mesh_slots, grid_slots), F32),
        ],
    )
    sent, parts = call(
        encode_kernel,
        "encode",
        (3 * grid_slots + mesh_slots) * square * 3,
        [],
        [],
        [grid_in, *first],
        [first_low, match, self_sent, onward_high, onward_low, update_high, nodes_sent],
        [flat((mesh_slots, width)), flat((grid_slots, width))],
    )
    mesh_in = exchange(sent, patches)
    *first, normed, base, firsts = call(
        between_kernel,
        "between",
        (3 * number + mesh_slots) * square * 3,
        [mesh_targets],
        [
            grid_targets,
            mesh_targets,
            mesh_geometry,
            process_geometry,
            row(process_bias),
            row(refine_bias),
            row(update_outbias),
            row(refine_outbias),
        ],
        [],
        [
            parts,
            self_all,
            mesh_latent,
            update_high,
            update_low,
            refine_self,
            process_receiver,
            refine_high,
            refine_low,
        ],
        [
            flat((mesh_slots, width)),
            flat((number, width)),
            flat((number, mesh_slots), BF16),
        ],
        [
            *halves,
            halves[0],
            flat((mesh_slots, width)),
            flat((mesh_slots, width)),
            flat((mesh_slots, mesh_slots), BF16),
            flat((8, width)),
        ],
        [
            pltpu.VMEM((mesh_slots, width), F32),
            pltpu.VMEM((number, width), F32),
            pltpu.VMEM((number, width), F32),
            pltpu.VMEM((number, width), F32),
            pltpu.VMEM((number + 8, mesh_slots), F32),
            pltpu.VMEM((mesh_slots, mesh_slots), F32),
        ],
        [merged_high, merged_low, second_high, biases],
    )
    (out,) = call(
        refine_kernel,
        "refine",
        4 * mesh_slots * square * 3,
        [],
        [],
        [mesh_in, *first],
        [
            refine_high,
            refine_low,
            normed,
            firsts,
            base,
        ],
        [flat((number, width))],
    )
    return out


def solution(mesh):
    patch = P(("lat", "lon"), None)
    block = P(("lat", "lon"), None, None)
    feature = P(None, ("lat", "lon"), None)
    return jax.shard_map(
        per_device,
        mesh=mesh,
        in_specs=(P("lat", "lon", None), patch, block, patch, feature, block, patch, feature)
        + (P(),) * 22,
        out_specs=patch,
        check_vma=False,
    )
```
